16 devices in a mesh: task: 2 (over y, z), row: 8 (over x, core).
Axes of the slice: x: 4, y: 2, z: 1, core: 2. Of those that a mesh axis runs over, the one named last changes fastest.
The devices are a block of a 4x4x8 slice.
Arguments:
- points: bfloat16 [32768, 768], P(('task', 'row')), parts along dimension 0
- vectors: bfloat16 [32768, 64], P(('task', 'row')), parts along dimension 0
- length_scale: float32 [2], P('task'), parts along dimension 0
- out_scale: float32 [2], P('task'), parts along dimension 0
Outputs:
- output: float32 [32768, 64], P(('task', 'row')), parts along dimension 0
There are 2 independent parts. The reference program is written for one: setup_inputs(seed, part) draws one part's arguments, and reference() takes and returns one part's arrays. A program takes and returns all parts, laid end to end along the dimension named above; each array names one.
All inputs are finite; a program needn't handle non-finite values.
Results may differ from the reference program's by a relative error of at most 0.001.
Values are sent between devices in bfloat16 or wider.
A program may use at most 768 MiB of HBM per device.

```python
import jax
import jax.numpy as jnp
from jax import lax

ROWS_DEV = 2048
GROUP = 8
FEAT = 768
COLS = 64
N_POINTS = GROUP * ROWS_DEV


def setup_inputs(seed: int = 0, part: int = 0) -> dict:
    base_key = jax.random.fold_in(jax.random.key(seed), part)
    key_x, key_o, key_m, key_v, key_l, key_s = jax.random.split(base_key, 6)
    base_pts = jax.random.normal(key_x, (GROUP, ROWS_DEV, FEAT), jnp.float32)
    offset = 1.6 * jax.random.normal(key_o, (GROUP, 1, FEAT), jnp.float32)
    points = (base_pts + offset).reshape(N_POINTS, FEAT).astype(jnp.bfloat16)
    block_mean = jax.random.normal(key_m, (GROUP, 1, COLS), jnp.float32)
    block_mean = block_mean - jnp.mean(block_mean, axis=0, keepdims=True)
    noise_val = 0.5 * jax.random.normal(key_v, (GROUP, ROWS_DEV, COLS), jnp.float32)
    vectors = (block_mean + noise_val).reshape(N_POINTS, COLS).astype(jnp.bfloat16)
    ell_ratio = jax.random.uniform(key_l, (1,), jnp.float32, 0.8, 1.25)
    length_scale = jnp.sqrt(2.0 * FEAT * ell_ratio)
    out_scale = jax.random.uniform(key_s, (1,), jnp.float32, 1.0, 2.0) / ROWS_DEV
    return {"points": points, "vectors": vectors, "length_scale": length_scale, "out_scale": out_scale}


def kernel_tile(x_rows, x_cols, length_scale, out_scale):
    norm_rows = jnp.sum(jnp.square(x_rows.astype(jnp.float32)), axis=1)
    norm_cols = jnp.sum(jnp.square(x_cols.astype(jnp.float32)), axis=1)
    gram_mat = jnp.dot(x_rows, x_cols.T, preferred_element_type=jnp.float32)
    sq_dist = jnp.maximum(norm_rows[:, None] + norm_cols[None, :] - 2.0 * gram_mat, 0.0)
    return (out_scale * jnp.exp(-sq_dist / (2.0 * length_scale * length_scale))).astype(jnp.bfloat16)


def kernel_apply(points, vectors, length_scale, out_scale):
    x_blocks = points.reshape(GROUP, ROWS_DEV, FEAT)
    v_blocks = vectors.reshape(GROUP, ROWS_DEV, COLS)

    def row_block(x_rows):
        def col_step(running, col_pair):
            x_cols, v_cols = col_pair
            kern_tile = kernel_tile(x_rows, x_cols, length_scale, out_scale)
            return running + jnp.dot(kern_tile, v_cols, preferred_element_type=jnp.float32), None

        running, _ = lax.scan(col_step, jnp.zeros((ROWS_DEV, COLS), jnp.float32), (x_blocks, v_blocks))
        return running

    return lax.map(row_block, x_blocks).reshape(N_POINTS, COLS)


def reference(points, vectors, length_scale, out_scale):
    first_pass = kernel_apply(points, vectors, length_scale, out_scale).astype(jnp.bfloat16)
    return kernel_apply(points, first_pass, length_scale, out_scale)
```

```python
import functools

import jax
import jax.numpy as jnp
from jax import lax
from jax.experimental import pallas as pl
from jax.experimental.pallas import tpu as pltpu
from jax.sharding import PartitionSpec as P

F32 = jnp.float32
BF16 = jnp.bfloat16
LOG2E = 1.4426950408889634
OWN, PLUS, MINUS, CROSS, SIB = 0, 1, 2, 3, 4
N_BIG, BIG, N_SMALL, SMALL = 3, 512, 2, 256
N_PIECE = N_BIG + N_SMALL


def dot_nn(a, b):
    return lax.dot_general(a, b, (((1,), (0,)), ((), ())), preferred_element_type=F32)


def dot_nt(a, b):
    return lax.dot_general(a, b, (((1,), (1,)), ((), ())), preferred_element_type=F32)


def kernel(n_row, x_hbm, vt_hbm, coef, out_hbm, xb, kb, vb, yb, hr, acc, rb,
           x_s, x_r, f_s, f_r, sib_s, sib_r, loc, v_s, v_r, y_s, y_r, p_s, p_r, free):
    rows = xb.shape[1]
    me = lax.axis_index("row")
    core = me % 2
    sib = me + 1 - 2 * core
    plus = (me + 2) % n_row
    minus = (me + n_row - 2) % n_row
    far = 2 + (me // 2) // 2

    def remote(src, dst, s_sem, r_sem, dev):
        return pltpu.make_async_remote_copy(
            src_ref=src, dst_ref=dst, send_sem=s_sem, recv_sem=r_sem,
            device_id={"row": dev}, device_id_type=pl.DeviceIdType.MESH)

    def x_copy(direction, piece, start, width):
        slot, dev = ((MINUS, plus), (PLUS, minus))[direction]
        return remote(x_hbm.at[pl.ds(start, width)], xb.at[slot, pl.ds(start, width)],
                      x_s.at[direction, piece], x_r.at[direction, piece], dev)

    def forward(piece, start, width):
        return remote(xb.at[MINUS, pl.ds(start, width)], xb.at[CROSS, pl.ds(start, width)],
                      f_s.at[piece], f_r.at[piece], sib)

    def vec_copies(src, buf, s_sem, r_sem):
        return (remote(src, buf.at[MINUS], s_sem.at[0], r_sem.at[0], plus),
                remote(src, buf.at[PLUS], s_sem.at[1], r_sem.at[1], minus),
                remote(src, buf.at[SIB], s_sem.at[2], r_sem.at[2], sib),
                remote(buf.at[MINUS], buf.at[CROSS], s_sem.at[3], r_sem.at[3], sib))

    def part_copies(step):
        return (remote(acc.at[PLUS], rb.at[0], p_s.at[step, 0], p_r.at[step, 0], plus),
                remote(acc.at[MINUS], rb.at[1], p_s.at[step, 1], p_r.at[step, 1], minus),
                remote(acc.at[CROSS], rb.at[2], p_s.at[step, 2], p_r.at[step, 2], sib))

    pieces = [(i, i * BIG, BIG) for i in range(N_BIG)]
    pieces += [(N_BIG + i, N_BIG * BIG + i * SMALL, SMALL) for i in range(N_SMALL)]

    barrier = pltpu.get_barrier_semaphore()
    for dev in (sib, plus, minus):
        pl.semaphore_signal(barrier, inc=1, device_id={"row": dev}, device_id_type=pl.DeviceIdType.MESH)
    pl.semaphore_wait(barrier, 3)

    own_x = pltpu.make_async_copy(x_hbm, xb.at[OWN], loc.at[0])
    own_v = pltpu.make_async_copy(vt_hbm, vb.at[OWN], loc.at[1])
    own_x.start()
    own_v.start()
    v_plus, v_minus, v_sib, v_cross = vec_copies(vt_hbm, vb, v_s, v_r)
    sib_x = remote(x_hbm, xb.at[CROSS], sib_s, sib_r, sib)
    v_plus.start()
    v_minus.start()
    for piece in pieces:
        x_copy(0, *piece).start()
        x_copy(1, *piece).start()
    v_sib.start()
    sib_x.start()

    coef_d = coef[0, 0]
    coef_s = coef[0, 1]
    eye = (lax.broadcasted_iota(jnp.int32, (128, 128), 0) == lax.broadcasted_iota(jnp.int32, (128, 128), 1))

    def half_norms(slot, start, width):
        for sub in range(0, width, 128):
            x_sub = xb[slot, pl.ds(start + sub, 128), :].astype(F32)
            col = jnp.sum(x_sub * x_sub, axis=1, keepdims=True) * 0.5
            hr[slot, :, pl.ds(start + sub, 128)] = jnp.sum(jnp.where(eye, col, 0.0), axis=0, keepdims=True)

    def tile(p_slot, p0, m, q_slot, q0, n, k_slot, v_p, acc_q, v_q=None, acc_p=None):
        gram = dot_nt(xb[p_slot, pl.ds(p0, m), :], xb[q_slot, pl.ds(q0, n), :])
        h_q = hr[q_slot, :, pl.ds(q0, n)]
        for sub in range(0, m, 128):
            h_row = hr[p_slot, :, pl.ds(p0 + sub, 128)]
            h_p = jnp.sum(jnp.where(eye, h_row, 0.0), axis=1, keepdims=True)
            half_d = jnp.maximum(h_p + h_q - gram[sub:sub + 128], 0.0)
            kb[k_slot, pl.ds(p0 + sub, 128), pl.ds(q0, n)] = (coef_s * jnp.exp2(half_d * coef_d)).astype(BF16)
        k_tile = kb[k_slot, pl.ds(p0, m), pl.ds(q0, n)]
        acc[acc_q, :, pl.ds(q0, n)] += dot_nn(vb[v_p, :, pl.ds(p0, m)], k_tile)
        if v_q is not None:
            acc[acc_p, :, pl.ds(p0, m)] += dot_nt(vb[v_q, :, pl.ds(q0, n)], k_tile)

    def mul(i, size):
        return pl.multiple_of(i * size, size)

    acc[...] = jnp.zeros_like(acc)
    own_x.wait()
    own_v.wait()

    def norm_loop(slot):
        @pl.loop(0, rows // 256)
        def _(i):
            half_norms(slot, mul(i, 256), 256)

    norm_loop(OWN)
    side = rows // 512

    @pl.loop(0, side * side)
    def _(i):
        tile(OWN, mul(i // side, 512), 512, OWN, mul(i % side, 512), 512, 0, OWN, OWN)

    sib_x.wait_recv()
    v_sib.wait_recv()
    norm_loop(CROSS)

    @pl.loop(0, side * side)
    def _(i):
        tile(CROSS, mul(i // side, 512), 512, OWN, mul(i % side, 512), 512, 1, SIB, OWN)

    pl.semaphore_signal(free, inc=1, device_id={"row": sib}, device_id_type=pl.DeviceIdType.MESH)
    v_minus.wait_recv()
    v_plus.wait_recv()
    v_cross.start()
    pl.semaphore_wait(free, 1)
    v_cross.wait_recv()

    def own_pairs(q0, n, m):
        @pl.loop(0, rows // m)
        def _(i):
            tile(OWN, mul(i, m), m, PLUS, q0, n, 2, OWN, PLUS, PLUS, OWN)

    def own_cross(q0, n, m):
        @pl.loop(0, rows // m)
        def _(i):
            tile(OWN, mul(i, m), m, CROSS, q0, n, 3, OWN, CROSS, CROSS, OWN)

    def far_tile(p0, m, q0, n):
        tile(PLUS, p0, m, far, q0, n, 4, PLUS, far, far, PLUS)

    def arrive(piece, start, width, m):
        x_copy(0, piece, start, width).wait_recv()
        forward(piece, start, width).start()
        x_copy(1, piece, start, width).wait_recv()
        for sub in range(0, width, 256):
            half_norms(PLUS, start + sub, 256)
            half_norms(MINUS, start + sub, 256)
        own_pairs(start, width, m)
        forward(piece, start, width).wait_recv()
        for sub in range(0, width, 256):
            half_norms(CROSS, start + sub, 256)
        own_cross(start, width, m)

    @pl.loop(0, N_BIG)
    def _(j):
        start = mul(j, BIG)
        arrive(j, start, BIG, 512)

        @pl.loop(0, j)
        def _(i):
            far_tile(mul(i, BIG), BIG, start, BIG)

        @pl.loop(0, j + 1)
        def _(i):
            far_tile(start, BIG, mul(i, BIG), BIG)

    @pl.loop(0, N_SMALL)
    def _(j):
        start = pl.multiple_of(N_BIG * BIG + j * SMALL, SMALL)
        arrive(N_BIG + j, start, SMALL, 1024)

        @pl.loop(0, N_BIG)
        def _(i):
            far_tile(mul(i, BIG), BIG, start, SMALL)

        @pl.loop(0, N_BIG)
        def _(i):
            far_tile(start, SMALL, mul(i, BIG), BIG)

    far_tile(N_BIG * BIG, N_SMALL * SMALL, N_BIG * BIG, N_SMALL * SMALL)

    def exchange(step):
        to_plus, to_minus, to_sib = part_copies(step)
        to_sib.start()
        to_plus.start()
        to_sib.wait_recv()
        acc[MINUS] += rb[2]
        to_minus.start()
        return to_plus, to_minus, to_sib

    copies = exchange(0)
    copies[0].wait_recv()
    copies[1].wait_recv()
    yb[OWN] = (acc[OWN] + rb[0] + rb[1]).astype(BF16)
    y_plus, y_minus, y_sib, y_cross = vec_copies(yb.at[OWN], yb, y_s, y_r)
    y_plus.start()
    y_minus.start()
    y_sib.start()
    for copy in copies:
        copy.wait_send()
    acc[...] = jnp.zeros_like(acc)

    half = rows // 2

    def apply_nn(k_slot, y_slot, out):
        for q0 in (0, half):
            acc[out, :, pl.ds(q0, half)] += dot_nn(yb[y_slot], kb[k_slot, :, pl.ds(q0, half)])

    def apply_nt(k_slot, y_slot, out):
        for p0 in (0, half):
            acc[out, :, pl.ds(p0, half)] += dot_nt(yb[y_slot], kb[k_slot, pl.ds(p0, half), :])

    @pl.loop(0, 3)
    def _(i):
        apply_nn((2 + i) % 4, OWN, (1 + 2 * i) % 5)

    y_sib.wait_recv()
    apply_nn(1, SIB, OWN)
    y_plus.wait_recv()
    y_cross.start()
    y_minus.wait_recv()
    apply_nn(4, PLUS, far)
    y_cross.wait_recv()
    apply_nt(4, far, PLUS)
    to_plus, to_minus, to_sib = exchange(1)

    @pl.loop(0, 2)
    def _(i):
        apply_nt(2 + i, 1 + 2 * i, OWN)

    to_plus.wait_recv()
    to_minus.wait_recv()
    acc[OWN] += rb[0] + rb[1]
    out_copy = pltpu.make_async_copy(acc.at[OWN], out_hbm, loc.at[0])
    out_copy.start()
    for copy in (to_plus, to_minus, to_sib, y_plus, y_minus, y_sib, y_cross, v_plus, v_minus, v_sib, v_cross, sib_x):
        copy.wait_send()
    for piece in pieces:
        x_copy(0, *piece).wait_send()
        x_copy(1, *piece).wait_send()
        forward(*piece).wait_send()
    out_copy.wait()


def solution(mesh):
    n_row = mesh.shape["row"]
    assert n_row == 8

    def local_program(x_loc, v_loc, length_scale, out_scale):
        rows, feat = x_loc.shape
        cols = v_loc.shape[1]
        coef = jnp.stack([-LOG2E / (length_scale[0] * length_scale[0]), out_scale[0]]).reshape(1, 2)
        dma = pltpu.SemaphoreType.DMA
        out = pl.pallas_call(
            functools.partial(kernel, n_row),
            out_shape=jax.ShapeDtypeStruct((cols, rows), F32),
            in_specs=[pl.BlockSpec(memory_space=pl.ANY), pl.BlockSpec(memory_space=pl.ANY),
                      pl.BlockSpec(memory_space=pltpu.SMEM)],
            out_specs=pl.BlockSpec(memory_space=pl.ANY),
            scratch_shapes=[
                pltpu.VMEM((4, rows, feat), BF16),
                pltpu.VMEM((5, rows, rows), BF16),
                pltpu.VMEM((5, cols, rows), BF16),
                pltpu.VMEM((5, cols, rows), BF16),
                pltpu.VMEM((4, 1, rows), F32),
                pltpu.VMEM((4, cols, rows), F32),
                pltpu.VMEM((3, cols, rows), F32),
                dma((2, N_PIECE)), dma((2, N_PIECE)), dma((N_PIECE,)), dma((N_PIECE,)),
                dma, dma, dma((2,)), dma((4,)), dma((4,)), dma((4,)), dma((4,)),
                dma((2, 3)), dma((2, 3)), pltpu.SemaphoreType.REGULAR,
            ],
            compiler_params=pltpu.CompilerParams(
                collective_id=0, has_side_effects=True, vmem_limit_bytes=67043328),
        )(x_loc, v_loc.T, coef)
        return out.T

    row_spec = P(("task", "row"), None)
    return jax.shard_map(local_program, mesh=mesh, in_specs=(row_spec, row_spec, P("task"), P("task")),
                         out_specs=row_spec, check_vma=False)
```

```python
import functools

import jax
import jax.numpy as jnp
from jax import lax
from jax.experimental import pallas as pl
from jax.experimental.pallas import tpu as pltpu
from jax.sharding import PartitionSpec as P

F32 = jnp.float32
BF16 = jnp.bfloat16
LOG2E = 1.4426950408889634
OWN, PLUS, MINUS, CROSS, SIB = 0, 1, 2, 3, 4
TRASH = 4
T = 512
N_PIECE = 4


def dot_nn(a, b):
    return lax.dot_general(a, b, (((1,), (0,)), ((), ())), preferred_element_type=F32)


def dot_nt(a, b):
    return lax.dot_general(a, b, (((1,), (1,)), ((), ())), preferred_element_type=F32)


def kernel(n_row, x_hbm, vt_hbm, coef, out_hbm, xb, kb, vb, yb, hr, acc, rb,
           x_s, x_r, f_s, f_r, sib_s, sib_r, loc, v_s, v_r, y_s, y_r, p_s, p_r, free):
    rows = xb.shape[1]
    me = lax.axis_index("row")
    core = me % 2
    sib = me + 1 - 2 * core
    plus = (me + 2) % n_row
    minus = (me + n_row - 2) % n_row
    far = 2 + (me // 2) // 2

    def remote(src, dst, s_sem, r_sem, dev):
        return pltpu.make_async_remote_copy(
            src_ref=src, dst_ref=dst, send_sem=s_sem, recv_sem=r_sem,
            device_id={"row": dev}, device_id_type=pl.DeviceIdType.MESH)

    def x_copy(direction, piece, start, width):
        slot, dev = ((MINUS, plus), (PLUS, minus))[direction]
        return remote(x_hbm.at[pl.ds(start, width)], xb.at[slot, pl.ds(start, width)],
                      x_s.at[direction, piece], x_r.at[direction, piece], dev)

    def forward(piece, start, width):
        return remote(xb.at[MINUS, pl.ds(start, width)], xb.at[CROSS, pl.ds(start, width)],
                      f_s.at[piece], f_r.at[piece], sib)

    def vec_copies(src, buf, s_sem, r_sem):
        return (remote(src, buf.at[MINUS], s_sem.at[0], r_sem.at[0], plus),
                remote(src, buf.at[PLUS], s_sem.at[1], r_sem.at[1], minus),
                remote(src, buf.at[SIB], s_sem.at[2], r_sem.at[2], sib),
                remote(buf.at[MINUS], buf.at[CROSS], s_sem.at[3], r_sem.at[3], sib))

    def part_copies(step):
        return (remote(acc.at[PLUS], rb.at[0], p_s.at[step, 0], p_r.at[step, 0], plus),
                remote(acc.at[MINUS], rb.at[1], p_s.at[step, 1], p_r.at[step, 1], minus),
                remote(acc.at[CROSS], rb.at[2], p_s.at[step, 2], p_r.at[step, 2], sib))

    pieces = [(i, i * T, T) for i in range(N_PIECE)]

    barrier = pltpu.get_barrier_semaphore()
    for dev in (sib, plus, minus):
        pl.semaphore_signal(barrier, inc=1, device_id={"row": dev}, device_id_type=pl.DeviceIdType.MESH)
    pl.semaphore_wait(barrier, 3)

    own_x = pltpu.make_async_copy(x_hbm, xb.at[OWN], loc.at[0])
    own_v = pltpu.make_async_copy(vt_hbm, vb.at[OWN], loc.at[1])
    own_x.start()
    own_v.start()
    v_plus, v_minus, v_sib, v_cross = vec_copies(vt_hbm, vb, v_s, v_r)
    sib_x = remote(x_hbm, xb.at[CROSS], sib_s, sib_r, sib)
    v_plus.start()
    v_minus.start()
    for piece in pieces:
        x_copy(0, *piece).start()
        x_copy(1, *piece).start()
    v_sib.start()
    sib_x.start()

    coef_d = coef[0, 0]
    coef_s = coef[0, 1]
    eye = (lax.broadcasted_iota(jnp.int32, (128, 128), 0) == lax.broadcasted_iota(jnp.int32, (128, 128), 1))

    def half_norms(slot, start, width):
        for sub in range(0, width, 128):
            x_sub = xb[slot, pl.ds(start + sub, 128), :].astype(F32)
            col = jnp.sum(x_sub * x_sub, axis=1, keepdims=True) * 0.5
            hr[slot, :, pl.ds(start + sub, 128)] = jnp.sum(jnp.where(eye, col, 0.0), axis=0, keepdims=True)

    def products(pend, both):
        k_slot, p0, q0, v_p, acc_q, v_q, acc_p = pend
        k_tile = kb[k_slot, pl.ds(p0, T), pl.ds(q0, T)]
        acc[acc_q, :, pl.ds(q0, T)] += dot_nn(vb[v_p, :, pl.ds(p0, T)], k_tile)
        if both:
            acc[acc_p, :, pl.ds(p0, T)] += dot_nt(vb[v_q, :, pl.ds(q0, T)], k_tile)

    def tile(p_slot, p0, q_slot, q0, k_slot, pend, both):
        gram = dot_nt(xb[p_slot, pl.ds(p0, T), :], xb[q_slot, pl.ds(q0, T), :])
        products(pend, both)
        h_q = hr[q_slot, :, pl.ds(q0, T)]
        for sub in range(0, T, 128):
            h_row = hr[p_slot, :, pl.ds(p0 + sub, 128)]
            h_p = jnp.sum(jnp.where(eye, h_row, 0.0), axis=1, keepdims=True)
            half_d = jnp.maximum(h_p + h_q - gram[sub:sub + 128], 0.0)
            kb[k_slot, pl.ds(p0 + sub, 128), pl.ds(q0, T)] = (coef_s * jnp.exp2(half_d * coef_d)).astype(BF16)

    def tiles(count, place, pend, p_slot, q_slot, k_slot, v_p, acc_q, v_q, acc_p, both=True, unroll=1):
        def one(i, pend):
            p_i, q_i = place(i)
            p0, q0 = mul(p_i, T), mul(q_i, T)
            pend = (pend[0], pl.multiple_of(pend[1], T), pl.multiple_of(pend[2], T)) + tuple(pend[3:])
            tile(p_slot, p0, q_slot, q0, k_slot, pend, both)
            return tuple(jnp.int32(v) for v in (k_slot, p0, q0, v_p, acc_q, v_q, acc_p))

        def step(i, pend):
            for sub in range(unroll):
                pend = one(i * unroll + sub, pend)
            return pend

        return lax.fori_loop(0, count // unroll, step, pend)

    def flush(pend, both):
        products((pend[0], pl.multiple_of(pend[1], T), pl.multiple_of(pend[2], T)) + tuple(pend[3:]), both)

    nothing = tuple(jnp.int32(v) for v in (0, 0, 0, OWN, TRASH, OWN, TRASH))

    def mul(i, size):
        return pl.multiple_of(i * size, size)

    acc[...] = jnp.zeros_like(acc)
    own_x.wait()
    own_v.wait()

    def norm_loop(slot):
        @pl.loop(0, rows // 256)
        def _(i):
            half_norms(slot, mul(i, 256), 256)

    norm_loop(OWN)
    side = rows // T
    pend = tiles(side * side, lambda i: (i // side, i % side), nothing, OWN, OWN, 0, OWN, OWN, OWN, TRASH, False, 4)

    sib_x.wait_recv()
    v_sib.wait_recv()
    norm_loop(CROSS)

    pend = tiles(side * side, lambda i: (i // side, i % side), pend, CROSS, OWN, 1, SIB, OWN, OWN, TRASH, False, 4)
    flush(pend, False)
    pl.semaphore_signal(free, inc=1, device_id={"row": sib}, device_id_type=pl.DeviceIdType.MESH)
    v_minus.wait_recv()
    v_plus.wait_recv()
    v_cross.start()
    pl.semaphore_wait(free, 1)
    v_cross.wait_recv()

    def stage(j, pend):
        start = mul(j, T)
        x_copy(0, j, start, T).wait_recv()
        forward(j, start, T).start()
        x_copy(1, j, start, T).wait_recv()
        half_norms(PLUS, start, T)
        half_norms(MINUS, start, T)
        pend = tiles(side, lambda i: (i, j), pend, OWN, PLUS, 2, OWN, PLUS, PLUS, OWN, True, 4)
        forward(j, start, T).wait_recv()
        half_norms(CROSS, start, T)
        pend = tiles(side, lambda i: (i, j), pend, OWN, CROSS, 3, OWN, CROSS, CROSS, OWN, True, 4)
        pend = tiles(1, lambda i: (j, j), pend, PLUS, far, 4, PLUS, far, far, PLUS)
        return tiles(2 * j, lambda i: (jnp.where(i % 2 == 0, i // 2, j), jnp.where(i % 2 == 0, j, i // 2)), pend,
                     PLUS, far, 4, PLUS, far, far, PLUS, True, 2)

    pend = lax.fori_loop(0, side, stage, nothing)
    flush(pend, True)

    def exchange(step):
        to_plus, to_minus, to_sib = part_copies(step)
        to_sib.start()
        to_plus.start()
        to_sib.wait_recv()
        acc[MINUS] += rb[2]
        to_minus.start()
        return to_plus, to_minus, to_sib

    copies = exchange(0)
    copies[0].wait_recv()
    copies[1].wait_recv()
    yb[OWN] = (acc[OWN] + rb[0] + rb[1]).astype(BF16)
    y_plus, y_minus, y_sib, y_cross = vec_copies(yb.at[OWN], yb, y_s, y_r)
    y_plus.start()
    y_minus.start()
    y_sib.start()
    for copy in copies:
        copy.wait_send()
    acc[...] = jnp.zeros_like(acc)

    half = rows // 2

    def apply_nn(k_slot, y_slot, out):
        for q0 in (0, half):
            acc[out, :, pl.ds(q0, half)] += dot_nn(yb[y_slot], kb[k_slot, :, pl.ds(q0, half)])

    def apply_nt(k_slot, y_slot, out):
        for p0 in (0, half):
            acc[out, :, pl.ds(p0, half)] += dot_nt(yb[y_slot], kb[k_slot, pl.ds(p0, half), :])

    @pl.loop(0, 3)
    def _(i):
        apply_nn((2 + i) % 4, OWN, (1 + 2 * i) % 5)

    y_sib.wait_recv()
    apply_nn(1, SIB, OWN)
    y_plus.wait_recv()
    y_cross.start()
    y_minus.wait_recv()
    apply_nn(4, PLUS, far)
    y_cross.wait_recv()
    apply_nt(4, far, PLUS)
    to_plus, to_minus, to_sib = exchange(1)

    @pl.loop(0, 2)
    def _(i):
        apply_nt(2 + i, 1 + 2 * i, OWN)

    to_plus.wait_recv()
    to_minus.wait_recv()
    acc[OWN] += rb[0] + rb[1]
    out_copy = pltpu.make_async_copy(acc.at[OWN], out_hbm, loc.at[0])
    out_copy.start()
    for copy in (to_plus, to_minus, to_sib, y_plus, y_minus, y_sib, y_cross, v_plus, v_minus, v_sib, v_cross, sib_x):
        copy.wait_send()
    for piece in pieces:
        x_copy(0, *piece).wait_send()
        x_copy(1, *piece).wait_send()
        forward(*piece).wait_send()
    out_copy.wait()


def solution(mesh):
    n_row = mesh.shape["row"]
    assert n_row == 8

    def local_program(x_loc, v_loc, length_scale, out_scale):
        rows, feat = x_loc.shape
        cols = v_loc.shape[1]
        coef = jnp.stack([-LOG2E / (length_scale[0] * length_scale[0]), out_scale[0]]).reshape(1, 2)
        dma = pltpu.SemaphoreType.DMA
        out = pl.pallas_call(
            functools.partial(kernel, n_row),
            out_shape=jax.ShapeDtypeStruct((cols, rows), F32),
            in_specs=[pl.BlockSpec(memory_space=pl.ANY), pl.BlockSpec(memory_space=pl.ANY),
                      pl.BlockSpec(memory_space=pltpu.SMEM)],
            out_specs=pl.BlockSpec(memory_space=pl.ANY),
            scratch_shapes=[
                pltpu.VMEM((4, rows, feat), BF16),
                pltpu.VMEM((5, rows, rows), BF16),
                pltpu.VMEM((5, cols, rows), BF16),
                pltpu.VMEM((5, cols, rows), BF16),
                pltpu.VMEM((4, 1, rows), F32),
                pltpu.VMEM((5, cols, rows), F32),
                pltpu.VMEM((3, cols, rows), F32),
                dma((2, N_PIECE)), dma((2, N_PIECE)), dma((N_PIECE,)), dma((N_PIECE,)),
                dma, dma, dma((2,)), dma((4,)), dma((4,)), dma((4,)), dma((4,)),
                dma((2, 3)), dma((2, 3)), pltpu.SemaphoreType.REGULAR,
            ],
            compiler_params=pltpu.CompilerParams(
                collective_id=0, has_side_effects=True, vmem_limit_bytes=67043328),
        )(x_loc, v_loc.T, coef)
        return out.T

    row_spec = P(("task", "row"), None)
    return jax.shard_map(local_program, mesh=mesh, in_specs=(row_spec, row_spec, P("task"), P("task")),
                         out_specs=row_spec, check_vma=False)
```

```python
import functools

import jax
import jax.numpy as jnp
from jax import lax
from jax.experimental import pallas as pl
from jax.experimental.pallas import tpu as pltpu
from jax.sharding import PartitionSpec as P

F32 = jnp.float32
BF16 = jnp.bfloat16
LOG2E = 1.4426950408889634
OWN, PLUS, MINUS, CROSS, SIB = 0, 1, 2, 3, 4
TRASH = 4
T = 512
N_PIECE = 4


def dot_nn(a, b):
    return lax.dot_general(a, b, (((1,), (0,)), ((), ())), preferred_element_type=F32)


def dot_nt(a, b):
    return lax.dot_general(a, b, (((1,), (1,)), ((), ())), preferred_element_type=F32)


def kernel(n_row, x_hbm, vt_hbm, coef, out_hbm, xb, kb, vb, yb, hr, acc, acc2, rb,
           x_s, x_r, f_s, f_r, sib_s, sib_r, loc, v_s, v_r, y_s, y_r, p_s, p_r, free):
    rows = xb.shape[1]
    me = lax.axis_index("row")
    core = me % 2
    sib = me + 1 - 2 * core
    plus = (me + 2) % n_row
    minus = (me + n_row - 2) % n_row
    far = 2 + (me // 2) // 2

    def remote(src, dst, s_sem, r_sem, dev):
        return pltpu.make_async_remote_copy(
            src_ref=src, dst_ref=dst, send_sem=s_sem, recv_sem=r_sem,
            device_id={"row": dev}, device_id_type=pl.DeviceIdType.MESH)

    def x_copy(direction, piece, start, width):
        slot, dev = ((MINUS, plus), (PLUS, minus))[direction]
        return remote(x_hbm.at[pl.ds(start, width)], xb.at[slot, pl.ds(start, width)],
                      x_s.at[direction, piece], x_r.at[direction, piece], dev)

    def forward(piece, start, width):
        return remote(xb.at[MINUS, pl.ds(start, width)], xb.at[CROSS, pl.ds(start, width)],
                      f_s.at[piece], f_r.at[piece], sib)

    def vec_copies(own, src, buf, s_sem, r_sem):
        return (remote(own, src(buf, MINUS), s_sem(0), r_sem(0), plus),
                remote(own, src(buf, PLUS), s_sem(1), r_sem(1), minus),
                remote(own, src(buf, SIB), s_sem(2), r_sem(2), sib),
                remote(src(buf, MINUS), src(buf, CROSS), s_sem(3), r_sem(3), sib))

    def y_copies(k):
        part = lambda buf, slot: buf.at[slot, :, pl.ds(mul(k, T), T)]
        return vec_copies(part(yb, OWN), part, yb, lambda d: y_s.at[d, k], lambda d: y_r.at[d, k])

    def part_copies(step, buf, k):
        cols = pl.ds(mul(k, T), T)
        return tuple(remote(buf.at[slot, :, cols], rb.at[i, :, cols], p_s.at[step, i, k], p_r.at[step, i, k], dev)
                     for i, (slot, dev) in enumerate(((PLUS, plus), (MINUS, minus), (CROSS, sib))))

    def mul(i, size):
        return i * size if isinstance(i, int) else pl.multiple_of(i * size, size)

    pieces = [(i, i * T, T) for i in range(N_PIECE)]

    barrier = pltpu.get_barrier_semaphore()
    for dev in (sib, plus, minus):
        pl.semaphore_signal(barrier, inc=1, device_id={"row": dev}, device_id_type=pl.DeviceIdType.MESH)
    pl.semaphore_wait(barrier, 3)

    own_x = pltpu.make_async_copy(x_hbm, xb.at[OWN], loc.at[0])
    own_v = pltpu.make_async_copy(vt_hbm, vb.at[OWN], loc.at[1])
    own_x.start()
    own_v.start()
    v_plus, v_minus, v_sib, v_cross = vec_copies(
        vt_hbm, lambda buf, slot: buf.at[slot], vb, lambda d: v_s.at[d], lambda d: v_r.at[d])
    sib_x = remote(x_hbm, xb.at[CROSS], sib_s, sib_r, sib)
    v_plus.start()
    v_minus.start()
    for piece in pieces:
        x_copy(0, *piece).start()
        x_copy(1, *piece).start()
    v_sib.start()
    sib_x.start()

    coef_d = coef[0, 0]
    coef_s = coef[0, 1]
    eye = (lax.broadcasted_iota(jnp.int32, (128, 128), 0) == lax.broadcasted_iota(jnp.int32, (128, 128), 1))

    def half_norms(slot, start, width):
        for sub in range(0, width, 128):
            x_sub = xb[slot, pl.ds(start + sub, 128), :].astype(F32)
            col = jnp.sum(x_sub * x_sub, axis=1, keepdims=True) * 0.5
            hr[slot, :, pl.ds(start + sub, 128)] = jnp.sum(jnp.where(eye, col, 0.0), axis=0, keepdims=True)

    def products(pend, both):
        k_slot, p0, q0, v_p, acc_q, v_q, acc_p = pend
        k_tile = kb[k_slot, pl.ds(p0, T), pl.ds(q0, T)]
        acc[acc_q, :, pl.ds(q0, T)] += dot_nn(vb[v_p, :, pl.ds(p0, T)], k_tile)
        if both:
            acc[acc_p, :, pl.ds(p0, T)] += dot_nt(vb[v_q, :, pl.ds(q0, T)], k_tile)

    def tile(p_slot, p0, q_slot, q0, k_slot, pend, both):
        gram = dot_nt(xb[p_slot, pl.ds(p0, T), :], xb[q_slot, pl.ds(q0, T), :])
        products(pend, both)
        h_q = hr[q_slot, :, pl.ds(q0, T)]
        for sub in range(0, T, 128):
            h_row = hr[p_slot, :, pl.ds(p0 + sub, 128)]
            h_p = jnp.sum(jnp.where(eye, h_row, 0.0), axis=1, keepdims=True)
            half_d = jnp.maximum(h_p + h_q - gram[sub:sub + 128], 0.0)
            kb[k_slot, pl.ds(p0 + sub, 128), pl.ds(q0, T)] = (coef_s * jnp.exp2(half_d * coef_d)).astype(BF16)

    def tiles(count, place, pend, p_slot, q_slot, k_slot, v_p, acc_q, v_q, acc_p, both=True, unroll=1):
        def one(i, pend):
            p_i, q_i = place(i)
            p0, q0 = mul(p_i, T), mul(q_i, T)
            pend = (pend[0], pl.multiple_of(pend[1], T), pl.multiple_of(pend[2], T)) + tuple(pend[3:])
            tile(p_slot, p0, q_slot, q0, k_slot, pend, both)
            return tuple(jnp.int32(v) for v in (k_slot, p0, q0, v_p, acc_q, v_q, acc_p))

        def step(i, pend):
            for sub in range(unroll):
                pend = one(i * unroll + sub, pend)
            return pend

        return lax.fori_loop(0, count // unroll, step, pend)

    def flush(pend, both):
        products((pend[0], pl.multiple_of(pend[1], T), pl.multiple_of(pend[2], T)) + tuple(pend[3:]), both)

    nothing = tuple(jnp.int32(v) for v in (0, 0, 0, OWN, TRASH, OWN, TRASH))

    acc[...] = jnp.zeros_like(acc)
    acc2[...] = jnp.zeros_like(acc2)
    own_x.wait()
    own_v.wait()

    def norm_loop(slot):
        @pl.loop(0, rows // 256)
        def _(i):
            half_norms(slot, mul(i, 256), 256)

    norm_loop(OWN)
    side = rows // T
    pend = tiles(side * side, lambda i: (i // side, i % side), nothing, OWN, OWN, 0, OWN, OWN, OWN, TRASH, False, 4)

    sib_x.wait_recv()
    v_sib.wait_recv()
    norm_loop(CROSS)

    pend = tiles(side * side, lambda i: (i // side, i % side), pend, CROSS, OWN, 1, SIB, OWN, OWN, TRASH, False, 4)
    flush(pend, False)
    pl.semaphore_signal(free, inc=1, device_id={"row": sib}, device_id_type=pl.DeviceIdType.MESH)
    v_minus.wait_recv()
    v_plus.wait_recv()
    v_cross.start()
    pl.semaphore_wait(free, 1)
    v_cross.wait_recv()

    def stage(j, pend):
        start = mul(j, T)
        x_copy(0, j, start, T).wait_recv()
        forward(j, start, T).start()
        x_copy(1, j, start, T).wait_recv()
        half_norms(PLUS, start, T)
        half_norms(MINUS, start, T)
        pend = tiles(side, lambda i: (i, j), pend, OWN, PLUS, 2, OWN, PLUS, PLUS, OWN, True, 4)
        forward(j, start, T).wait_recv()
        half_norms(CROSS, start, T)
        pend = tiles(side, lambda i: (i, j), pend, OWN, CROSS, 3, OWN, CROSS, CROSS, OWN, True, 4)
        pend = tiles(1, lambda i: (j, j), pend, PLUS, far, 4, PLUS, far, far, PLUS)
        return tiles(2 * j, lambda i: (jnp.where(i % 2 == 0, i // 2, j), jnp.where(i % 2 == 0, j, i // 2)), pend,
                     PLUS, far, 4, PLUS, far, far, PLUS, True, 2)

    pend = lax.fori_loop(0, side, stage, nothing)
    flush(pend, True)

    def exchange(step, buf):
        for k in range(N_PIECE):
            to_plus, _, to_sib = part_copies(step, buf, k)
            to_sib.start()
            to_plus.start()
        for k in range(N_PIECE):
            cols = pl.ds(k * T, T)
            _, to_minus, to_sib = part_copies(step, buf, k)
            to_sib.wait_recv()
            buf[MINUS, :, cols] += rb[2, :, cols]
            to_minus.start()

    def arrived(step, buf, k):
        to_plus, to_minus, _ = part_copies(step, buf, k)
        to_plus.wait_recv()
        to_minus.wait_recv()

    def apply_nn(k_slot, y_slot, out, k):
        piece = pl.ds(mul(k, T), T)
        acc2[out] += dot_nn(yb[y_slot, :, piece], kb[k_slot, piece, :])

    def apply_nt(k_slot, y_slot, out, k):
        piece = pl.ds(mul(k, T), T)
        acc2[out] += dot_nt(yb[y_slot, :, piece], kb[k_slot, :, piece])

    exchange(0, acc)

    @pl.loop(0, N_PIECE)
    def _(k):
        piece = pl.ds(mul(k, T), T)
        arrived(0, acc, k)
        yb[OWN, :, piece] = (acc[OWN, :, piece] + rb[0, :, piece] + rb[1, :, piece]).astype(BF16)
        y_plus, y_minus, y_sib, _ = y_copies(k)
        y_plus.start()
        y_minus.start()
        y_sib.start()
        apply_nn(2, OWN, PLUS, k)
        apply_nn(3, OWN, CROSS, k)
        apply_nn(0, OWN, OWN, k)

    @pl.loop(0, N_PIECE)
    def _(k):
        y_plus, y_minus, y_sib, y_cross = y_copies(k)
        y_sib.wait_recv()
        apply_nn(1, SIB, OWN, k)

    @pl.loop(0, N_PIECE)
    def _(k):
        y_plus, y_minus, y_sib, y_cross = y_copies(k)
        y_plus.wait_recv()
        y_cross.start()
        y_minus.wait_recv()
        apply_nn(4, PLUS, far, k)
        y_cross.wait_recv()
        apply_nt(4, far, PLUS, k)

    exchange(1, acc2)

    @pl.loop(0, N_PIECE)
    def _(k):
        apply_nt(2, PLUS, OWN, k)
        apply_nt(3, CROSS, OWN, k)

    def out_copy(k):
        piece = pl.ds(k * T, T)
        return pltpu.make_async_copy(acc.at[OWN, :, piece], out_hbm.at[:, piece], loc.at[k])

    for k in range(N_PIECE):
        piece = pl.ds(k * T, T)
        arrived(1, acc2, k)
        acc[OWN, :, piece] = acc2[OWN, :, piece] + rb[0, :, piece] + rb[1, :, piece]
        out_copy(k).start()
    for copy in (v_plus, v_minus, v_sib, v_cross, sib_x):
        copy.wait_send()
    for k in range(N_PIECE):
        for copy in part_copies(0, acc, k) + part_copies(1, acc2, k) + y_copies(k):
            copy.wait_send()
        x_copy(0, *pieces[k]).wait_send()
        x_copy(1, *pieces[k]).wait_send()
        forward(*pieces[k]).wait_send()
        out_copy(k).wait()


def solution(mesh):
    n_row = mesh.shape["row"]
    assert n_row == 8

    def local_program(x_loc, v_loc, length_scale, out_scale):
        rows, feat = x_loc.shape
        cols = v_loc.shape[1]
        coef = jnp.stack([-LOG2E / (length_scale[0] * length_scale[0]), out_scale[0]]).reshape(1, 2)
        dma = pltpu.SemaphoreType.DMA
        out = pl.pallas_call(
            functools.partial(kernel, n_row),
            out_shape=jax.ShapeDtypeStruct((cols, rows), F32),
            in_specs=[pl.BlockSpec(memory_space=pl.ANY), pl.BlockSpec(memory_space=pl.ANY),
                      pl.BlockSpec(memory_space=pltpu.SMEM)],
            out_specs=pl.BlockSpec(memory_space=pl.ANY),
            scratch_shapes=[
                pltpu.VMEM((4, rows, feat), BF16),
                pltpu.VMEM((5, rows, rows), BF16),
                pltpu.VMEM((5, cols, rows), BF16),
                pltpu.VMEM((5, cols, rows), BF16),
                pltpu.VMEM((4, 1, rows), F32),
                pltpu.VMEM((5, cols, rows), F32),
                pltpu.VMEM((4, cols, rows), F32),
                pltpu.VMEM((3, cols, rows), F32),
                dma((2, N_PIECE)), dma((2, N_PIECE)), dma((N_PIECE,)), dma((N_PIECE,)),
                dma, dma, dma((N_PIECE,)), dma((4,)), dma((4,)), dma((4, N_PIECE)), dma((4, N_PIECE)),
                dma((2, 3, N_PIECE)), dma((2, 3, N_PIECE)), pltpu.SemaphoreType.REGULAR,
            ],
            compiler_params=pltpu.CompilerParams(
                collective_id=0, has_side_effects=True, vmem_limit_bytes=67043328),
        )(x_loc, v_loc.T, coef)
        return out.T

    row_spec = P(("task", "row"), None)
    return jax.shard_map(local_program, mesh=mesh, in_specs=(row_spec, row_spec, P("task"), P("task")),
                         out_specs=row_spec, check_vma=False)
```

```python
import functools

import jax
import jax.numpy as jnp
from jax import lax
from jax.experimental import pallas as pl
from jax.experimental.pallas import tpu as pltpu
from jax.sharding import PartitionSpec as P

F32 = jnp.float32
BF16 = jnp.bfloat16
LOG2E = 1.4426950408889634
OWN, PLUS, MINUS, CROSS, SIB = 0, 1, 2, 3, 4
N_SUM = 4
TRASH = 7
T = 512
N_PIECE = 4


def dot_nn(a, b):
    return lax.dot_general(a, b, (((1,), (0,)), ((), ())), preferred_element_type=F32)


def dot_nt(a, b):
    return lax.dot_general(a, b, (((1,), (1,)), ((), ())), preferred_element_type=F32)


def kernel(n_row, x_hbm, vt_hbm, length_scale, out_scale, out_hbm, xb, kb, vb, yb, hr, acc, rb,
           x_s, x_r, f_s, f_r, sib_s, sib_r, loc, v_s, v_r, y_s, y_r, p_s, p_r, free):
    rows = xb.shape[1]
    me = lax.axis_index("row")
    core = me % 2
    sib = me + 1 - 2 * core
    plus = (me + 2) % n_row
    minus = (me + n_row - 2) % n_row
    half_ring = n_row // 2

    def order(dev, j):
        flip = dev // half_ring
        return j + flip * (N_PIECE - 1 - 2 * j)

    def remote(src, dst, s_sem, r_sem, dev):
        return pltpu.make_async_remote_copy(
            src_ref=src, dst_ref=dst, send_sem=s_sem, recv_sem=r_sem,
            device_id={"row": dev}, device_id_type=pl.DeviceIdType.MESH)

    def x_send(direction, j):
        slot, dev = ((MINUS, plus), (PLUS, minus))[direction]
        piece = pl.ds(mul(order(dev, j), T), T)
        return remote(x_hbm.at[piece], xb.at[slot, piece], x_s.at[direction, j], x_r.at[direction, j], dev)

    def x_recv(direction, j):
        slot, dev = ((MINUS, plus), (PLUS, minus))[direction]
        piece = pl.ds(mul(order(me, j), T), T)
        return remote(x_hbm.at[piece], xb.at[slot, piece], x_s.at[direction, j], x_r.at[direction, j], dev)

    def forward(j):
        piece = pl.ds(mul(order(me, j), T), T)
        return remote(xb.at[MINUS, piece], xb.at[CROSS, piece], f_s.at[j], f_r.at[j], sib)

    def vec_copies(own, place, s_sem, r_sem):
        return (remote(own, place(MINUS), s_sem(0), r_sem(0), plus),
                remote(own, place(PLUS), s_sem(1), r_sem(1), minus),
                remote(own, place(SIB), s_sem(2), r_sem(2), sib),
                remote(place(MINUS), place(CROSS), s_sem(3), r_sem(3), sib))

    def y_ref(slot):
        return vb.at[slot] if slot in (OWN, SIB) else yb.at[slot - PLUS]

    def y_copies(k):
        piece = pl.ds(mul(k, T), T)
        return vec_copies(y_ref(OWN).at[:, piece], lambda slot: y_ref(slot).at[:, piece],
                          lambda d: y_s.at[d, k], lambda d: y_r.at[d, k])

    def part_copies(step, k):
        cols = pl.ds(mul(k, T), T)
        return tuple(remote(acc.at[step * N_SUM + slot, :, cols], rb.at[i, :, cols], p_s.at[step, i, k], p_r.at[step, i, k], dev)
                     for i, (slot, dev) in enumerate(((PLUS, plus), (MINUS, minus), (CROSS, sib))))

    def mul(i, size):
        return i * size if isinstance(i, int) else pl.multiple_of(i * size, size)

    barrier = pltpu.get_barrier_semaphore()
    for dev in (sib, plus, minus):
        pl.semaphore_signal(barrier, inc=1, device_id={"row": dev}, device_id_type=pl.DeviceIdType.MESH)
    pl.semaphore_wait(barrier, 3)

    own_x = pltpu.make_async_copy(x_hbm, xb.at[OWN], loc.at[0])
    own_v = pltpu.make_async_copy(vt_hbm, vb.at[OWN], loc.at[1])
    own_x.start()
    own_v.start()
    v_plus, v_minus, v_sib, v_cross = vec_copies(
        vt_hbm, lambda slot: vb.at[slot], lambda d: v_s.at[d], lambda d: v_r.at[d])
    sib_x = remote(x_hbm, xb.at[CROSS], sib_s, sib_r, sib)
    v_plus.start()
    v_minus.start()
    for j in range(N_PIECE):
        x_send(0, j).start()
        x_send(1, j).start()
    v_sib.start()
    sib_x.start()

    scale = jnp.full((8, 128), length_scale[0], F32)
    coef_d = (-LOG2E / (scale * scale))[0, 0]
    coef_s = out_scale[0]
    eye = (lax.broadcasted_iota(jnp.int32, (128, 128), 0) == lax.broadcasted_iota(jnp.int32, (128, 128), 1))

    def half_norms(slot, start, width):
        for sub in range(0, width, 128):
            x_sub = xb[slot, pl.ds(start + sub, 128), :].astype(F32)
            col = jnp.sum(x_sub * x_sub, axis=1, keepdims=True) * 0.5
            hr[slot, :, pl.ds(start + sub, 128)] = jnp.sum(jnp.where(eye, col, 0.0), axis=0, keepdims=True)

    def products(t, both):
        k_slot, k_row, k_col, p0, q0, v_p, v_q, acc_p, acc_q = t
        p_piece, q_piece = pl.ds(pl.multiple_of(p0, T), T), pl.ds(pl.multiple_of(q0, T), T)
        k_tile = kb[k_slot, pl.ds(pl.multiple_of(k_row, T), T), pl.ds(pl.multiple_of(k_col, T), T)]
        acc[acc_q, :, q_piece] += dot_nn(vb[v_p, :, p_piece], k_tile)
        if both:
            acc[acc_p, :, p_piece] += dot_nt(vb[v_q, :, q_piece], k_tile)

    def tile(p_slot, q_slot, t, pend, both):
        k_slot, k_row, k_col, p0, q0 = t[:5]
        k_row, k_col, p0, q0 = (pl.multiple_of(v, T) for v in (k_row, k_col, p0, q0))
        gram = dot_nt(xb[p_slot, pl.ds(p0, T), :], xb[q_slot, pl.ds(q0, T), :])
        products(pend, both)
        h_q = hr[q_slot, :, pl.ds(q0, T)]
        for sub in range(0, T, 128):
            h_row = hr[p_slot, :, pl.ds(p0 + sub, 128)]
            h_p = jnp.sum(jnp.where(eye, h_row, 0.0), axis=1, keepdims=True)
            half_d = jnp.maximum(h_p + h_q - gram[sub:sub + 128], 0.0)
            kb[k_slot, pl.ds(k_row + sub, 128), pl.ds(k_col, T)] = (coef_s * jnp.exp2(half_d * coef_d)).astype(BF16)

    def tiles(count, unroll, place, pend, both=True):
        def step(i, pend):
            for sub in range(unroll):
                p_slot, q_slot, t = place(i, sub)
                t = tuple(jnp.int32(v) for v in t)
                tile(p_slot, q_slot, t, pend, both)
                pend = t
            return pend

        return lax.fori_loop(0, count, step, pend)

    nothing = tuple(jnp.int32(v) for v in (0, 0, 0, 0, 0, OWN, OWN, TRASH, TRASH))

    acc[...] = jnp.zeros_like(acc)
    own_x.wait()
    own_v.wait()

    def norm_loop(slot):
        @pl.loop(0, rows // 256)
        def _(i):
            half_norms(slot, mul(i, 256), 256)

    norm_loop(OWN)
    side = rows // T
    pend = tiles(side, side, lambda i, sub: (OWN, OWN, (0, i * T, sub * T, i * T, sub * T, OWN, OWN, TRASH, OWN)), nothing, False)

    sib_x.wait_recv()
    v_sib.wait_recv()
    norm_loop(CROSS)

    pend = tiles(side, side, lambda i, sub: (CROSS, OWN, (1, i * T, sub * T, i * T, sub * T, SIB, OWN, TRASH, OWN)), pend, False)
    products(pend, False)
    pl.semaphore_signal(free, inc=1, device_id={"row": sib}, device_id_type=pl.DeviceIdType.MESH)
    v_minus.wait_recv()
    v_plus.wait_recv()
    v_cross.start()
    pl.semaphore_wait(free, 1)
    v_cross.wait_recv()

    def own_tiles(slot, j, pend):
        q0 = order(me, j) * T
        k_slot = 2 if slot == PLUS else 3
        return tiles(1, side, lambda i, sub: (OWN, slot, (k_slot, sub * T, q0, sub * T, q0, OWN, slot, OWN, slot)), pend)

    swap = me // half_ring

    def far_slots(which):
        other = MINUS + which
        return PLUS + swap * (other - PLUS), other + swap * (PLUS - other)

    def far_place(r, q, which):
        k_row = r + which * (N_PIECE - 1 - 2 * r)
        k_col = q + which * (N_PIECE - 1 - 2 * q)
        return k_row * T, k_col * T, order(me, r) * T, order(me, q) * T

    def far_tiles(count, j, pend):
        def place(i, which):
            r = jnp.where(i == 0, 0, jnp.where(i == 1, j, 1))
            q = jnp.where(i == 1, 0, j)
            p_slot, q_slot = far_slots(which)
            return p_slot, q_slot, (4,) + far_place(r, q, which) + (p_slot, q_slot, p_slot, q_slot)

        return tiles(count, 2, place, pend)

    def arrive(j):
        start = mul(order(me, j), T)
        x_recv(0, j).wait_recv()
        forward(j).start()
        x_recv(1, j).wait_recv()
        half_norms(PLUS, start, T)
        half_norms(MINUS, start, T)

    def arrive_cross(j):
        forward(j).wait_recv()
        half_norms(CROSS, mul(order(me, j), T), T)

    def stage(j, pend):
        arrive(j)
        pend = own_tiles(PLUS, j, pend)
        arrive_cross(j)
        pend = own_tiles(CROSS, j, pend)
        return far_tiles(jnp.where(j == 0, 1, 3), j, pend)

    def to_plus(step, j):
        return part_copies(step, order(me, j))[0]

    def to_minus(step, j):
        return part_copies(step, order(me, j))[1]

    def to_sib(step, j):
        return part_copies(step, order(me, j))[2]

    def combine(step, j):
        piece = pl.ds(mul(order(me, j), T), T)
        to_sib(step, j).wait_recv()
        acc[step * N_SUM + MINUS, :, piece] += rb[2, :, piece]
        to_minus(step, j).start()

    def arrived(step, k):
        for copy in part_copies(step, k)[:2]:
            copy.wait_recv()

    pend = lax.fori_loop(0, side - 1, stage, nothing)
    products(pend, True)
    for j in (1, 2):
        to_sib(0, j).start()
        to_plus(0, j).start()
    for j in (1, 2):
        combine(0, j)
    last = side - 1
    arrive(last)
    arrive_cross(last)
    pend = far_tiles(1, last, nothing)
    pend = own_tiles(CROSS, last, pend)
    to_sib(0, 0).start()
    to_plus(0, 0).start()
    pend = own_tiles(PLUS, last, pend)
    to_sib(0, last).start()
    combine(0, 0)
    products(pend, True)
    to_plus(0, last).start()
    combine(0, last)
    acc[pl.ds(N_SUM, N_SUM)] = jnp.zeros((N_SUM,) + acc.shape[1:], F32)

    def apply_nn(k_slot, y_slot, out, k):
        piece = pl.ds(mul(k, T), T)
        acc[N_SUM + out] += dot_nn(y_ref(y_slot)[:, piece], kb[k_slot, piece, :])

    def apply_nt(k_slot, y_slot, out, k):
        piece = pl.ds(mul(k, T), T)
        acc[N_SUM + out] += dot_nt(y_ref(y_slot)[:, piece], kb[k_slot, :, piece])

    def make_y(k):
        piece = pl.ds(mul(k, T), T)
        arrived(0, k)
        y_ref(OWN)[:, piece] = (acc[OWN, :, piece] + rb[0, :, piece] + rb[1, :, piece]).astype(BF16)

    def apply_own(k):
        apply_nn(2, OWN, PLUS, k)
        apply_nn(3, OWN, CROSS, k)
        apply_nn(0, OWN, OWN, k)

    @pl.loop(1, 3)
    def _(k):
        make_y(k)
        y_plus, y_minus, y_sib, _ = y_copies(k)
        y_plus.start()
        y_minus.start()
        y_sib.start()
        apply_own(k)

    first, final = order(minus, 0), order(minus, N_PIECE - 1)
    make_y(first)
    make_y(final)
    y_copies(first)[1].start()
    y_copies(final)[0].start()
    y_copies(final)[1].start()
    y_copies(first)[0].start()
    y_copies(first)[2].start()
    y_copies(final)[2].start()

    @pl.loop(0, 2)
    def _(i):
        apply_own(first + i * (final - first))


    @pl.loop(0, N_PIECE)
    def _(k):
        y_copies(k)[2].wait_recv()
        apply_nn(1, SIB, OWN, k)

    def far_products(group):
        for which in (0, 1):
            p_slot, q_slot = far_slots(which)

            def y_piece(slot, start):
                return yb[slot - PLUS, :, pl.ds(pl.multiple_of(start, T), T)]

            for q in sorted({q for _, q in group}):
                total = None
                for r in sorted({r for r, c in group if c == q}):
                    k_row, k_col, p0, q0 = far_place(r, q, which)
                    part = dot_nn(y_piece(p_slot, p0), kb[4, k_row:k_row + T, k_col:k_col + T])
                    total = part if total is None else total + part
                acc[N_SUM + q_slot, :, pl.ds(pl.multiple_of(q0, T), T)] += total
            for r in sorted({r for r, _ in group}):
                total = None
                for q in sorted({q for c, q in group if c == r}):
                    k_row, k_col, p0, q0 = far_place(r, q, which)
                    part = dot_nt(y_piece(q_slot, q0), kb[4, k_row:k_row + T, k_col:k_col + T])
                    total = part if total is None else total + part
                acc[N_SUM + p_slot, :, pl.ds(pl.multiple_of(p0, T), T)] += total

    def y_arrive(js):
        for j in js:
            y_copies(order(me, j))[0].wait_recv()
            y_copies(order(me, j))[3].start()
        for j in js:
            y_copies(order(me, j))[1].wait_recv()
            y_copies(order(me, j))[3].wait_recv()

    y_arrive((1, 2))
    far_products(((1, 1), (1, 2)))
    y_arrive((0,))
    far_products(((0, 0), (0, 1), (1, 0), (0, 2), (2, 0)))
    for j in (1, 2):
        to_sib(1, j).start()
        to_plus(1, j).start()
    for j in (1, 2):
        combine(1, j)
    y_arrive((last,))
    far_products(((0, last),))
    for j in (0, last):
        to_sib(1, j).start()
        to_plus(1, j).start()
    for j in (0, last):
        combine(1, j)

    @pl.loop(0, N_PIECE)
    def _(k):
        apply_nt(2, PLUS, OWN, k)
        apply_nt(3, CROSS, OWN, k)

    def out_copy(k):
        piece = pl.ds(mul(k, T), T)
        return pltpu.make_async_copy(acc.at[OWN, :, piece], out_hbm.at[:, piece], loc.at[k])

    for k in (1, 2, first, final):
        piece = pl.ds(mul(k, T), T)
        arrived(1, k)
        acc[OWN, :, piece] = acc[N_SUM + OWN, :, piece] + rb[0, :, piece] + rb[1, :, piece]
        out_copy(k).start()
    for copy in (v_plus, v_minus, v_sib, v_cross, sib_x):
        copy.wait_send()
    for k in range(N_PIECE):
        for copy in part_copies(0, k) + part_copies(1, k) + y_copies(k):
            copy.wait_send()
        x_send(0, k).wait_send()
        x_send(1, k).wait_send()
        forward(k).wait_send()
        out_copy(k).wait()


def solution(mesh):
    n_row = mesh.shape["row"]
    assert n_row == 8

    def local_program(x_loc, v_loc, length_scale, out_scale):
        rows, feat = x_loc.shape
        cols = v_loc.shape[1]
        dma = pltpu.SemaphoreType.DMA
        out = pl.pallas_call(
            functools.partial(kernel, n_row),
            out_shape=jax.ShapeDtypeStruct((cols, rows), F32),
            in_specs=[pl.BlockSpec(memory_space=pl.ANY), pl.BlockSpec(memory_space=pl.ANY),
                      pl.BlockSpec(memory_space=pltpu.SMEM), pl.BlockSpec(memory_space=pltpu.SMEM)],
            out_specs=pl.BlockSpec(memory_space=pl.ANY),
            scratch_shapes=[
                pltpu.VMEM((4, rows, feat), BF16),
                pltpu.VMEM((5, rows, rows), BF16),
                pltpu.VMEM((5, cols, rows), BF16),
                pltpu.VMEM((3, cols, rows), BF16),
                pltpu.VMEM((4, 1, rows), F32),
                pltpu.VMEM((2 * N_SUM, cols, rows), F32),
                pltpu.VMEM((3, cols, rows), F32),
                dma((2, N_PIECE)), dma((2, N_PIECE)), dma((N_PIECE,)), dma((N_PIECE,)),
                dma, dma, dma((N_PIECE,)), dma((4,)), dma((4,)), dma((4, N_PIECE)), dma((4, N_PIECE)),
                dma((2, 3, N_PIECE)), dma((2, 3, N_PIECE)), pltpu.SemaphoreType.REGULAR,
            ],
            compiler_params=pltpu.CompilerParams(
                collective_id=0, has_side_effects=True, vmem_limit_bytes=67043328),
        )(x_loc, v_loc.T, length_scale, out_scale)
        return out.T

    row_spec = P(("task", "row"), None)
    return jax.shard_map(local_program, mesh=mesh, in_specs=(row_spec, row_spec, P("task"), P("task")),
                         out_specs=row_spec, check_vma=False)
```

```python
import functools

import jax
import jax.numpy as jnp
from jax import lax
from jax.experimental import pallas as pl
from jax.experimental.pallas import tpu as pltpu
from jax.sharding import PartitionSpec as P

F32 = jnp.float32
BF16 = jnp.bfloat16
LOG2E = 1.4426950408889634
OWN, PLUS, MINUS, CROSS, SIB = 0, 1, 2, 3, 4
N_SUM = 4
TRASH = 7
T = 512
N_PIECE = 4


def dot_nn(a, b):
    return lax.dot_general(a, b, (((1,), (0,)), ((), ())), preferred_element_type=F32)


def dot_nt(a, b):
    return lax.dot_general(a, b, (((1,), (1,)), ((), ())), preferred_element_type=F32)


def kernel(n_row, x_hbm, vt_hbm, length_scale, out_scale, out_hbm, xb, kb, vb, yb, hr, acc, rb,
           x_s, x_r, f_s, f_r, sib_s, sib_r, loc, v_s, v_r, y_s, y_r, p_s, p_r, free):
    rows = xb.shape[1]
    me = lax.axis_index("row")
    core = me % 2
    sib = me + 1 - 2 * core
    plus = (me + 2) % n_row
    minus = (me + n_row - 2) % n_row
    half_ring = n_row // 2

    def order(dev, j):
        flip = dev // half_ring
        return j + flip * (N_PIECE - 1 - 2 * j)

    def remote(src, dst, s_sem, r_sem, dev):
        return pltpu.make_async_remote_copy(
            src_ref=src, dst_ref=dst, send_sem=s_sem, recv_sem=r_sem,
            device_id={"row": dev}, device_id_type=pl.DeviceIdType.MESH)

    def x_send(direction, j):
        slot, dev = ((MINUS, plus), (PLUS, minus))[direction]
        piece = pl.ds(mul(order(dev, j), T), T)
        return remote(x_hbm.at[piece], xb.at[slot, piece], x_s.at[direction, j], x_r.at[direction, j], dev)

    def x_recv(direction, j):
        slot, dev = ((MINUS, plus), (PLUS, minus))[direction]
        piece = pl.ds(mul(order(me, j), T), T)
        return remote(x_hbm.at[piece], xb.at[slot, piece], x_s.at[direction, j], x_r.at[direction, j], dev)

    def forward(j):
        piece = pl.ds(mul(order(me, j), T), T)
        return remote(xb.at[MINUS, piece], xb.at[CROSS, piece], f_s.at[j], f_r.at[j], sib)

    def vec_copies(own, place, s_sem, r_sem):
        return (remote(own, place(MINUS), s_sem(0), r_sem(0), plus),
                remote(own, place(PLUS), s_sem(1), r_sem(1), minus),
                remote(own, place(SIB), s_sem(2), r_sem(2), sib),
                remote(place(MINUS), place(CROSS), s_sem(3), r_sem(3), sib))

    def y_ref(slot):
        return vb.at[slot] if slot in (OWN, SIB) else yb.at[slot - PLUS]

    def y_copies(k):
        piece = pl.ds(mul(k, T), T)
        return vec_copies(y_ref(OWN).at[:, piece], lambda slot: y_ref(slot).at[:, piece],
                          lambda d: y_s.at[d, k], lambda d: y_r.at[d, k])

    def part_copies(step, k):
        cols = pl.ds(mul(k, T), T)
        return tuple(remote(acc.at[step * N_SUM + slot, :, cols], rb.at[i, :, cols], p_s.at[step, i, k], p_r.at[step, i, k], dev)
                     for i, (slot, dev) in enumerate(((PLUS, plus), (MINUS, minus), (CROSS, sib))))

    def mul(i, size):
        return i * size if isinstance(i, int) else pl.multiple_of(i * size, size)

    barrier = pltpu.get_barrier_semaphore()
    for dev in (sib, plus, minus):
        pl.semaphore_signal(barrier, inc=1, device_id={"row": dev}, device_id_type=pl.DeviceIdType.MESH)
    pl.semaphore_wait(barrier, 3)

    own_x = pltpu.make_async_copy(x_hbm, xb.at[OWN], loc.at[0])
    own_v = pltpu.make_async_copy(vt_hbm, vb.at[OWN], loc.at[1])
    own_x.start()
    own_v.start()
    v_plus, v_minus, v_sib, v_cross = vec_copies(
        vt_hbm, lambda slot: vb.at[slot], lambda d: v_s.at[d], lambda d: v_r.at[d])
    sib_x = remote(x_hbm, xb.at[CROSS], sib_s, sib_r, sib)
    v_plus.start()
    v_minus.start()
    for j in range(N_PIECE):
        x_send(0, j).start()
        x_send(1, j).start()
    v_sib.start()
    sib_x.start()

    scale = jnp.full((8, 128), length_scale[0], F32)
    coef_d = (-LOG2E / (scale * scale))[0, 0]
    coef_s = out_scale[0]
    eye = (lax.broadcasted_iota(jnp.int32, (128, 128), 0) == lax.broadcasted_iota(jnp.int32, (128, 128), 1))

    def half_norms(slot, start, width):
        for sub in range(0, width, 128):
            x_sub = xb[slot, pl.ds(start + sub, 128), :].astype(F32)
            col = jnp.sum(x_sub * x_sub, axis=1, keepdims=True) * 0.5
            hr[slot, :, pl.ds(start + sub, 128)] = jnp.sum(jnp.where(eye, col, 0.0), axis=0, keepdims=True)

    def products(t, both):
        k_slot, k_row, k_col, p0, q0, v_p, v_q, acc_p, acc_q = t
        p_piece, q_piece = pl.ds(pl.multiple_of(p0, T), T), pl.ds(pl.multiple_of(q0, T), T)
        k_tile = kb[k_slot, pl.ds(pl.multiple_of(k_row, T), T), pl.ds(pl.multiple_of(k_col, T), T)]
        yield
        acc[acc_q, :, q_piece] += dot_nn(vb[v_p, :, p_piece], k_tile)
        yield
        if both:
            acc[acc_p, :, p_piece] += dot_nt(vb[v_q, :, q_piece], k_tile)
        yield

    def flush(pend, both):
        for _ in products(pend, both):
            pass

    def tile(p_slot, q_slot, t, pend, both):
        k_slot, k_row, k_col, p0, q0 = t[:5]
        k_row, k_col, p0, q0 = (pl.multiple_of(v, T) for v in (k_row, k_col, p0, q0))
        pending = products(pend, both)
        gram = None
        for f in range(0, xb.shape[2], 256):
            part = dot_nt(xb[p_slot, pl.ds(p0, T), pl.ds(f, 256)], xb[q_slot, pl.ds(q0, T), pl.ds(f, 256)])
            gram = part if gram is None else gram + part
            next(pending)
        h_q = hr[q_slot, :, pl.ds(q0, T)]
        for sub in range(0, T, 128):
            h_row = hr[p_slot, :, pl.ds(p0 + sub, 128)]
            h_p = jnp.sum(jnp.where(eye, h_row, 0.0), axis=1, keepdims=True)
            half_d = jnp.maximum(h_p + h_q - gram[sub:sub + 128], 0.0)
            kb[k_slot, pl.ds(k_row + sub, 128), pl.ds(k_col, T)] = (coef_s * jnp.exp2(half_d * coef_d)).astype(BF16)

    def tiles(count, unroll, place, pend, both=True):
        def step(i, pend):
            for sub in range(unroll):
                p_slot, q_slot, t = place(i, sub)
                t = tuple(jnp.int32(v) for v in t)
                tile(p_slot, q_slot, t, pend, both)
                pend = t
            return pend

        return lax.fori_loop(0, count, step, pend)

    nothing = tuple(jnp.int32(v) for v in (0, 0, 0, 0, 0, OWN, OWN, TRASH, TRASH))

    acc[...] = jnp.zeros_like(acc)
    own_x.wait()
    own_v.wait()

    def norm_loop(slot):
        @pl.loop(0, rows // 256)
        def _(i):
            half_norms(slot, mul(i, 256), 256)

    norm_loop(OWN)
    side = rows // T
    pend = tiles(side, side, lambda i, sub: (OWN, OWN, (0, i * T, sub * T, i * T, sub * T, OWN, OWN, TRASH, OWN)), nothing, False)

    sib_x.wait_recv()
    v_sib.wait_recv()
    norm_loop(CROSS)

    pend = tiles(side, side, lambda i, sub: (CROSS, OWN, (1, i * T, sub * T, i * T, sub * T, SIB, OWN, TRASH, OWN)), pend, False)
    flush(pend, False)
    pl.semaphore_signal(free, inc=1, device_id={"row": sib}, device_id_type=pl.DeviceIdType.MESH)
    v_minus.wait_recv()
    v_plus.wait_recv()
    v_cross.start()
    pl.semaphore_wait(free, 1)
    v_cross.wait_recv()

    def own_tiles(slot, j, pend, begin=0, end=side):
        q0 = order(me, j) * T
        k_slot = 2 if slot == PLUS else 3

        def place(i, sub):
            p0 = (begin + sub) * T
            return OWN, slot, (k_slot, p0, q0, p0, q0, OWN, slot, OWN, slot)

        return tiles(1, end - begin, place, pend)

    swap = me // half_ring

    def far_slots(which):
        other = MINUS + which
        return PLUS + swap * (other - PLUS), other + swap * (PLUS - other)

    def far_place(r, q, which):
        k_row = r + which * (N_PIECE - 1 - 2 * r)
        k_col = q + which * (N_PIECE - 1 - 2 * q)
        return k_row * T, k_col * T, order(me, r) * T, order(me, q) * T

    def far_tiles(count, j, pend):
        def place(i, which):
            r = jnp.where(i == 0, 0, jnp.where(i == 1, j, 1))
            q = jnp.where(i == 1, 0, j)
            p_slot, q_slot = far_slots(which)
            return p_slot, q_slot, (4,) + far_place(r, q, which) + (p_slot, q_slot, p_slot, q_slot)

        return tiles(count, 2, place, pend)

    def arrive(j):
        start = mul(order(me, j), T)
        x_recv(0, j).wait_recv()
        forward(j).start()
        x_recv(1, j).wait_recv()
        half_norms(PLUS, start, T)
        half_norms(MINUS, start, T)

    def arrive_cross(j):
        forward(j).wait_recv()
        half_norms(CROSS, mul(order(me, j), T), T)

    def stage(j, pend):
        arrive(j)
        pend = own_tiles(PLUS, j, pend)
        arrive_cross(j)
        pend = own_tiles(CROSS, j, pend)
        return far_tiles(jnp.where(j == 0, 1, 3), j, pend)

    def to_plus(step, j):
        return part_copies(step, order(me, j))[0]

    def to_minus(step, j):
        return part_copies(step, order(me, j))[1]

    def to_sib(step, j):
        return part_copies(step, order(me, j))[2]

    def combine(step, j):
        piece = pl.ds(mul(order(me, j), T), T)
        to_sib(step, j).wait_recv()
        acc[step * N_SUM + MINUS, :, piece] += rb[2, :, piece]
        to_minus(step, j).start()

    def arrived(step, k):
        for copy in part_copies(step, k)[:2]:
            copy.wait_recv()

    pend = lax.fori_loop(0, side - 1, stage, nothing)
    flush(pend, True)
    for j in (1, 2):
        to_sib(0, j).start()
        to_plus(0, j).start()
    for j in (1, 2):
        combine(0, j)
    last = side - 1
    arrive(last)
    pend = own_tiles(PLUS, last, nothing, 0, side // 2)
    arrive_cross(last)
    pend = far_tiles(1, last, pend)
    flush(pend, True)
    to_sib(0, 0).start()
    to_plus(0, 0).start()
    pend = own_tiles(CROSS, last, nothing)
    flush(pend, True)
    to_sib(0, last).start()
    combine(0, 0)
    pend = own_tiles(PLUS, last, nothing, side // 2)
    flush(pend, True)
    to_plus(0, last).start()
    combine(0, last)
    acc[pl.ds(N_SUM, N_SUM)] = jnp.zeros((N_SUM,) + acc.shape[1:], F32)

    def apply_nn(k_slot, y_slot, out, k):
        piece = pl.ds(mul(k, T), T)
        acc[N_SUM + out] += dot_nn(y_ref(y_slot)[:, piece], kb[k_slot, piece, :])

    def apply_nt(k_slot, y_slot, out, k):
        piece = pl.ds(mul(k, T), T)
        acc[N_SUM + out] += dot_nt(y_ref(y_slot)[:, piece], kb[k_slot, :, piece])

    def make_y(k):
        piece = pl.ds(mul(k, T), T)
        arrived(0, k)
        y_ref(OWN)[:, piece] = (acc[OWN, :, piece] + rb[0, :, piece] + rb[1, :, piece]).astype(BF16)

    def apply_own(k):
        apply_nn(2, OWN, PLUS, k)
        apply_nn(3, OWN, CROSS, k)
        apply_nn(0, OWN, OWN, k)

    @pl.loop(1, 3)
    def _(k):
        make_y(k)
        y_plus, y_minus, y_sib, _ = y_copies(k)
        y_plus.start()
        y_minus.start()
        y_sib.start()
        apply_own(k)

    first, final = order(minus, 0), order(minus, N_PIECE - 1)
    make_y(first)
    make_y(final)
    y_copies(first)[1].start()
    y_copies(final)[0].start()
    y_copies(final)[1].start()
    y_copies(first)[0].start()
    y_copies(first)[2].start()
    y_copies(final)[2].start()

    @pl.loop(0, 2)
    def _(i):
        apply_own(first + i * (final - first))


    @pl.loop(0, N_PIECE)
    def _(k):
        y_copies(k)[2].wait_recv()
        apply_nn(1, SIB, OWN, k)

    def far_products(group_nn, group_nt):
        for which in (0, 1):
            p_slot, q_slot = far_slots(which)

            def y_piece(slot, start):
                return yb[slot - PLUS, :, pl.ds(pl.multiple_of(start, T), T)]

            for q in sorted({q for _, q in group_nn}):
                total = None
                for r in sorted({r for r, c in group_nn if c == q}):
                    k_row, k_col, p0, q0 = far_place(r, q, which)
                    part = dot_nn(y_piece(p_slot, p0), kb[4, k_row:k_row + T, k_col:k_col + T])
                    total = part if total is None else total + part
                acc[N_SUM + q_slot, :, pl.ds(pl.multiple_of(q0, T), T)] += total
            for r in sorted({r for r, _ in group_nt}):
                total = None
                for q in sorted({q for c, q in group_nt if c == r}):
                    k_row, k_col, p0, q0 = far_place(r, q, which)
                    part = dot_nt(y_piece(q_slot, q0), kb[4, k_row:k_row + T, k_col:k_col + T])
                    total = part if total is None else total + part
                acc[N_SUM + p_slot, :, pl.ds(pl.multiple_of(p0, T), T)] += total

    def y_arrive(js):
        for j in js:
            y_copies(order(me, j))[0].wait_recv()
            y_copies(order(me, j))[3].start()
        for j in js:
            y_copies(order(me, j))[1].wait_recv()
            y_copies(order(me, j))[3].wait_recv()

    y_arrive((1, 2))
    far_products(((1, 1), (1, 2)), ((1, 1), (1, 2)))
    y_arrive((0,))
    far_products(((0, 1), (0, 2)), ((1, 0), (2, 0)))
    for j in (1, 2):
        to_sib(1, j).start()
        to_plus(1, j).start()
    far_products(((0, 0), (1, 0), (2, 0)), ((0, 0), (0, 1), (0, 2)))
    for j in (1, 2):
        combine(1, j)
    y_arrive((last,))
    far_products(((0, last),), ((0, last),))
    for j in (0, last):
        to_sib(1, j).start()
        to_plus(1, j).start()
    apply_nt(2, PLUS, OWN, 0)
    apply_nt(3, CROSS, OWN, 0)
    for j in (0, last):
        combine(1, j)

    @pl.loop(1, N_PIECE)
    def _(k):
        apply_nt(2, PLUS, OWN, k)
        apply_nt(3, CROSS, OWN, k)

    def out_copy(k):
        piece = pl.ds(mul(k, T), T)
        return pltpu.make_async_copy(acc.at[OWN, :, piece], out_hbm.at[:, piece], loc.at[k])

    for k in (1, 2, first, final):
        piece = pl.ds(mul(k, T), T)
        arrived(1, k)
        acc[OWN, :, piece] = acc[N_SUM + OWN, :, piece] + rb[0, :, piece] + rb[1, :, piece]
        out_copy(k).start()
    for copy in (v_plus, v_minus, v_sib, v_cross, sib_x):
        copy.wait_send()
    for k in range(N_PIECE):
        for copy in part_copies(0, k) + part_copies(1, k) + y_copies(k):
            copy.wait_send()
        x_send(0, k).wait_send()
        x_send(1, k).wait_send()
        forward(k).wait_send()
        out_copy(k).wait()


def solution(mesh):
    n_row = mesh.shape["row"]
    assert n_row == 8

    def local_program(x_loc, v_loc, length_scale, out_scale):
        rows, feat = x_loc.shape
        cols = v_loc.shape[1]
        dma = pltpu.SemaphoreType.DMA
        out = pl.pallas_call(
            functools.partial(kernel, n_row),
            out_shape=jax.ShapeDtypeStruct((cols, rows), F32),
            in_specs=[pl.BlockSpec(memory_space=pl.ANY), pl.BlockSpec(memory_space=pl.ANY),
                      pl.BlockSpec(memory_space=pltpu.SMEM), pl.BlockSpec(memory_space=pltpu.SMEM)],
            out_specs=pl.BlockSpec(memory_space=pl.ANY),
            scratch_shapes=[
                pltpu.VMEM((4, rows, feat), BF16),
                pltpu.VMEM((5, rows, rows), BF16),
                pltpu.VMEM((5, cols, rows), BF16),
                pltpu.VMEM((3, cols, rows), BF16),
                pltpu.VMEM((4, 1, rows), F32),
                pltpu.VMEM((2 * N_SUM, cols, rows), F32),
                pltpu.VMEM((3, cols, rows), F32),
                dma((2, N_PIECE)), dma((2, N_PIECE)), dma((N_PIECE,)), dma((N_PIECE,)),
                dma, dma, dma((N_PIECE,)), dma((4,)), dma((4,)), dma((4, N_PIECE)), dma((4, N_PIECE)),
                dma((2, 3, N_PIECE)), dma((2, 3, N_PIECE)), pltpu.SemaphoreType.REGULAR,
            ],
            compiler_params=pltpu.CompilerParams(
                collective_id=0, has_side_effects=True, vmem_limit_bytes=67043328),
        )(x_loc, v_loc.T, length_scale, out_scale)
        return out.T

    row_spec = P(("task", "row"), None)
    return jax.shard_map(local_program, mesh=mesh, in_specs=(row_spec, row_spec, P("task"), P("task")),
                         out_specs=row_spec, check_vma=False)
```

```python
import functools

import jax
import jax.numpy as jnp
from jax import lax
from jax.experimental import pallas as pl
from jax.experimental.pallas import tpu as pltpu
from jax.sharding import PartitionSpec as P

F32 = jnp.float32
BF16 = jnp.bfloat16
LOG2E = 1.4426950408889634
OWN, PLUS, MINUS, CROSS, SIB = 0, 1, 2, 3, 4
N_SUM = 4
TRASH = 7
T = 512
N_PIECE = 4


def dot_nn(a, b):
    return lax.dot_general(a, b, (((1,), (0,)), ((), ())), preferred_element_type=F32)


def dot_nt(a, b):
    return lax.dot_general(a, b, (((1,), (1,)), ((), ())), preferred_element_type=F32)


def kernel(n_row, x_hbm, vt_hbm, length_scale, out_scale, out_hbm, xb, kb, vb, yb, hr, acc, rb,
           x_s, x_r, f_s, f_r, sib_s, sib_r, loc, v_s, v_r, y_s, y_r, p_s, p_r, free):
    rows = xb.shape[1]
    me = lax.axis_index("row")
    core = me % 2
    sib = me + 1 - 2 * core
    plus = (me + 2) % n_row
    minus = (me + n_row - 2) % n_row
    half_ring = n_row // 2

    def order(dev, j):
        flip = dev // half_ring
        return j + flip * (N_PIECE - 1 - 2 * j)

    def remote(src, dst, s_sem, r_sem, dev):
        return pltpu.make_async_remote_copy(
            src_ref=src, dst_ref=dst, send_sem=s_sem, recv_sem=r_sem,
            device_id={"row": dev}, device_id_type=pl.DeviceIdType.MESH)

    def x_send(direction, j):
        slot, dev = ((MINUS, plus), (PLUS, minus))[direction]
        piece = pl.ds(mul(order(dev, j), T), T)
        return remote(x_hbm.at[piece], xb.at[slot, piece], x_s.at[direction, j], x_r.at[direction, j], dev)

    def x_recv(direction, j):
        slot, dev = ((MINUS, plus), (PLUS, minus))[direction]
        piece = pl.ds(mul(order(me, j), T), T)
        return remote(x_hbm.at[piece], xb.at[slot, piece], x_s.at[direction, j], x_r.at[direction, j], dev)

    def forward(j):
        piece = pl.ds(mul(order(me, j), T), T)
        return remote(xb.at[MINUS, piece], xb.at[CROSS, piece], f_s.at[j], f_r.at[j], sib)

    def vec_copies(own, place, s_sem, r_sem):
        return (remote(own, place(MINUS), s_sem(0), r_sem(0), plus),
                remote(own, place(PLUS), s_sem(1), r_sem(1), minus),
                remote(own, place(SIB), s_sem(2), r_sem(2), sib),
                remote(place(MINUS), place(CROSS), s_sem(3), r_sem(3), sib))

    def y_ref(slot):
        return vb.at[slot] if slot in (OWN, SIB) else yb.at[slot - PLUS]

    def y_copies(k):
        piece = pl.ds(mul(k, T), T)
        return vec_copies(y_ref(OWN).at[:, piece], lambda slot: y_ref(slot).at[:, piece],
                          lambda d: y_s.at[d, k], lambda d: y_r.at[d, k])

    def part_copies(step, k):
        cols = pl.ds(mul(k, T), T)
        return tuple(remote(acc.at[step * N_SUM + slot, :, cols], rb.at[i, :, cols], p_s.at[step, i, k], p_r.at[step, i, k], dev)
                     for i, (slot, dev) in enumerate(((PLUS, plus), (MINUS, minus), (CROSS, sib))))

    def mul(i, size):
        return i * size if isinstance(i, int) else pl.multiple_of(i * size, size)

    barrier = pltpu.get_barrier_semaphore()
    for dev in (sib, plus, minus):
        pl.semaphore_signal(barrier, inc=1, device_id={"row": dev}, device_id_type=pl.DeviceIdType.MESH)
    pl.semaphore_wait(barrier, 3)

    own_x = pltpu.make_async_copy(x_hbm, xb.at[OWN], loc.at[0])
    own_v = pltpu.make_async_copy(vt_hbm, vb.at[OWN], loc.at[1])
    own_x.start()
    own_v.start()
    v_plus, v_minus, v_sib, v_cross = vec_copies(
        vt_hbm, lambda slot: vb.at[slot], lambda d: v_s.at[d], lambda d: v_r.at[d])
    sib_x = remote(x_hbm, xb.at[CROSS], sib_s, sib_r, sib)
    v_plus.start()
    v_minus.start()
    for j in range(N_PIECE):
        x_send(0, j).start()
        x_send(1, j).start()
    v_sib.start()
    sib_x.start()

    scale = jnp.full((8, 128), length_scale[0], F32)
    coef_d = (-LOG2E / (scale * scale))[0, 0]
    coef_s = out_scale[0]
    eye = (lax.broadcasted_iota(jnp.int32, (128, 128), 0) == lax.broadcasted_iota(jnp.int32, (128, 128), 1))

    def half_norms(slot, start, width):
        for sub in range(0, width, 128):
            x_sub = xb[slot, pl.ds(start + sub, 128), :].astype(F32)
            col = jnp.sum(x_sub * x_sub, axis=1, keepdims=True) * 0.5
            hr[slot, :, pl.ds(start + sub, 128)] = jnp.sum(jnp.where(eye, col, 0.0), axis=0, keepdims=True)

    def products(t, both):
        k_slot, k_row, k_col, p0, q0, v_p, v_q, acc_p, acc_q = t
        p_piece, q_piece = pl.ds(pl.multiple_of(p0, T), T), pl.ds(pl.multiple_of(q0, T), T)
        k_tile = kb[k_slot, pl.ds(pl.multiple_of(k_row, T), T), pl.ds(pl.multiple_of(k_col, T), T)]
        yield
        acc[acc_q, :, q_piece] += dot_nn(vb[v_p, :, p_piece], k_tile)
        yield
        if both:
            acc[acc_p, :, p_piece] += dot_nt(vb[v_q, :, q_piece], k_tile)
        yield

    def flush(pend, both):
        for _ in products(pend, both):
            pass

    def tile(p_slot, q_slot, t, pend, both):
        k_slot, k_row, k_col, p0, q0 = t[:5]
        k_row, k_col, p0, q0 = (pl.multiple_of(v, T) for v in (k_row, k_col, p0, q0))
        pending = products(pend, both)
        gram = None
        for f in range(0, xb.shape[2], 256):
            part = dot_nt(xb[p_slot, pl.ds(p0, T), pl.ds(f, 256)], xb[q_slot, pl.ds(q0, T), pl.ds(f, 256)])
            gram = part if gram is None else gram + part
            next(pending)
        h_q = hr[q_slot, :, pl.ds(q0, T)]
        for sub in range(0, T, 128):
            h_row = hr[p_slot, :, pl.ds(p0 + sub, 128)]
            h_p = jnp.sum(jnp.where(eye, h_row, 0.0), axis=1, keepdims=True)
            half_d = jnp.maximum(h_p + h_q - gram[sub:sub + 128], 0.0)
            kb[k_slot, pl.ds(k_row + sub, 128), pl.ds(k_col, T)] = (coef_s * jnp.exp2(half_d * coef_d)).astype(BF16)

    def tiles(count, unroll, place, pend, both=True):
        def step(i, pend):
            for sub in range(unroll):
                p_slot, q_slot, t = place(i, sub)
                t = tuple(jnp.int32(v) for v in t)
                tile(p_slot, q_slot, t, pend, both)
                pend = t
            return pend

        return lax.fori_loop(0, count, step, pend)

    nothing = tuple(jnp.int32(v) for v in (0, 0, 0, 0, 0, OWN, OWN, TRASH, TRASH))

    acc[...] = jnp.zeros_like(acc)
    own_x.wait()
    own_v.wait()

    def norm_loop(slot):
        @pl.loop(0, rows // 256)
        def _(i):
            half_norms(slot, mul(i, 256), 256)

    norm_loop(OWN)
    side = rows // T
    pend = tiles(side, side, lambda i, sub: (OWN, OWN, (0, i * T, sub * T, i * T, sub * T, OWN, OWN, TRASH, OWN)), nothing, False)

    sib_x.wait_recv()
    v_sib.wait_recv()
    norm_loop(CROSS)

    pend = tiles(side, side, lambda i, sub: (CROSS, OWN, (1, i * T, sub * T, i * T, sub * T, SIB, OWN, TRASH, OWN)), pend, False)
    flush(pend, False)
    pl.semaphore_signal(free, inc=1, device_id={"row": sib}, device_id_type=pl.DeviceIdType.MESH)
    v_minus.wait_recv()
    v_plus.wait_recv()
    v_cross.start()
    pl.semaphore_wait(free, 1)
    v_cross.wait_recv()

    def own_tiles(slot, j, pend, begin=0, end=side, both=True):
        q0 = order(me, j) * T
        k_slot = 2 if slot == PLUS else 3

        def place(i, sub):
            p0 = (begin + sub) * T
            return OWN, slot, (k_slot, p0, q0, p0, q0, OWN, slot, OWN, slot)

        return tiles(1, end - begin, place, pend, both)

    swap = me // half_ring

    def far_slots(which):
        other = MINUS + which
        return PLUS + swap * (other - PLUS), other + swap * (PLUS - other)

    def far_place(r, q, which):
        k_row = r + which * (N_PIECE - 1 - 2 * r)
        k_col = q + which * (N_PIECE - 1 - 2 * q)
        return k_row * T, k_col * T, order(me, r) * T, order(me, q) * T

    def far_tiles(count, j, pend):
        def place(i, which):
            r = jnp.where(i == 0, 0, jnp.where(i == 1, j, 1))
            q = jnp.where(i == 1, 0, j)
            p_slot, q_slot = far_slots(which)
            return p_slot, q_slot, (4,) + far_place(r, q, which) + (p_slot, q_slot, p_slot, q_slot)

        return tiles(count, 2, place, pend)

    def arrive(j):
        start = mul(order(me, j), T)
        x_recv(0, j).wait_recv()
        forward(j).start()
        x_recv(1, j).wait_recv()
        half_norms(PLUS, start, T)
        half_norms(MINUS, start, T)

    def arrive_cross(j):
        forward(j).wait_recv()
        half_norms(CROSS, mul(order(me, j), T), T)

    def stage(j, pend):
        arrive(j)
        pend = own_tiles(PLUS, j, pend)
        arrive_cross(j)
        pend = own_tiles(CROSS, j, pend)
        return far_tiles(jnp.where(j == 0, 1, 3), j, pend)

    def to_plus(step, j):
        return part_copies(step, order(me, j))[0]

    def to_minus(step, j):
        return part_copies(step, order(me, j))[1]

    def to_sib(step, j):
        return part_copies(step, order(me, j))[2]

    def combine(step, j):
        piece = pl.ds(mul(order(me, j), T), T)
        to_sib(step, j).wait_recv()
        acc[step * N_SUM + MINUS, :, piece] += rb[2, :, piece]
        to_minus(step, j).start()

    def arrived(step, k):
        for copy in part_copies(step, k)[:2]:
            copy.wait_recv()

    pend = lax.fori_loop(0, side - 1, stage, nothing)
    flush(pend, True)
    for j in (1, 2):
        to_sib(0, j).start()
        to_plus(0, j).start()
    for j in (1, 2):
        combine(0, j)
    last = side - 1
    arrive(last)
    flush(own_tiles(PLUS, last, nothing, 0, side // 2, False), False)
    arrive_cross(last)
    flush(far_tiles(1, last, nothing), True)
    to_sib(0, 0).start()
    to_plus(0, 0).start()
    flush(own_tiles(CROSS, last, nothing, 0, side, False), False)
    to_sib(0, last).start()
    combine(0, 0)
    flush(own_tiles(PLUS, last, nothing, side // 2, side, False), False)
    to_plus(0, last).start()
    combine(0, last)
    last_piece = pl.ds(mul(order(me, last), T), T)
    acc[OWN] += (dot_nt(vb[PLUS, :, last_piece], kb[2, :, last_piece])
                 + dot_nt(vb[CROSS, :, last_piece], kb[3, :, last_piece]))
    acc[pl.ds(N_SUM, N_SUM)] = jnp.zeros((N_SUM,) + acc.shape[1:], F32)

    def apply_nn(k_slot, y_slot, out, k):
        piece = pl.ds(mul(k, T), T)
        acc[N_SUM + out] += dot_nn(y_ref(y_slot)[:, piece], kb[k_slot, piece, :])

    def apply_nt(k_slot, y_slot, out, k):
        piece = pl.ds(mul(k, T), T)
        acc[N_SUM + out] += dot_nt(y_ref(y_slot)[:, piece], kb[k_slot, :, piece])

    def make_y(k):
        piece = pl.ds(mul(k, T), T)
        arrived(0, k)
        y_ref(OWN)[:, piece] = (acc[OWN, :, piece] + rb[0, :, piece] + rb[1, :, piece]).astype(BF16)

    def apply_own(k):
        apply_nn(2, OWN, PLUS, k)
        apply_nn(3, OWN, CROSS, k)
        apply_nn(0, OWN, OWN, k)

    @pl.loop(1, 3)
    def _(k):
        make_y(k)
        y_plus, y_minus, y_sib, _ = y_copies(k)
        y_plus.start()
        y_minus.start()
        y_sib.start()
        apply_own(k)

    first, final = order(minus, 0), order(minus, N_PIECE - 1)
    make_y(first)
    make_y(final)
    y_copies(first)[1].start()
    y_copies(final)[0].start()
    y_copies(final)[1].start()
    y_copies(first)[0].start()
    y_copies(first)[2].start()
    y_copies(final)[2].start()

    def y_forward(j):
        y_copies(order(me, j))[0].wait_recv()
        y_copies(order(me, j))[3].start()

    def y_rest(j):
        y_copies(order(me, j))[1].wait_recv()
        y_copies(order(me, j))[3].wait_recv()

    def apply_sib(k):
        y_copies(k)[2].wait_recv()
        apply_nn(1, SIB, OWN, k)

    y_forward(1)
    y_forward(2)

    @pl.loop(0, 2)
    def _(i):
        apply_own(first + i * (final - first))

    apply_sib(1)
    apply_sib(2)
    y_forward(0)

    @pl.loop(0, 2)
    def _(i):
        apply_sib(first + i * (final - first))

    def far_products(group_nn, group_nt):
        for which in (0, 1):
            p_slot, q_slot = far_slots(which)

            def y_piece(slot, start):
                return yb[slot - PLUS, :, pl.ds(pl.multiple_of(start, T), T)]

            for q in sorted({q for _, q in group_nn}):
                total = None
                for r in sorted({r for r, c in group_nn if c == q}):
                    k_row, k_col, p0, q0 = far_place(r, q, which)
                    part = dot_nn(y_piece(p_slot, p0), kb[4, k_row:k_row + T, k_col:k_col + T])
                    total = part if total is None else total + part
                acc[N_SUM + q_slot, :, pl.ds(pl.multiple_of(q0, T), T)] += total
            for r in sorted({r for r, _ in group_nt}):
                total = None
                for q in sorted({q for c, q in group_nt if c == r}):
                    k_row, k_col, p0, q0 = far_place(r, q, which)
                    part = dot_nt(y_piece(q_slot, q0), kb[4, k_row:k_row + T, k_col:k_col + T])
                    total = part if total is None else total + part
                acc[N_SUM + p_slot, :, pl.ds(pl.multiple_of(p0, T), T)] += total

    y_rest(1)
    y_rest(2)
    far_products(((1, 1), (1, 2)), ((1, 1), (1, 2)))
    y_forward(last)
    y_rest(0)
    far_products(((0, 1), (0, 2)), ((1, 0), (2, 0)))
    for j in (1, 2):
        to_sib(1, j).start()
        to_plus(1, j).start()
    far_products(((0, 0), (1, 0), (2, 0)), ((0, 0), (0, 1), (0, 2)))
    for j in (1, 2):
        combine(1, j)
    y_rest(last)
    far_products(((0, last),), ((0, last),))
    for j in (0, last):
        to_sib(1, j).start()
        to_plus(1, j).start()
    apply_nt(2, PLUS, OWN, 0)
    apply_nt(3, CROSS, OWN, 0)
    for j in (0, last):
        combine(1, j)

    @pl.loop(1, N_PIECE)
    def _(k):
        apply_nt(2, PLUS, OWN, k)
        apply_nt(3, CROSS, OWN, k)

    def out_copy(k):
        piece = pl.ds(mul(k, T), T)
        return pltpu.make_async_copy(acc.at[OWN, :, piece], out_hbm.at[:, piece], loc.at[k])

    for k in (1, 2, first, final):
        piece = pl.ds(mul(k, T), T)
        arrived(1, k)
        acc[OWN, :, piece] = acc[N_SUM + OWN, :, piece] + rb[0, :, piece] + rb[1, :, piece]
        out_copy(k).start()
    for copy in (v_plus, v_minus, v_sib, v_cross, sib_x):
        copy.wait_send()
    for k in range(N_PIECE):
        for copy in part_copies(0, k) + part_copies(1, k) + y_copies(k):
            copy.wait_send()
        x_send(0, k).wait_send()
        x_send(1, k).wait_send()
        forward(k).wait_send()
        out_copy(k).wait()


def solution(mesh):
    n_row = mesh.shape["row"]
    assert n_row == 8

    def local_program(x_loc, v_loc, length_scale, out_scale):
        rows, feat = x_loc.shape
        cols = v_loc.shape[1]
        dma = pltpu.SemaphoreType.DMA
        out = pl.pallas_call(
            functools.partial(kernel, n_row),
            out_shape=jax.ShapeDtypeStruct((cols, rows), F32),
            in_specs=[pl.BlockSpec(memory_space=pl.ANY), pl.BlockSpec(memory_space=pl.ANY),
                      pl.BlockSpec(memory_space=pltpu.SMEM), pl.BlockSpec(memory_space=pltpu.SMEM)],
            out_specs=pl.BlockSpec(memory_space=pl.ANY),
            scratch_shapes=[
                pltpu.VMEM((4, rows, feat), BF16),
                pltpu.VMEM((5, rows, rows), BF16),
                pltpu.VMEM((5, cols, rows), BF16),
                pltpu.VMEM((3, cols, rows), BF16),
                pltpu.VMEM((4, 1, rows), F32),
                pltpu.VMEM((2 * N_SUM, cols, rows), F32),
                pltpu.VMEM((3, cols, rows), F32),
                dma((2, N_PIECE)), dma((2, N_PIECE)), dma((N_PIECE,)), dma((N_PIECE,)),
                dma, dma, dma((N_PIECE,)), dma((4,)), dma((4,)), dma((4, N_PIECE)), dma((4, N_PIECE)),
                dma((2, 3, N_PIECE)), dma((2, 3, N_PIECE)), pltpu.SemaphoreType.REGULAR,
            ],
            compiler_params=pltpu.CompilerParams(
                collective_id=0, has_side_effects=True, vmem_limit_bytes=67043328),
        )(x_loc, v_loc.T, length_scale, out_scale)
        return out.T

    row_spec = P(("task", "row"), None)
    return jax.shard_map(local_program, mesh=mesh, in_specs=(row_spec, row_spec, P("task"), P("task")),
                         out_specs=row_spec, check_vma=False)
```

```python
import functools

import jax
import jax.numpy as jnp
from jax import lax
from jax.experimental import pallas as pl
from jax.experimental.pallas import tpu as pltpu
from jax.sharding import PartitionSpec as P

F32 = jnp.float32
BF16 = jnp.bfloat16
LOG2E = 1.4426950408889634
OWN, PLUS, MINUS, CROSS, SIB = 0, 1, 2, 3, 4
N_SUM = 4
TRASH = 7
T = 512
N_PIECE = 4


def dot_nn(a, b):
    return lax.dot_general(a, b, (((1,), (0,)), ((), ())), preferred_element_type=F32)


def dot_nt(a, b):
    return lax.dot_general(a, b, (((1,), (1,)), ((), ())), preferred_element_type=F32)


def kernel(n_row, x_hbm, vt_hbm, length_scale, out_scale, out_hbm, xb, kb, vb, yb, hr, acc, rb,
           x_s, x_r, f_s, f_r, sib_s, sib_r, loc, v_s, v_r, y_s, y_r, p_s, p_r, free):
    rows = xb.shape[1]
    me = lax.axis_index("row")
    core = me % 2
    sib = me + 1 - 2 * core
    plus = (me + 2) % n_row
    minus = (me + n_row - 2) % n_row
    half_ring = n_row // 2

    def order(dev, j):
        flip = dev // half_ring
        return j + flip * (N_PIECE - 1 - 2 * j)

    def remote(src, dst, s_sem, r_sem, dev):
        return pltpu.make_async_remote_copy(
            src_ref=src, dst_ref=dst, send_sem=s_sem, recv_sem=r_sem,
            device_id={"row": dev}, device_id_type=pl.DeviceIdType.MESH)

    def x_send(direction, j):
        slot, dev = ((MINUS, plus), (PLUS, minus))[direction]
        piece = pl.ds(mul(order(dev, j), T), T)
        return remote(x_hbm.at[piece], xb.at[slot, piece], x_s.at[direction, j], x_r.at[direction, j], dev)

    def x_recv(direction, j):
        slot, dev = ((MINUS, plus), (PLUS, minus))[direction]
        piece = pl.ds(mul(order(me, j), T), T)
        return remote(x_hbm.at[piece], xb.at[slot, piece], x_s.at[direction, j], x_r.at[direction, j], dev)

    def forward(j):
        piece = pl.ds(mul(order(me, j), T), T)
        return remote(xb.at[MINUS, piece], xb.at[CROSS, piece], f_s.at[j], f_r.at[j], sib)

    def vec_copies(own, place, s_sem, r_sem):
        return (remote(own, place(MINUS), s_sem(0), r_sem(0), plus),
                remote(own, place(PLUS), s_sem(1), r_sem(1), minus),
                remote(own, place(SIB), s_sem(2), r_sem(2), sib),
                remote(place(MINUS), place(CROSS), s_sem(3), r_sem(3), sib))

    def y_ref(slot):
        return vb.at[slot] if slot in (OWN, SIB) else yb.at[slot - PLUS]

    def y_copies(k):
        piece = pl.ds(mul(k, T), T)
        return vec_copies(y_ref(OWN).at[:, piece], lambda slot: y_ref(slot).at[:, piece],
                          lambda d: y_s.at[d, k], lambda d: y_r.at[d, k])

    def part_copies(step, k):
        cols = pl.ds(mul(k, T), T)
        return tuple(remote(acc.at[step * N_SUM + slot, :, cols], rb.at[i, :, cols], p_s.at[step, i, k], p_r.at[step, i, k], dev)
                     for i, (slot, dev) in enumerate(((PLUS, plus), (MINUS, minus), (CROSS, sib))))

    def mul(i, size):
        return i * size if isinstance(i, int) else pl.multiple_of(i * size, size)

    barrier = pltpu.get_barrier_semaphore()
    for dev in (sib, plus, minus):
        pl.semaphore_signal(barrier, inc=1, device_id={"row": dev}, device_id_type=pl.DeviceIdType.MESH)
    pl.semaphore_wait(barrier, 3)

    own_x = pltpu.make_async_copy(x_hbm, xb.at[OWN], loc.at[0])
    own_v = pltpu.make_async_copy(vt_hbm, vb.at[OWN], loc.at[1])
    own_x.start()
    own_v.start()
    v_plus, v_minus, v_sib, v_cross = vec_copies(
        vt_hbm, lambda slot: vb.at[slot], lambda d: v_s.at[d], lambda d: v_r.at[d])
    sib_x = remote(x_hbm, xb.at[CROSS], sib_s, sib_r, sib)
    v_plus.start()
    v_minus.start()
    for j in range(N_PIECE):
        x_send(0, j).start()
        x_send(1, j).start()
    v_sib.start()
    sib_x.start()

    scale = jnp.full((8, 128), length_scale[0], F32)
    coef_d = (-LOG2E / (scale * scale))[0, 0]
    coef_s = out_scale[0]
    eye = (lax.broadcasted_iota(jnp.int32, (128, 128), 0) == lax.broadcasted_iota(jnp.int32, (128, 128), 1))

    def half_norms(slot, start, width):
        for sub in range(0, width, 128):
            x_sub = xb[slot, pl.ds(start + sub, 128), :].astype(F32)
            col = jnp.sum(x_sub * x_sub, axis=1, keepdims=True) * 0.5
            hr[slot, :, pl.ds(start + sub, 128)] = jnp.sum(jnp.where(eye, col, 0.0), axis=0, keepdims=True)

    def products(t, both):
        k_slot, k_row, k_col, p0, q0, v_p, v_q, acc_p, acc_q = t
        p_piece, q_piece = pl.ds(pl.multiple_of(p0, T), T), pl.ds(pl.multiple_of(q0, T), T)
        k_tile = kb[k_slot, pl.ds(pl.multiple_of(k_row, T), T), pl.ds(pl.multiple_of(k_col, T), T)]
        yield
        acc[acc_q, :, q_piece] += dot_nn(vb[v_p, :, p_piece], k_tile)
        yield
        if both:
            acc[acc_p, :, p_piece] += dot_nt(vb[v_q, :, q_piece], k_tile)
        yield

    def flush(pend, both):
        for _ in products(pend, both):
            pass

    def tile(p_slot, q_slot, t, pend, both):
        k_slot, k_row, k_col, p0, q0 = t[:5]
        k_row, k_col, p0, q0 = (pl.multiple_of(v, T) for v in (k_row, k_col, p0, q0))
        pending = products(pend, both)
        gram = None
        for f in range(0, xb.shape[2], 256):
            part = dot_nt(xb[p_slot, pl.ds(p0, T), pl.ds(f, 256)], xb[q_slot, pl.ds(q0, T), pl.ds(f, 256)])
            gram = part if gram is None else gram + part
            next(pending)
        h_q = hr[q_slot, :, pl.ds(q0, T)]
        for sub in range(0, T, 128):
            h_row = hr[p_slot, :, pl.ds(p0 + sub, 128)]
            h_p = jnp.sum(jnp.where(eye, h_row, 0.0), axis=1, keepdims=True)
            half_d = jnp.maximum(h_p + h_q - gram[sub:sub + 128], 0.0)
            kb[k_slot, pl.ds(k_row + sub, 128), pl.ds(k_col, T)] = (coef_s * jnp.exp2(half_d * coef_d)).astype(BF16)

    def tiles(count, unroll, place, pend, both=True):
        def step(i, pend):
            for sub in range(unroll):
                p_slot, q_slot, t = place(i, sub)
                t = tuple(jnp.int32(v) for v in t)
                tile(p_slot, q_slot, t, pend, both)
                pend = t
            return pend

        return lax.fori_loop(0, count, step, pend)

    nothing = tuple(jnp.int32(v) for v in (0, 0, 0, 0, 0, OWN, OWN, TRASH, TRASH))

    acc[...] = jnp.zeros_like(acc)
    own_x.wait()
    own_v.wait()

    def norm_loop(slot):
        @pl.loop(0, rows // 256)
        def _(i):
            half_norms(slot, mul(i, 256), 256)

    norm_loop(OWN)
    side = rows // T
    pend = tiles(side, side, lambda i, sub: (OWN, OWN, (0, i * T, sub * T, i * T, sub * T, OWN, OWN, TRASH, OWN)), nothing, False)

    sib_x.wait_recv()
    v_sib.wait_recv()
    norm_loop(CROSS)

    pend = tiles(side, side, lambda i, sub: (CROSS, OWN, (1, i * T, sub * T, i * T, sub * T, SIB, OWN, TRASH, OWN)), pend, False)
    flush(pend, False)
    pl.semaphore_signal(free, inc=1, device_id={"row": sib}, device_id_type=pl.DeviceIdType.MESH)
    v_minus.wait_recv()
    v_plus.wait_recv()
    v_cross.start()
    pl.semaphore_wait(free, 1)
    v_cross.wait_recv()

    def own_place(slot, j, sub):
        p0, q0 = sub * T, order(me, j) * T
        return OWN, slot, (2 if slot == PLUS else 3, p0, q0, p0, q0, OWN, slot, OWN, slot)

    final = order(minus, side - 1)
    spare = order(me, side - 1)

    def minus_place(j):
        return OWN, MINUS, (2, j * T, spare * T, final * T, order(me, j) * T, OWN, MINUS, OWN, MINUS)

    swap = me // half_ring

    def far_slots(which):
        other = MINUS + which
        return PLUS + swap * (other - PLUS), other + swap * (PLUS - other)

    def far_place(r, q, which):
        k_row = r + which * (N_PIECE - 1 - 2 * r)
        k_col = q + which * (N_PIECE - 1 - 2 * q)
        return k_row * T, k_col * T, order(me, r) * T, order(me, q) * T

    def far_tiles(count, j, pend):
        def place(i, which):
            r = jnp.where(i == 0, 0, jnp.where(i == 1, j, 1))
            q = jnp.where(i == 1, 0, j)
            p_slot, q_slot = far_slots(which)
            return p_slot, q_slot, (4,) + far_place(r, q, which) + (p_slot, q_slot, p_slot, q_slot)

        return tiles(count, 2, place, pend)

    def arrive(j):
        start = mul(order(me, j), T)
        x_recv(0, j).wait_recv()
        forward(j).start()
        x_recv(1, j).wait_recv()
        half_norms(PLUS, start, T)
        half_norms(MINUS, start, T)

    def arrive_cross(j):
        forward(j).wait_recv()
        half_norms(CROSS, mul(order(me, j), T), T)

    def stage(j, pend):
        arrive(j)
        pend = tiles(1, side + 1, lambda i, sub: own_place(PLUS, j, sub) if sub < side else minus_place(j), pend)
        arrive_cross(j)
        pend = tiles(1, side, lambda i, sub: own_place(CROSS, j, sub), pend)
        return far_tiles(jnp.where(j == 0, 1, 3), j, pend)

    def to_plus(step, j):
        return part_copies(step, order(me, j))[0]

    def to_minus(step, j):
        return part_copies(step, order(me, j))[1]

    def to_sib(step, j):
        return part_copies(step, order(me, j))[2]

    def combine(step, j):
        piece = pl.ds(mul(order(me, j), T), T)
        to_sib(step, j).wait_recv()
        acc[step * N_SUM + MINUS, :, piece] += rb[2, :, piece]
        to_minus(step, j).start()

    def arrived(step, k):
        for copy in part_copies(step, k)[:2]:
            copy.wait_recv()

    pend = lax.fori_loop(0, side - 1, stage, nothing)
    flush(pend, True)
    for j in (1, 2):
        to_sib(0, j).start()
        to_plus(0, j).start()
    for j in (1, 2):
        combine(0, j)
    last = side - 1
    arrive(last)
    flush(tiles(1, 1, lambda i, sub: minus_place(last), nothing), True)
    arrive_cross(last)
    flush(far_tiles(1, last, nothing), True)
    to_sib(0, 0).start()
    to_plus(0, 0).start()
    to_plus(0, last).start()
    pend = tiles(1, side // 2, lambda i, sub: own_place(CROSS, last, sub), nothing, False)
    combine(0, 0)
    pend = tiles(1, side // 2, lambda i, sub: own_place(CROSS, last, side // 2 + sub), pend, False)
    flush(pend, False)
    to_sib(0, last).start()
    last_piece = pl.ds(mul(order(me, last), T), T)
    acc[OWN] += dot_nt(vb[CROSS, :, last_piece], kb[3, :, last_piece])
    combine(0, last)
    acc[pl.ds(N_SUM, N_SUM)] = jnp.zeros((N_SUM,) + acc.shape[1:], F32)

    def apply_nn(k_slot, y_slot, out, k):
        piece = pl.ds(mul(k, T), T)
        acc[N_SUM + out] += dot_nn(y_ref(y_slot)[:, piece], kb[k_slot, piece, :])

    def apply_nt(k_slot, y_slot, out, k):
        piece = pl.ds(mul(k, T), T)
        acc[N_SUM + out] += dot_nt(y_ref(y_slot)[:, piece], kb[k_slot, :, piece])

    def make_y(k):
        piece = pl.ds(mul(k, T), T)
        arrived(0, k)
        y_ref(OWN)[:, piece] = (acc[OWN, :, piece] + rb[0, :, piece] + rb[1, :, piece]).astype(BF16)

    plus_cols = pl.ds(mul(me // half_ring, T), rows - T)

    def apply_own(k):
        piece = pl.ds(mul(k, T), T)
        acc[N_SUM + PLUS, :, plus_cols] += dot_nn(y_ref(OWN)[:, piece], kb[2, piece, plus_cols])
        apply_nn(3, OWN, CROSS, k)

    @pl.loop(1, 3)
    def _(k):
        make_y(k)
        y_plus, y_minus, y_sib, _ = y_copies(k)
        y_plus.start()
        y_minus.start()
        y_sib.start()
        apply_own(k)

    first = order(minus, 0)
    make_y(first)
    make_y(final)
    y_copies(first)[1].start()
    y_copies(final)[0].start()
    y_copies(final)[1].start()
    y_copies(first)[0].start()
    y_copies(first)[2].start()
    y_copies(final)[2].start()

    def y_forward(j):
        y_copies(order(me, j))[0].wait_recv()
        y_copies(order(me, j))[3].start()

    def y_rest(j):
        y_copies(order(me, j))[1].wait_recv()
        y_copies(order(me, j))[3].wait_recv()

    def apply_sib(k):
        y_copies(k)[2].wait_recv()
        apply_nn(1, SIB, OWN, k)

    y_forward(1)
    y_forward(2)

    @pl.loop(0, 2)
    def _(i):
        apply_own(first + i * (final - first))

    spare_cols = pl.ds(mul(spare, T), T)
    for j in range(N_PIECE):
        acc[N_SUM + MINUS, :, pl.ds(mul(order(me, j), T), T)] += dot_nn(
            y_ref(OWN)[:, pl.ds(mul(final, T), T)], kb[2, j * T:(j + 1) * T, spare_cols])
    y_forward(0)

    def far_products(group_nn, group_nt):
        for which in (0, 1):
            p_slot, q_slot = far_slots(which)

            def y_piece(slot, start):
                return yb[slot - PLUS, :, pl.ds(pl.multiple_of(start, T), T)]

            for q in sorted({q for _, q in group_nn}):
                total = None
                for r in sorted({r for r, c in group_nn if c == q}):
                    k_row, k_col, p0, q0 = far_place(r, q, which)
                    part = dot_nn(y_piece(p_slot, p0), kb[4, k_row:k_row + T, k_col:k_col + T])
                    total = part if total is None else total + part
                acc[N_SUM + q_slot, :, pl.ds(pl.multiple_of(q0, T), T)] += total
            for r in sorted({r for r, _ in group_nt}):
                total = None
                for q in sorted({q for c, q in group_nt if c == r}):
                    k_row, k_col, p0, q0 = far_place(r, q, which)
                    part = dot_nt(y_piece(q_slot, q0), kb[4, k_row:k_row + T, k_col:k_col + T])
                    total = part if total is None else total + part
                acc[N_SUM + p_slot, :, pl.ds(pl.multiple_of(p0, T), T)] += total

    y_rest(1)
    y_rest(2)
    far_products(((1, 1), (1, 2)), ((1, 1), (1, 2)))
    y_forward(last)
    y_rest(0)
    far_products(((0, 1), (0, 2)), ((1, 0), (2, 0)))
    for j in (1, 2):
        to_sib(1, j).start()
        to_plus(1, j).start()
    far_products(((0, 0), (1, 0), (2, 0)), ((0, 0), (0, 1), (0, 2)))
    for j in (1, 2):
        combine(1, j)
    y_rest(last)
    far_products(((0, last),), ((0, last),))
    for j in (0, last):
        to_sib(1, j).start()
        to_plus(1, j).start()
    apply_nn(0, OWN, OWN, 0)
    apply_sib(0)
    for j in (0, last):
        combine(1, j)

    @pl.loop(1, N_PIECE)
    def _(k):
        apply_nn(0, OWN, OWN, k)
        apply_sib(k)

    @pl.loop(0, N_PIECE - 1)
    def _(j):
        apply_nt(2, PLUS, OWN, order(me, j))
        apply_nt(3, CROSS, OWN, order(me, j))

    apply_nt(3, CROSS, OWN, spare)
    acc[N_SUM + OWN, :, pl.ds(mul(final, T), T)] += sum(
        dot_nt(yb[MINUS - PLUS, :, pl.ds(mul(order(me, j), T), T)], kb[2, j * T:(j + 1) * T, spare_cols])
        for j in range(N_PIECE))

    def out_copy(k):
        piece = pl.ds(mul(k, T), T)
        return pltpu.make_async_copy(acc.at[OWN, :, piece], out_hbm.at[:, piece], loc.at[k])

    for k in (1, 2, first, final):
        piece = pl.ds(mul(k, T), T)
        arrived(1, k)
        acc[OWN, :, piece] = acc[N_SUM + OWN, :, piece] + rb[0, :, piece] + rb[1, :, piece]
        out_copy(k).start()
    for copy in (v_plus, v_minus, v_sib, v_cross, sib_x):
        copy.wait_send()
    for k in range(N_PIECE):
        for copy in part_copies(0, k) + part_copies(1, k) + y_copies(k):
            copy.wait_send()
        x_send(0, k).wait_send()
        x_send(1, k).wait_send()
        forward(k).wait_send()
        out_copy(k).wait()


def solution(mesh):
    n_row = mesh.shape["row"]
    assert n_row == 8

    def local_program(x_loc, v_loc, length_scale, out_scale):
        rows, feat = x_loc.shape
        cols = v_loc.shape[1]
        dma = pltpu.SemaphoreType.DMA
        out = pl.pallas_call(
            functools.partial(kernel, n_row),
            out_shape=jax.ShapeDtypeStruct((cols, rows), F32),
            in_specs=[pl.BlockSpec(memory_space=pl.ANY), pl.BlockSpec(memory_space=pl.ANY),
                      pl.BlockSpec(memory_space=pltpu.SMEM), pl.BlockSpec(memory_space=pltpu.SMEM)],
            out_specs=pl.BlockSpec(memory_space=pl.ANY),
            scratch_shapes=[
                pltpu.VMEM((4, rows, feat), BF16),
                pltpu.VMEM((5, rows, rows), BF16),
                pltpu.VMEM((5, cols, rows), BF16),
                pltpu.VMEM((3, cols, rows), BF16),
                pltpu.VMEM((4, 1, rows), F32),
                pltpu.VMEM((2 * N_SUM, cols, rows), F32),
                pltpu.VMEM((3, cols, rows), F32),
                dma((2, N_PIECE)), dma((2, N_PIECE)), dma((N_PIECE,)), dma((N_PIECE,)),
                dma, dma, dma((N_PIECE,)), dma((4,)), dma((4,)), dma((4, N_PIECE)), dma((4, N_PIECE)),
                dma((2, 3, N_PIECE)), dma((2, 3, N_PIECE)), pltpu.SemaphoreType.REGULAR,
            ],
            compiler_params=pltpu.CompilerParams(
                collective_id=0, has_side_effects=True, vmem_limit_bytes=67043328),
        )(x_loc, v_loc.T, length_scale, out_scale)
        return out.T

    row_spec = P(("task", "row"), None)
    return jax.shard_map(local_program, mesh=mesh, in_specs=(row_spec, row_spec, P("task"), P("task")),
                         out_specs=row_spec, check_vma=False)
```

```python
import functools

import jax
import jax.numpy as jnp
from jax import lax
from jax.experimental import pallas as pl
from jax.experimental.pallas import tpu as pltpu
from jax.sharding import PartitionSpec as P

F32 = jnp.float32
BF16 = jnp.bfloat16
LOG2E = 1.4426950408889634
OWN, PLUS, MINUS, CROSS, SIB = 0, 1, 2, 3, 4
N_SUM = 4
TRASH = 7
T = 512
N_PIECE = 4


def dot_nn(a, b):
    return lax.dot_general(a, b, (((1,), (0,)), ((), ())), preferred_element_type=F32)


def dot_nt(a, b):
    return lax.dot_general(a, b, (((1,), (1,)), ((), ())), preferred_element_type=F32)


def kernel(n_row, x_hbm, vt_hbm, length_scale, out_scale, out_hbm, xb, kb, vb, yb, hr, acc, rb,
           x_s, x_r, f_s, f_r, sib_s, sib_r, loc, v_s, v_r, y_s, y_r, p_s, p_r, free):
    rows = xb.shape[1]
    me = lax.axis_index("row")
    core = me % 2
    sib = me + 1 - 2 * core
    plus = (me + 2) % n_row
    minus = (me + n_row - 2) % n_row
    half_ring = n_row // 2

    def order(dev, j):
        flip = dev // half_ring
        return j + flip * (N_PIECE - 1 - 2 * j)

    def remote(src, dst, s_sem, r_sem, dev):
        return pltpu.make_async_remote_copy(
            src_ref=src, dst_ref=dst, send_sem=s_sem, recv_sem=r_sem,
            device_id={"row": dev}, device_id_type=pl.DeviceIdType.MESH)

    def x_send(direction, j):
        slot, dev = ((MINUS, plus), (PLUS, minus))[direction]
        piece = pl.ds(mul(order(dev, j), T), T)
        return remote(x_hbm.at[piece], xb.at[slot, piece], x_s.at[direction, j], x_r.at[direction, j], dev)

    def x_recv(direction, j):
        slot, dev = ((MINUS, plus), (PLUS, minus))[direction]
        piece = pl.ds(mul(order(me, j), T), T)
        return remote(x_hbm.at[piece], xb.at[slot, piece], x_s.at[direction, j], x_r.at[direction, j], dev)

    def forward(j):
        piece = pl.ds(mul(order(me, j), T), T)
        return remote(xb.at[MINUS, piece], xb.at[CROSS, piece], f_s.at[j], f_r.at[j], sib)

    def vec_copies(own, place, s_sem, r_sem):
        return (remote(own, place(MINUS), s_sem(0), r_sem(0), plus),
                remote(own, place(PLUS), s_sem(1), r_sem(1), minus),
                remote(own, place(SIB), s_sem(2), r_sem(2), sib),
                remote(place(MINUS), place(CROSS), s_sem(3), r_sem(3), sib))

    def y_ref(slot):
        return vb.at[slot] if slot in (OWN, SIB) else yb.at[slot - PLUS]

    def y_copies(k):
        piece = pl.ds(mul(k, T), T)
        return vec_copies(y_ref(OWN).at[:, piece], lambda slot: y_ref(slot).at[:, piece],
                          lambda d: y_s.at[d, k], lambda d: y_r.at[d, k])

    def part_copies(step, k):
        cols = pl.ds(mul(k, T), T)
        return tuple(remote(acc.at[step * N_SUM + slot, :, cols], rb.at[i, :, cols], p_s.at[step, i, k], p_r.at[step, i, k], dev)
                     for i, (slot, dev) in enumerate(((PLUS, plus), (MINUS, minus), (CROSS, sib))))

    def mul(i, size):
        return i * size if isinstance(i, int) else pl.multiple_of(i * size, size)

    barrier = pltpu.get_barrier_semaphore()
    for dev in (sib, plus, minus):
        pl.semaphore_signal(barrier, inc=1, device_id={"row": dev}, device_id_type=pl.DeviceIdType.MESH)
    pl.semaphore_wait(barrier, 3)

    own_x = pltpu.make_async_copy(x_hbm, xb.at[OWN], loc.at[0])
    own_v = pltpu.make_async_copy(vt_hbm, vb.at[OWN], loc.at[1])
    v_plus, v_minus, v_sib, v_cross = vec_copies(
        vt_hbm, lambda slot: vb.at[slot], lambda d: v_s.at[d], lambda d: v_r.at[d])
    sib_x = remote(x_hbm, xb.at[CROSS], sib_s, sib_r, sib)
    v_plus.start()
    v_minus.start()
    for j in range(N_PIECE):
        x_send(0, j).start()
        x_send(1, j).start()
    own_x.start()
    own_v.start()
    v_sib.start()
    sib_x.start()

    scale = jnp.full((8, 128), length_scale[0], F32)
    coef_d = (-LOG2E / (scale * scale))[0, 0]
    coef_s = out_scale[0]
    eye = (lax.broadcasted_iota(jnp.int32, (128, 128), 0) == lax.broadcasted_iota(jnp.int32, (128, 128), 1))

    def half_norms(slot, start, width):
        for sub in range(0, width, 128):
            x_sub = xb[slot, pl.ds(start + sub, 128), :].astype(F32)
            col = jnp.sum(x_sub * x_sub, axis=1, keepdims=True) * 0.5
            hr[slot, :, pl.ds(start + sub, 128)] = jnp.sum(jnp.where(eye, col, 0.0), axis=0, keepdims=True)

    def products(t, both):
        k_slot, k_row, k_col, p0, q0, v_p, v_q, acc_p, acc_q = t
        p_piece, q_piece = pl.ds(pl.multiple_of(p0, T), T), pl.ds(pl.multiple_of(q0, T), T)
        k_tile = kb[k_slot, pl.ds(pl.multiple_of(k_row, T), T), pl.ds(pl.multiple_of(k_col, T), T)]
        yield
        acc[acc_q, :, q_piece] += dot_nn(vb[v_p, :, p_piece], k_tile)
        yield
        if both:
            acc[acc_p, :, p_piece] += dot_nt(vb[v_q, :, q_piece], k_tile)
        yield

    def flush(pend, both):
        for _ in products(pend, both):
            pass

    def tile(p_slot, q_slot, t, pend, both):
        k_slot, k_row, k_col, p0, q0 = t[:5]
        k_row, k_col, p0, q0 = (pl.multiple_of(v, T) for v in (k_row, k_col, p0, q0))
        pending = products(pend, both)
        gram = None
        for f in range(0, xb.shape[2], 256):
            part = dot_nt(xb[p_slot, pl.ds(p0, T), pl.ds(f, 256)], xb[q_slot, pl.ds(q0, T), pl.ds(f, 256)])
            gram = part if gram is None else gram + part
            next(pending)
        h_q = hr[q_slot, :, pl.ds(q0, T)]
        for sub in range(0, T, 128):
            h_row = hr[p_slot, :, pl.ds(p0 + sub, 128)]
            h_p = jnp.sum(jnp.where(eye, h_row, 0.0), axis=1, keepdims=True)
            half_d = jnp.maximum(h_p + h_q - gram[sub:sub + 128], 0.0)
            kb[k_slot, pl.ds(k_row + sub, 128), pl.ds(k_col, T)] = (coef_s * jnp.exp2(half_d * coef_d)).astype(BF16)

    def tiles(count, unroll, place, pend, both=True):
        def step(i, pend):
            for sub in range(unroll):
                p_slot, q_slot, t = place(i, sub)
                t = tuple(jnp.int32(v) for v in t)
                tile(p_slot, q_slot, t, pend, both)
                pend = t
            return pend

        return lax.fori_loop(0, count, step, pend)

    nothing = tuple(jnp.int32(v) for v in (0, 0, 0, 0, 0, OWN, OWN, TRASH, TRASH))

    acc[...] = jnp.zeros_like(acc)
    own_x.wait()
    own_v.wait()

    def norm_loop(slot):
        @pl.loop(0, rows // 256)
        def _(i):
            half_norms(slot, mul(i, 256), 256)

    norm_loop(OWN)
    side = rows // T
    pend = tiles(side, side, lambda i, sub: (OWN, OWN, (0, i * T, sub * T, i * T, sub * T, OWN, OWN, TRASH, OWN)), nothing, False)

    sib_x.wait_recv()
    v_sib.wait_recv()
    norm_loop(CROSS)

    pend = tiles(side, side, lambda i, sub: (CROSS, OWN, (1, i * T, sub * T, i * T, sub * T, SIB, OWN, TRASH, OWN)), pend, False)
    flush(pend, False)
    pl.semaphore_signal(free, inc=1, device_id={"row": sib}, device_id_type=pl.DeviceIdType.MESH)
    v_minus.wait_recv()
    v_plus.wait_recv()
    v_cross.start()
    pl.semaphore_wait(free, 1)
    v_cross.wait_recv()

    def own_place(slot, j, sub):
        p0, q0 = sub * T, order(me, j) * T
        return OWN, slot, (2 if slot == PLUS else 3, p0, q0, p0, q0, OWN, slot, OWN, slot)

    final = order(minus, side - 1)
    spare = order(me, side - 1)

    def minus_place(j):
        return OWN, MINUS, (2, j * T, spare * T, final * T, order(me, j) * T, OWN, MINUS, OWN, MINUS)

    swap = me // half_ring

    def far_slots(which):
        other = MINUS + which
        return PLUS + swap * (other - PLUS), other + swap * (PLUS - other)

    def far_place(r, q, which):
        k_row = r + which * (N_PIECE - 1 - 2 * r)
        k_col = q + which * (N_PIECE - 1 - 2 * q)
        return k_row * T, k_col * T, order(me, r) * T, order(me, q) * T

    def far_tile(r, q, which):
        p_slot, q_slot = far_slots(which)
        return p_slot, q_slot, (4,) + far_place(r, q, which) + (p_slot, q_slot, p_slot, q_slot)

    def far_tiles(count, j, pend):
        def place(i, which):
            r = jnp.where(i == 0, 0, jnp.where(i == 1, j, 1))
            q = jnp.where(i == 1, 0, j)
            return far_tile(r, q, which)

        return tiles(count, 2, place, pend)

    def arrive(j):
        start = mul(order(me, j), T)
        x_recv(0, j).wait_recv()
        forward(j).start()
        x_recv(1, j).wait_recv()
        half_norms(PLUS, start, T)
        half_norms(MINUS, start, T)

    def arrive_cross(j):
        forward(j).wait_recv()
        half_norms(CROSS, mul(order(me, j), T), T)

    def stage(j, pend):
        arrive(j)
        pend = tiles(1, side + 1, lambda i, sub: own_place(PLUS, j, sub) if sub < side else minus_place(j), pend)
        arrive_cross(j)
        pend = tiles(1, side, lambda i, sub: own_place(CROSS, j, sub), pend)
        return far_tiles(jnp.where(j == 0, 1, 3), j, pend)

    def to_plus(step, j):
        return part_copies(step, order(me, j))[0]

    def to_minus(step, j):
        return part_copies(step, order(me, j))[1]

    def to_sib(step, j):
        return part_copies(step, order(me, j))[2]

    def combine(step, j):
        piece = pl.ds(mul(order(me, j), T), T)
        to_sib(step, j).wait_recv()
        acc[step * N_SUM + MINUS, :, piece] += rb[2, :, piece]
        to_minus(step, j).start()

    def arrived(step, k):
        for copy in part_copies(step, k)[:2]:
            copy.wait_recv()

    pend = lax.fori_loop(0, side - 1, stage, nothing)
    flush(pend, True)
    for j in (1, 2):
        to_sib(0, j).start()
        to_plus(0, j).start()
    for j in (1, 2):
        combine(0, j)
    last = side - 1
    arrive(last)
    flush(tiles(1, 2, lambda i, sub: far_tile(0, last, 0) if sub else minus_place(last), nothing), True)
    arrive_cross(last)
    flush(tiles(1, 1, lambda i, sub: far_tile(0, last, 1), nothing), True)
    to_sib(0, 0).start()
    to_plus(0, 0).start()
    to_plus(0, last).start()
    pend = tiles(1, side // 2, lambda i, sub: own_place(CROSS, last, sub), nothing, False)
    combine(0, 0)
    pend = tiles(1, side // 2, lambda i, sub: own_place(CROSS, last, side // 2 + sub), pend, False)
    flush(pend, False)
    to_sib(0, last).start()
    last_piece = pl.ds(mul(order(me, last), T), T)
    acc[OWN] += dot_nt(vb[CROSS, :, last_piece], kb[3, :, last_piece])
    combine(0, last)
    acc[pl.ds(N_SUM, N_SUM)] = jnp.zeros((N_SUM,) + acc.shape[1:], F32)

    def apply_nn(k_slot, y_slot, out, k):
        piece = pl.ds(mul(k, T), T)
        acc[N_SUM + out] += dot_nn(y_ref(y_slot)[:, piece], kb[k_slot, piece, :])

    def apply_nt(k_slot, y_slot, out, k):
        piece = pl.ds(mul(k, T), T)
        acc[N_SUM + out] += dot_nt(y_ref(y_slot)[:, piece], kb[k_slot, :, piece])

    def make_y(k):
        piece = pl.ds(mul(k, T), T)
        arrived(0, k)
        y_ref(OWN)[:, piece] = (acc[OWN, :, piece] + rb[0, :, piece] + rb[1, :, piece]).astype(BF16)

    plus_cols = pl.ds(mul(me // half_ring, T), rows - T)

    def apply_own(k):
        piece = pl.ds(mul(k, T), T)
        acc[N_SUM + PLUS, :, plus_cols] += dot_nn(y_ref(OWN)[:, piece], kb[2, piece, plus_cols])
        apply_nn(3, OWN, CROSS, k)

    @pl.loop(1, 3)
    def _(k):
        make_y(k)
        y_plus, y_minus, y_sib, _ = y_copies(k)
        y_plus.start()
        y_minus.start()
        y_sib.start()
        apply_own(k)

    first = order(minus, 0)
    make_y(first)
    make_y(final)
    y_copies(first)[1].start()
    y_copies(final)[0].start()
    y_copies(final)[1].start()
    y_copies(first)[0].start()
    y_copies(first)[2].start()
    y_copies(final)[2].start()

    def y_forward(j):
        y_copies(order(me, j))[0].wait_recv()
        y_copies(order(me, j))[3].start()

    def y_rest(j):
        y_copies(order(me, j))[1].wait_recv()
        y_copies(order(me, j))[3].wait_recv()

    def apply_sib(k):
        y_copies(k)[2].wait_recv()
        apply_nn(1, SIB, OWN, k)

    y_forward(1)
    y_forward(2)

    @pl.loop(0, 2)
    def _(i):
        apply_own(first + i * (final - first))

    spare_cols = pl.ds(mul(spare, T), T)
    for j in range(N_PIECE):
        acc[N_SUM + MINUS, :, pl.ds(mul(order(me, j), T), T)] += dot_nn(
            y_ref(OWN)[:, pl.ds(mul(final, T), T)], kb[2, j * T:(j + 1) * T, spare_cols])
    def far_products(group_nn, group_nt, pairs=(0, 1)):
        for which in pairs:
            p_slot, q_slot = far_slots(which)

            def y_piece(slot, start):
                return yb[slot - PLUS, :, pl.ds(pl.multiple_of(start, T), T)]

            for q in sorted({q for _, q in group_nn}):
                total = None
                for r in sorted({r for r, c in group_nn if c == q}):
                    k_row, k_col, p0, q0 = far_place(r, q, which)
                    part = dot_nn(y_piece(p_slot, p0), kb[4, k_row:k_row + T, k_col:k_col + T])
                    total = part if total is None else total + part
                acc[N_SUM + q_slot, :, pl.ds(pl.multiple_of(q0, T), T)] += total
            for r in sorted({r for r, _ in group_nt}):
                total = None
                for q in sorted({q for c, q in group_nt if c == r}):
                    k_row, k_col, p0, q0 = far_place(r, q, which)
                    part = dot_nt(y_piece(q_slot, q0), kb[4, k_row:k_row + T, k_col:k_col + T])
                    total = part if total is None else total + part
                acc[N_SUM + p_slot, :, pl.ds(pl.multiple_of(p0, T), T)] += total

    y_rest(1)
    y_rest(2)
    far_products(((1, 1), (1, 2)), ((1, 1), (1, 2)))
    y_forward(0)
    y_copies(order(me, 0))[1].wait_recv()
    far_products(((0, 1), (0, 2)), ((1, 0), (2, 0)), (0,))
    y_copies(order(me, 0))[3].wait_recv()
    far_products(((0, 1), (0, 2)), ((1, 0), (2, 0)), (1,))
    for j in (1, 2):
        to_sib(1, j).start()
        to_plus(1, j).start()
    y_forward(last)
    far_products(((0, 0), (1, 0), (2, 0)), ((0, 0), (0, 1), (0, 2)))
    for j in (1, 2):
        combine(1, j)
    y_rest(last)
    far_products(((0, last),), ((0, last),))
    for j in (0, last):
        to_sib(1, j).start()
        to_plus(1, j).start()
    apply_nn(0, OWN, OWN, 0)
    apply_sib(0)
    for j in (0, last):
        combine(1, j)

    @pl.loop(1, N_PIECE)
    def _(k):
        apply_nn(0, OWN, OWN, k)
        apply_sib(k)

    @pl.loop(0, N_PIECE - 1)
    def _(j):
        apply_nt(2, PLUS, OWN, order(me, j))
        apply_nt(3, CROSS, OWN, order(me, j))

    apply_nt(3, CROSS, OWN, spare)
    acc[N_SUM + OWN, :, pl.ds(mul(final, T), T)] += sum(
        dot_nt(yb[MINUS - PLUS, :, pl.ds(mul(order(me, j), T), T)], kb[2, j * T:(j + 1) * T, spare_cols])
        for j in range(N_PIECE))

    def out_copy(k):
        piece = pl.ds(mul(k, T), T)
        return pltpu.make_async_copy(acc.at[OWN, :, piece], out_hbm.at[:, piece], loc.at[k])

    for k in (1, 2, first, final):
        piece = pl.ds(mul(k, T), T)
        arrived(1, k)
        acc[OWN, :, piece] = acc[N_SUM + OWN, :, piece] + rb[0, :, piece] + rb[1, :, piece]
        out_copy(k).start()
    for copy in (v_plus, v_minus, v_sib, v_cross, sib_x):
        copy.wait_send()
    for k in range(N_PIECE):
        for copy in part_copies(0, k) + part_copies(1, k) + y_copies(k):
            copy.wait_send()
        x_send(0, k).wait_send()
        x_send(1, k).wait_send()
        forward(k).wait_send()
        out_copy(k).wait()


def solution(mesh):
    n_row = mesh.shape["row"]
    assert n_row == 8

    def local_program(x_loc, v_loc, length_scale, out_scale):
        rows, feat = x_loc.shape
        cols = v_loc.shape[1]
        dma = pltpu.SemaphoreType.DMA
        out = pl.pallas_call(
            functools.partial(kernel, n_row),
            out_shape=jax.ShapeDtypeStruct((cols, rows), F32),
            in_specs=[pl.BlockSpec(memory_space=pl.ANY), pl.BlockSpec(memory_space=pl.ANY),
                      pl.BlockSpec(memory_space=pltpu.SMEM), pl.BlockSpec(memory_space=pltpu.SMEM)],
            out_specs=pl.BlockSpec(memory_space=pl.ANY),
            scratch_shapes=[
                pltpu.VMEM((4, rows, feat), BF16),
                pltpu.VMEM((5, rows, rows), BF16),
                pltpu.VMEM((5, cols, rows), BF16),
                pltpu.VMEM((3, cols, rows), BF16),
                pltpu.VMEM((4, 1, rows), F32),
                pltpu.VMEM((2 * N_SUM, cols, rows), F32),
                pltpu.VMEM((3, cols, rows), F32),
                dma((2, N_PIECE)), dma((2, N_PIECE)), dma((N_PIECE,)), dma((N_PIECE,)),
                dma, dma, dma((N_PIECE,)), dma((4,)), dma((4,)), dma((4, N_PIECE)), dma((4, N_PIECE)),
                dma((2, 3, N_PIECE)), dma((2, 3, N_PIECE)), pltpu.SemaphoreType.REGULAR,
            ],
            compiler_params=pltpu.CompilerParams(
                collective_id=0, has_side_effects=True, vmem_limit_bytes=67043328),
        )(x_loc, v_loc.T, length_scale, out_scale)
        return out.T

    row_spec = P(("task", "row"), None)
    return jax.shard_map(local_program, mesh=mesh, in_specs=(row_spec, row_spec, P("task"), P("task")),
                         out_specs=row_spec, check_vma=False)
```

```python
import functools

import jax
import jax.numpy as jnp
from jax import lax
from jax.experimental import pallas as pl
from jax.experimental.pallas import tpu as pltpu
from jax.sharding import PartitionSpec as P

F32 = jnp.float32
BF16 = jnp.bfloat16
LOG2E = 1.4426950408889634
OWN, PLUS, MINUS, CROSS, SIB = 0, 1, 2, 3, 4
N_SUM = 4
TRASH = 7
T = 512
N_PIECE = 4


def dot_nn(a, b):
    return lax.dot_general(a, b, (((1,), (0,)), ((), ())), preferred_element_type=F32)


def dot_nt(a, b):
    return lax.dot_general(a, b, (((1,), (1,)), ((), ())), preferred_element_type=F32)


def kernel(n_row, x_hbm, vt_hbm, length_scale, out_scale, out_hbm, xb, kb, vb, yb, hr, acc, rb,
           x_s, x_r, f_s, f_r, sib_s, sib_r, loc, v_s, v_r, y_s, y_r, p_s, p_r, free):
    rows = xb.shape[1]
    me = lax.axis_index("row")
    core = me % 2
    sib = me + 1 - 2 * core
    plus = (me + 2) % n_row
    minus = (me + n_row - 2) % n_row
    half_ring = n_row // 2

    def order(dev, j):
        flip = dev // half_ring
        return j + flip * (N_PIECE - 1 - 2 * j)

    def remote(src, dst, s_sem, r_sem, dev):
        return pltpu.make_async_remote_copy(
            src_ref=src, dst_ref=dst, send_sem=s_sem, recv_sem=r_sem,
            device_id={"row": dev}, device_id_type=pl.DeviceIdType.MESH)

    def x_send(direction, j):
        slot, dev = ((MINUS, plus), (PLUS, minus))[direction]
        piece = pl.ds(mul(order(dev, j), T), T)
        return remote(x_hbm.at[piece], xb.at[slot, piece], x_s.at[direction, j], x_r.at[direction, j], dev)

    def x_recv(direction, j):
        slot, dev = ((MINUS, plus), (PLUS, minus))[direction]
        piece = pl.ds(mul(order(me, j), T), T)
        return remote(x_hbm.at[piece], xb.at[slot, piece], x_s.at[direction, j], x_r.at[direction, j], dev)

    def forward(j):
        piece = pl.ds(mul(order(me, j), T), T)
        return remote(xb.at[MINUS, piece], xb.at[CROSS, piece], f_s.at[j], f_r.at[j], sib)

    def vec_copies(own, place, s_sem, r_sem):
        return (remote(own, place(MINUS), s_sem(0), r_sem(0), plus),
                remote(own, place(PLUS), s_sem(1), r_sem(1), minus),
                remote(own, place(SIB), s_sem(2), r_sem(2), sib),
                remote(place(MINUS), place(CROSS), s_sem(3), r_sem(3), sib))

    def y_ref(slot):
        return vb.at[slot] if slot in (OWN, SIB) else yb.at[slot - PLUS]

    def y_copies(k):
        piece = pl.ds(mul(k, T), T)
        return vec_copies(y_ref(OWN).at[:, piece], lambda slot: y_ref(slot).at[:, piece],
                          lambda d: y_s.at[d, k], lambda d: y_r.at[d, k])

    def part_copies(step, k):
        cols = pl.ds(mul(k, T), T)
        return tuple(remote(acc.at[step * N_SUM + slot, :, cols], rb.at[i, :, cols], p_s.at[step, i, k], p_r.at[step, i, k], dev)
                     for i, (slot, dev) in enumerate(((PLUS, plus), (MINUS, minus), (CROSS, sib))))

    def mul(i, size):
        return i * size if isinstance(i, int) else pl.multiple_of(i * size, size)

    barrier = pltpu.get_barrier_semaphore()
    for dev in (sib, plus, minus):
        pl.semaphore_signal(barrier, inc=1, device_id={"row": dev}, device_id_type=pl.DeviceIdType.MESH)
    pl.semaphore_wait(barrier, 3)

    own_x = pltpu.make_async_copy(x_hbm, xb.at[OWN], loc.at[0])
    own_v = pltpu.make_async_copy(vt_hbm, vb.at[OWN], loc.at[1])
    v_plus, v_minus, v_sib, v_cross = vec_copies(
        vt_hbm, lambda slot: vb.at[slot], lambda d: v_s.at[d], lambda d: v_r.at[d])
    sib_x = remote(x_hbm, xb.at[CROSS], sib_s, sib_r, sib)
    v_plus.start()
    v_minus.start()
    for j in range(N_PIECE):
        x_send(0, j).start()
        x_send(1, j).start()
    own_x.start()
    own_v.start()
    v_sib.start()
    sib_x.start()

    scale = jnp.full((8, 128), length_scale[0], F32)
    coef_d = (-LOG2E / (scale * scale))[0, 0]
    coef_s = out_scale[0]
    eye = (lax.broadcasted_iota(jnp.int32, (128, 128), 0) == lax.broadcasted_iota(jnp.int32, (128, 128), 1))

    def half_norms(slot, start, width):
        for sub in range(0, width, 128):
            x_sub = xb[slot, pl.ds(start + sub, 128), :].astype(F32)
            col = jnp.sum(x_sub * x_sub, axis=1, keepdims=True) * 0.5
            hr[slot, :, pl.ds(start + sub, 128)] = jnp.sum(jnp.where(eye, col, 0.0), axis=0, keepdims=True)

    def products(t, both):
        k_slot, k_row, k_col, p0, q0, v_p, v_q, acc_p, acc_q = t
        p_piece, q_piece = pl.ds(pl.multiple_of(p0, T), T), pl.ds(pl.multiple_of(q0, T), T)
        k_tile = kb[k_slot, pl.ds(pl.multiple_of(k_row, T), T), pl.ds(pl.multiple_of(k_col, T), T)]
        yield
        acc[acc_q, :, q_piece] += dot_nn(vb[v_p, :, p_piece], k_tile)
        yield
        if both:
            acc[acc_p, :, p_piece] += dot_nt(vb[v_q, :, q_piece], k_tile)
        yield

    def flush(pend, both):
        for _ in products(pend, both):
            pass

    def tile(p_slot, q_slot, t, pend, both):
        k_slot, k_row, k_col, p0, q0 = t[:5]
        k_row, k_col, p0, q0 = (pl.multiple_of(v, T) for v in (k_row, k_col, p0, q0))
        pending = products(pend, both)
        gram = None
        for f in range(0, xb.shape[2], 256):
            part = dot_nt(xb[p_slot, pl.ds(p0, T), pl.ds(f, 256)], xb[q_slot, pl.ds(q0, T), pl.ds(f, 256)])
            gram = part if gram is None else gram + part
            next(pending)
        h_q = hr[q_slot, :, pl.ds(q0, T)]
        for sub in range(0, T, 128):
            h_row = hr[p_slot, :, pl.ds(p0 + sub, 128)]
            h_p = jnp.sum(jnp.where(eye, h_row, 0.0), axis=1, keepdims=True)
            half_d = jnp.maximum(h_p + h_q - gram[sub:sub + 128], 0.0)
            kb[k_slot, pl.ds(k_row + sub, 128), pl.ds(k_col, T)] = (coef_s * jnp.exp2(half_d * coef_d)).astype(BF16)

    def tiles(count, unroll, place, pend, both=True):
        def step(i, pend):
            for sub in range(unroll):
                p_slot, q_slot, t = place(i, sub)
                t = tuple(jnp.int32(v) for v in t)
                tile(p_slot, q_slot, t, pend, both)
                pend = t
            return pend

        return lax.fori_loop(0, count, step, pend)

    nothing = tuple(jnp.int32(v) for v in (0, 0, 0, 0, 0, OWN, OWN, TRASH, TRASH))

    acc[...] = jnp.zeros_like(acc)
    own_x.wait()
    own_v.wait()

    def norm_loop(slot):
        @pl.loop(0, rows // 256)
        def _(i):
            half_norms(slot, mul(i, 256), 256)

    norm_loop(OWN)
    side = rows // T
    pend = tiles(side, side, lambda i, sub: (OWN, OWN, (0, i * T, sub * T, i * T, sub * T, OWN, OWN, TRASH, OWN)), nothing, False)

    sib_x.wait_recv()
    v_sib.wait_recv()
    norm_loop(CROSS)

    pend = tiles(side, side, lambda i, sub: (CROSS, OWN, (1, i * T, sub * T, i * T, sub * T, SIB, OWN, TRASH, OWN)), pend, False)
    flush(pend, False)
    pl.semaphore_signal(free, inc=1, device_id={"row": sib}, device_id_type=pl.DeviceIdType.MESH)
    v_minus.wait_recv()
    v_plus.wait_recv()
    v_cross.start()
    pl.semaphore_wait(free, 1)
    v_cross.wait_recv()

    def own_place(slot, j, sub):
        p0, q0 = sub * T, order(me, j) * T
        return OWN, slot, (2 if slot == PLUS else 3, p0, q0, p0, q0, OWN, slot, OWN, slot)

    final = order(minus, side - 1)
    spare = order(me, side - 1)

    def minus_place(j):
        return OWN, MINUS, (2, j * T, spare * T, final * T, order(me, j) * T, OWN, MINUS, OWN, MINUS)

    swap = me // half_ring

    def far_slots(which):
        other = MINUS + which
        return PLUS + swap * (other - PLUS), other + swap * (PLUS - other)

    def far_place(r, q, which):
        k_row = r + which * (N_PIECE - 1 - 2 * r)
        k_col = q + which * (N_PIECE - 1 - 2 * q)
        return k_row * T, k_col * T, order(me, r) * T, order(me, q) * T

    def far_tile(r, q, which):
        p_slot, q_slot = far_slots(which)
        return p_slot, q_slot, (4,) + far_place(r, q, which) + (p_slot, q_slot, p_slot, q_slot)

    def far_tiles(count, j, pend):
        def place(i, which):
            r = jnp.where(i == 0, 0, jnp.where(i == 1, j, 1))
            q = jnp.where(i == 1, 0, j)
            return far_tile(r, q, which)

        return tiles(count, 2, place, pend)

    def arrive(j):
        start = mul(order(me, j), T)
        x_recv(0, j).wait_recv()
        forward(j).start()
        x_recv(1, j).wait_recv()
        half_norms(PLUS, start, T)
        half_norms(MINUS, start, T)

    def arrive_cross(j):
        forward(j).wait_recv()
        half_norms(CROSS, mul(order(me, j), T), T)

    def stage(j, pend):
        arrive(j)
        pend = tiles(1, side + 1, lambda i, sub: own_place(PLUS, j, sub) if sub < side else minus_place(j), pend)
        arrive_cross(j)
        pend = tiles(1, side, lambda i, sub: own_place(CROSS, j, sub), pend)
        return far_tiles(jnp.where(j == 0, 1, 3), j, pend)

    def to_plus(step, j):
        return part_copies(step, order(me, j))[0]

    def to_minus(step, j):
        return part_copies(step, order(me, j))[1]

    def to_sib(step, j):
        return part_copies(step, order(me, j))[2]

    def combine(step, j):
        piece = pl.ds(mul(order(me, j), T), T)
        to_sib(step, j).wait_recv()
        acc[step * N_SUM + MINUS, :, piece] += rb[2, :, piece]
        to_minus(step, j).start()

    def arrived(step, k):
        for copy in part_copies(step, k)[:2]:
            copy.wait_recv()

    pend = lax.fori_loop(0, side - 1, stage, nothing)
    flush(pend, True)
    for j in (1, 2):
        to_sib(0, j).start()
        to_plus(0, j).start()
    for j in (1, 2):
        combine(0, j)
    last = side - 1
    arrive(last)
    flush(tiles(1, 2, lambda i, sub: far_tile(0, last, 0) if sub else minus_place(last), nothing), True)
    arrive_cross(last)
    flush(tiles(1, 1, lambda i, sub: far_tile(0, last, 1), nothing), True)
    to_sib(0, 0).start()
    to_plus(0, last).start()
    to_plus(0, 0).start()
    pend = tiles(1, side // 2, lambda i, sub: own_place(CROSS, last, sub), nothing, False)
    combine(0, 0)
    pend = tiles(1, side // 2, lambda i, sub: own_place(CROSS, last, side // 2 + sub), pend, False)
    flush(pend, False)
    to_sib(0, last).start()
    last_piece = pl.ds(mul(order(me, last), T), T)
    acc[OWN] += dot_nt(vb[CROSS, :, last_piece], kb[3, :, last_piece])
    combine(0, last)
    acc[pl.ds(N_SUM, N_SUM)] = jnp.zeros((N_SUM,) + acc.shape[1:], F32)

    def apply_nn(k_slot, y_slot, out, k):
        piece = pl.ds(mul(k, T), T)
        acc[N_SUM + out] += dot_nn(y_ref(y_slot)[:, piece], kb[k_slot, piece, :])

    def apply_nt(k_slot, y_slot, out, k):
        piece = pl.ds(mul(k, T), T)
        acc[N_SUM + out] += dot_nt(y_ref(y_slot)[:, piece], kb[k_slot, :, piece])

    def make_y(k):
        piece = pl.ds(mul(k, T), T)
        arrived(0, k)
        y_ref(OWN)[:, piece] = (acc[OWN, :, piece] + rb[0, :, piece] + rb[1, :, piece]).astype(BF16)

    plus_cols = pl.ds(mul(me // half_ring, T), rows - T)

    def apply_own(k):
        piece = pl.ds(mul(k, T), T)
        acc[N_SUM + PLUS, :, plus_cols] += dot_nn(y_ref(OWN)[:, piece], kb[2, piece, plus_cols])
        apply_nn(3, OWN, CROSS, k)

    @pl.loop(1, 3)
    def _(k):
        make_y(k)
        y_copies(k)[1].start()
        y_copies(k)[2].start()
        apply_own(k)

    first = order(minus, 0)
    make_y(final)
    for k in (final, 1, 2):
        y_copies(k)[0].start()
    apply_own(final)
    make_y(first)
    y_copies(first)[1].start()
    y_copies(final)[1].start()
    y_copies(first)[0].start()
    y_copies(first)[2].start()
    y_copies(final)[2].start()

    def y_forward(j):
        y_copies(order(me, j))[0].wait_recv()
        y_copies(order(me, j))[3].start()

    def y_rest(j):
        y_copies(order(me, j))[1].wait_recv()
        y_copies(order(me, j))[3].wait_recv()

    def apply_sib(k):
        y_copies(k)[2].wait_recv()
        apply_nn(1, SIB, OWN, k)

    apply_own(first)

    for j in (0, 1, 2):
        y_forward(j)
    spare_cols = pl.ds(mul(spare, T), T)
    for j in range(N_PIECE):
        acc[N_SUM + MINUS, :, pl.ds(mul(order(me, j), T), T)] += dot_nn(
            y_ref(OWN)[:, pl.ds(mul(final, T), T)], kb[2, j * T:(j + 1) * T, spare_cols])
    def far_products(group_nn, group_nt, pairs=(0, 1)):
        for which in pairs:
            p_slot, q_slot = far_slots(which)

            def y_piece(slot, start):
                return yb[slot - PLUS, :, pl.ds(pl.multiple_of(start, T), T)]

            for q in sorted({q for _, q in group_nn}):
                total = None
                for r in sorted({r for r, c in group_nn if c == q}):
                    k_row, k_col, p0, q0 = far_place(r, q, which)
                    part = dot_nn(y_piece(p_slot, p0), kb[4, k_row:k_row + T, k_col:k_col + T])
                    total = part if total is None else total + part
                acc[N_SUM + q_slot, :, pl.ds(pl.multiple_of(q0, T), T)] += total
            for r in sorted({r for r, _ in group_nt}):
                total = None
                for q in sorted({q for c, q in group_nt if c == r}):
                    k_row, k_col, p0, q0 = far_place(r, q, which)
                    part = dot_nt(y_piece(q_slot, q0), kb[4, k_row:k_row + T, k_col:k_col + T])
                    total = part if total is None else total + part
                acc[N_SUM + p_slot, :, pl.ds(pl.multiple_of(p0, T), T)] += total

    y_rest(1)
    y_rest(2)
    far_products(((1, 1), (1, 2)), ((1, 1), (1, 2)))
    y_copies(order(me, 0))[3].wait_recv()

    by_row = lambda: far_products(((0, 1), (0, 2)), ())
    by_col = lambda: far_products((), ((1, 0), (2, 0)))
    pl.when(swap == 0)(by_col)
    pl.when(swap != 0)(by_row)
    y_copies(order(me, 0))[1].wait_recv()
    pl.when(swap == 0)(by_row)
    pl.when(swap != 0)(by_col)
    for j in (1, 2):
        to_sib(1, j).start()
        to_plus(1, j).start()
    y_forward(last)
    far_products(((0, 0), (1, 0), (2, 0)), ((0, 0), (0, 1), (0, 2)))
    for j in (1, 2):
        combine(1, j)
    y_rest(last)
    far_products(((0, last),), ((0, last),))
    for j in (0, last):
        to_sib(1, j).start()
        to_plus(1, j).start()
    apply_nn(0, OWN, OWN, 0)
    apply_sib(0)
    for j in (0, last):
        combine(1, j)

    @pl.loop(1, N_PIECE)
    def _(k):
        apply_nn(0, OWN, OWN, k)
        apply_sib(k)

    @pl.loop(0, N_PIECE - 1)
    def _(j):
        apply_nt(2, PLUS, OWN, order(me, j))
        apply_nt(3, CROSS, OWN, order(me, j))

    apply_nt(3, CROSS, OWN, spare)
    acc[N_SUM + OWN, :, pl.ds(mul(final, T), T)] += sum(
        dot_nt(yb[MINUS - PLUS, :, pl.ds(mul(order(me, j), T), T)], kb[2, j * T:(j + 1) * T, spare_cols])
        for j in range(N_PIECE))

    def out_copy(k):
        piece = pl.ds(mul(k, T), T)
        return pltpu.make_async_copy(acc.at[OWN, :, piece], out_hbm.at[:, piece], loc.at[k])

    for k in (1, 2, first, final):
        piece = pl.ds(mul(k, T), T)
        arrived(1, k)
        acc[OWN, :, piece] = acc[N_SUM + OWN, :, piece] + rb[0, :, piece] + rb[1, :, piece]
        out_copy(k).start()
    for copy in (v_plus, v_minus, v_sib, v_cross, sib_x):
        copy.wait_send()
    for k in range(N_PIECE):
        for copy in part_copies(0, k) + part_copies(1, k) + y_copies(k):
            copy.wait_send()
        x_send(0, k).wait_send()
        x_send(1, k).wait_send()
        forward(k).wait_send()
        out_copy(k).wait()


def solution(mesh):
    n_row = mesh.shape["row"]
    assert n_row == 8

    def local_program(x_loc, v_loc, length_scale, out_scale):
        rows, feat = x_loc.shape
        cols = v_loc.shape[1]
        dma = pltpu.SemaphoreType.DMA
        out = pl.pallas_call(
            functools.partial(kernel, n_row),
            out_shape=jax.ShapeDtypeStruct((cols, rows), F32),
            in_specs=[pl.BlockSpec(memory_space=pl.ANY), pl.BlockSpec(memory_space=pl.ANY),
                      pl.BlockSpec(memory_space=pltpu.SMEM), pl.BlockSpec(memory_space=pltpu.SMEM)],
            out_specs=pl.BlockSpec(memory_space=pl.ANY),
            scratch_shapes=[
                pltpu.VMEM((4, rows, feat), BF16),
                pltpu.VMEM((5, rows, rows), BF16),
                pltpu.VMEM((5, cols, rows), BF16),
                pltpu.VMEM((3, cols, rows), BF16),
                pltpu.VMEM((4, 1, rows), F32),
                pltpu.VMEM((2 * N_SUM, cols, rows), F32),
                pltpu.VMEM((3, cols, rows), F32),
                dma((2, N_PIECE)), dma((2, N_PIECE)), dma((N_PIECE,)), dma((N_PIECE,)),
                dma, dma, dma((N_PIECE,)), dma((4,)), dma((4,)), dma((4, N_PIECE)), dma((4, N_PIECE)),
                dma((2, 3, N_PIECE)), dma((2, 3, N_PIECE)), pltpu.SemaphoreType.REGULAR,
            ],
            compiler_params=pltpu.CompilerParams(
                collective_id=0, has_side_effects=True, vmem_limit_bytes=67043328),
        )(x_loc, v_loc.T, length_scale, out_scale)
        return out.T

    row_spec = P(("task", "row"), None)
    return jax.shard_map(local_program, mesh=mesh, in_specs=(row_spec, row_spec, P("task"), P("task")),
                         out_specs=row_spec, check_vma=False)
```

```python
import functools

import jax
import jax.numpy as jnp
from jax import lax
from jax.experimental import pallas as pl
from jax.experimental.pallas import tpu as pltpu
from jax.sharding import PartitionSpec as P

F32 = jnp.float32
BF16 = jnp.bfloat16
LOG2E = 1.4426950408889634
OWN, PLUS, MINUS, CROSS, SIB = 0, 1, 2, 3, 4
N_SUM = 4
TRASH = 7
T = 512
N_PIECE = 4


def dot_nn(a, b):
    return lax.dot_general(a, b, (((1,), (0,)), ((), ())), preferred_element_type=F32)


def dot_nt(a, b):
    return lax.dot_general(a, b, (((1,), (1,)), ((), ())), preferred_element_type=F32)


def kernel(n_row, x_hbm, vt_hbm, length_scale, out_scale, out_hbm, xb, kb, vb, yb, hr, acc, rb,
           x_s, x_r, f_s, f_r, sib_s, sib_r, loc, v_s, v_r, y_s, y_r, p_s, p_r, free):
    rows = xb.shape[1]
    me = lax.axis_index("row")
    core = me % 2
    sib = me + 1 - 2 * core
    plus = (me + 2) % n_row
    minus = (me + n_row - 2) % n_row
    half_ring = n_row // 2

    def order(dev, j):
        flip = dev // half_ring
        return j + flip * (N_PIECE - 1 - 2 * j)

    def remote(src, dst, s_sem, r_sem, dev):
        return pltpu.make_async_remote_copy(
            src_ref=src, dst_ref=dst, send_sem=s_sem, recv_sem=r_sem,
            device_id={"row": dev}, device_id_type=pl.DeviceIdType.MESH)

    def x_send(direction, j):
        slot, dev = ((MINUS, plus), (PLUS, minus))[direction]
        piece = pl.ds(mul(order(dev, j), T), T)
        return remote(x_hbm.at[piece], xb.at[slot, piece], x_s.at[direction, j], x_r.at[direction, j], dev)

    def x_recv(direction, j):
        slot, dev = ((MINUS, plus), (PLUS, minus))[direction]
        piece = pl.ds(mul(order(me, j), T), T)
        return remote(x_hbm.at[piece], xb.at[slot, piece], x_s.at[direction, j], x_r.at[direction, j], dev)

    def forward(j):
        piece = pl.ds(mul(order(me, j), T), T)
        return remote(xb.at[MINUS, piece], xb.at[CROSS, piece], f_s.at[j], f_r.at[j], sib)

    def vec_copies(own, place, s_sem, r_sem):
        return (remote(own, place(MINUS), s_sem(0), r_sem(0), plus),
                remote(own, place(PLUS), s_sem(1), r_sem(1), minus),
                remote(own, place(SIB), s_sem(2), r_sem(2), sib),
                remote(place(MINUS), place(CROSS), s_sem(3), r_sem(3), sib))

    def y_ref(slot):
        return vb.at[slot] if slot in (OWN, SIB) else yb.at[slot - PLUS]

    def y_copies(k):
        piece = pl.ds(mul(k, T), T)
        return vec_copies(y_ref(OWN).at[:, piece], lambda slot: y_ref(slot).at[:, piece],
                          lambda d: y_s.at[d, k], lambda d: y_r.at[d, k])

    def part_copies(step, k):
        cols = pl.ds(mul(k, T), T)
        return tuple(remote(acc.at[step * N_SUM + slot, :, cols], rb.at[i, :, cols], p_s.at[step, i, k], p_r.at[step, i, k], dev)
                     for i, (slot, dev) in enumerate(((PLUS, plus), (MINUS, minus), (CROSS, sib))))

    def mul(i, size):
        return i * size if isinstance(i, int) else pl.multiple_of(i * size, size)

    barrier = pltpu.get_barrier_semaphore()
    for dev in (sib, plus, minus):
        pl.semaphore_signal(barrier, inc=1, device_id={"row": dev}, device_id_type=pl.DeviceIdType.MESH)
    pl.semaphore_wait(barrier, 3)

    own_x = pltpu.make_async_copy(x_hbm, xb.at[OWN], loc.at[0])
    own_v = pltpu.make_async_copy(vt_hbm, vb.at[OWN], loc.at[1])
    v_plus, v_minus, v_sib, v_cross = vec_copies(
        vt_hbm, lambda slot: vb.at[slot], lambda d: v_s.at[d], lambda d: v_r.at[d])
    sib_x = remote(x_hbm, xb.at[CROSS], sib_s, sib_r, sib)
    v_plus.start()
    v_minus.start()
    for j in range(N_PIECE):
        x_send(0, j).start()
        x_send(1, j).start()
    own_x.start()
    own_v.start()
    v_sib.start()
    sib_x.start()

    scale = jnp.full((8, 128), length_scale[0], F32)
    coef_d = (-LOG2E / (scale * scale))[0, 0]
    coef_s = out_scale[0]
    eye = (lax.broadcasted_iota(jnp.int32, (128, 128), 0) == lax.broadcasted_iota(jnp.int32, (128, 128), 1))

    def half_norms(slot, start, width):
        for sub in range(0, width, 128):
            x_sub = xb[slot, pl.ds(start + sub, 128), :].astype(F32)
            col = jnp.sum(x_sub * x_sub, axis=1, keepdims=True) * 0.5
            hr[slot, :, pl.ds(start + sub, 128)] = jnp.sum(jnp.where(eye, col, 0.0), axis=0, keepdims=True)

    def products(t, both):
        k_slot, k_row, k_col, p0, q0, v_p, v_q, acc_p, acc_q = t
        p_piece, q_piece = pl.ds(pl.multiple_of(p0, T), T), pl.ds(pl.multiple_of(q0, T), T)
        k_tile = kb[k_slot, pl.ds(pl.multiple_of(k_row, T), T), pl.ds(pl.multiple_of(k_col, T), T)]
        yield
        acc[acc_q, :, q_piece] += dot_nn(vb[v_p, :, p_piece], k_tile)
        yield
        if both:
            acc[acc_p, :, p_piece] += dot_nt(vb[v_q, :, q_piece], k_tile)
        yield

    def flush(pend, both):
        for _ in products(pend, both):
            pass

    def tile(p_slot, q_slot, t, pend, both):
        k_slot, k_row, k_col, p0, q0 = t[:5]
        k_row, k_col, p0, q0 = (pl.multiple_of(v, T) for v in (k_row, k_col, p0, q0))
        pending = products(pend, both)
        gram = None
        for f in range(0, xb.shape[2], 256):
            part = dot_nt(xb[p_slot, pl.ds(p0, T), pl.ds(f, 256)], xb[q_slot, pl.ds(q0, T), pl.ds(f, 256)])
            gram = part if gram is None else gram + part
            next(pending)
        h_q = hr[q_slot, :, pl.ds(q0, T)]
        for sub in range(0, T, 128):
            h_row = hr[p_slot, :, pl.ds(p0 + sub, 128)]
            h_p = jnp.sum(jnp.where(eye, h_row, 0.0), axis=1, keepdims=True)
            half_d = jnp.maximum(h_p + h_q - gram[sub:sub + 128], 0.0)
            kb[k_slot, pl.ds(k_row + sub, 128), pl.ds(k_col, T)] = (coef_s * jnp.exp2(half_d * coef_d)).astype(BF16)

    def tiles(count, unroll, place, pend, both=True):
        def step(i, pend):
            for sub in range(unroll):
                p_slot, q_slot, t = place(i, sub)
                t = tuple(jnp.int32(v) for v in t)
                tile(p_slot, q_slot, t, pend, both)
                pend = t
            return pend

        return lax.fori_loop(0, count, step, pend)

    nothing = tuple(jnp.int32(v) for v in (0, 0, 0, 0, 0, OWN, OWN, TRASH, TRASH))

    acc[...] = jnp.zeros_like(acc)
    own_x.wait()
    own_v.wait()

    def norm_loop(slot):
        @pl.loop(0, rows // 256)
        def _(i):
            half_norms(slot, mul(i, 256), 256)

    norm_loop(OWN)
    side = rows // T
    pend = tiles(side, side, lambda i, sub: (OWN, OWN, (0, i * T, sub * T, i * T, sub * T, OWN, OWN, TRASH, OWN)), nothing, False)

    sib_x.wait_recv()
    v_sib.wait_recv()
    norm_loop(CROSS)

    pend = tiles(side, side, lambda i, sub: (CROSS, OWN, (1, i * T, sub * T, i * T, sub * T, SIB, OWN, TRASH, OWN)), pend, False)
    flush(pend, False)
    pl.semaphore_signal(free, inc=1, device_id={"row": sib}, device_id_type=pl.DeviceIdType.MESH)
    v_minus.wait_recv()
    v_plus.wait_recv()
    v_cross.start()
    pl.semaphore_wait(free, 1)
    v_cross.wait_recv()

    def own_place(slot, j, sub):
        p0, q0 = sub * T, order(me, j) * T
        return OWN, slot, (2 if slot == PLUS else 3, p0, q0, p0, q0, OWN, slot, OWN, slot)

    final = order(minus, side - 1)
    spare = order(me, side - 1)

    def minus_place(j):
        return OWN, MINUS, (2, j * T, spare * T, final * T, order(me, j) * T, OWN, MINUS, OWN, MINUS)

    swap = me // half_ring

    def far_slots(which):
        other = MINUS + which
        return PLUS + swap * (other - PLUS), other + swap * (PLUS - other)

    def far_place(r, q, which):
        k_row = r + which * (N_PIECE - 1 - 2 * r)
        k_col = q + which * (N_PIECE - 1 - 2 * q)
        return k_row * T, k_col * T, order(me, r) * T, order(me, q) * T

    def far_tile(r, q, which):
        p_slot, q_slot = far_slots(which)
        return p_slot, q_slot, (4,) + far_place(r, q, which) + (p_slot, q_slot, p_slot, q_slot)

    def far_tiles(count, j, pend):
        def place(i, which):
            r = jnp.where(i == 0, 0, jnp.where(i == 1, j, 1))
            q = jnp.where(i == 1, 0, j)
            return far_tile(r, q, which)

        return tiles(count, 2, place, pend)

    def arrive(j):
        start = mul(order(me, j), T)
        x_recv(0, j).wait_recv()
        forward(j).start()
        x_recv(1, j).wait_recv()
        half_norms(PLUS, start, T)
        half_norms(MINUS, start, T)

    def arrive_cross(j):
        forward(j).wait_recv()
        half_norms(CROSS, mul(order(me, j), T), T)

    def stage(j, pend):
        arrive(j)
        pend = tiles(1, side + 1, lambda i, sub: own_place(PLUS, j, sub) if sub < side else minus_place(j), pend)
        arrive_cross(j)
        pend = tiles(1, side, lambda i, sub: own_place(CROSS, j, sub), pend)
        return far_tiles(jnp.where(j == 0, 1, 3), j, pend)

    def to_plus(step, j):
        return part_copies(step, order(me, j))[0]

    def to_minus(step, j):
        return part_copies(step, order(me, j))[1]

    def to_sib(step, j):
        return part_copies(step, order(me, j))[2]

    def combine(step, j):
        piece = pl.ds(mul(order(me, j), T), T)
        to_sib(step, j).wait_recv()
        acc[step * N_SUM + MINUS, :, piece] += rb[2, :, piece]
        to_minus(step, j).start()

    def arrived(step, k):
        for copy in part_copies(step, k)[:2]:
            copy.wait_recv()

    pend = lax.fori_loop(0, side - 1, stage, nothing)
    flush(pend, True)
    for j in (1, 2):
        to_sib(0, j).start()
        to_plus(0, j).start()
    for j in (1, 2):
        combine(0, j)
    last = side - 1
    arrive(last)
    flush(tiles(1, 2, lambda i, sub: far_tile(0, last, 0) if sub else minus_place(last), nothing), True)
    arrive_cross(last)
    flush(tiles(1, 1, lambda i, sub: far_tile(0, last, 1), nothing), True)
    to_sib(0, 0).start()
    to_plus(0, 0).start()
    to_plus(0, last).start()
    pend = tiles(1, side // 2, lambda i, sub: own_place(CROSS, last, sub), nothing, False)
    combine(0, 0)
    pend = tiles(1, side // 2, lambda i, sub: own_place(CROSS, last, side // 2 + sub), pend, False)
    flush(pend, False)
    to_sib(0, last).start()
    last_piece = pl.ds(mul(order(me, last), T), T)
    acc[OWN] += dot_nt(vb[CROSS, :, last_piece], kb[3, :, last_piece])
    combine(0, last)
    acc[pl.ds(N_SUM, N_SUM)] = jnp.zeros((N_SUM,) + acc.shape[1:], F32)

    def apply_nn(k_slot, y_slot, out, k):
        piece = pl.ds(mul(k, T), T)
        acc[N_SUM + out] += dot_nn(y_ref(y_slot)[:, piece], kb[k_slot, piece, :])

    def apply_nt(k_slot, y_slot, out, k):
        piece = pl.ds(mul(k, T), T)
        acc[N_SUM + out] += dot_nt(y_ref(y_slot)[:, piece], kb[k_slot, :, piece])

    def make_y(k):
        piece = pl.ds(mul(k, T), T)
        arrived(0, k)
        y_ref(OWN)[:, piece] = (acc[OWN, :, piece] + rb[0, :, piece] + rb[1, :, piece]).astype(BF16)

    plus_cols = pl.ds(mul(me // half_ring, T), rows - T)

    def apply_own(k):
        piece = pl.ds(mul(k, T), T)
        acc[N_SUM + PLUS, :, plus_cols] += dot_nn(y_ref(OWN)[:, piece], kb[2, piece, plus_cols])
        apply_nn(3, OWN, CROSS, k)

    @pl.loop(1, 3)
    def _(k):
        make_y(k)
        y_plus, y_minus, y_sib, _ = y_copies(k)
        y_plus.start()
        y_minus.start()
        y_sib.start()
        apply_own(k)

    first = order(minus, 0)
    make_y(first)
    make_y(final)
    y_copies(first)[1].start()
    y_copies(final)[0].start()
    y_copies(final)[1].start()
    y_copies(first)[0].start()
    y_copies(first)[2].start()
    y_copies(final)[2].start()

    def y_forward(j):
        y_copies(order(me, j))[0].wait_recv()
        y_copies(order(me, j))[3].start()

    def y_rest(j):
        y_copies(order(me, j))[1].wait_recv()
        y_copies(order(me, j))[3].wait_recv()

    def apply_sib(k):
        y_copies(k)[2].wait_recv()
        apply_nn(1, SIB, OWN, k)

    y_forward(1)
    y_forward(2)

    @pl.loop(0, 2)
    def _(i):
        apply_own(first + i * (final - first))

    spare_cols = pl.ds(mul(spare, T), T)
    for j in range(N_PIECE):
        acc[N_SUM + MINUS, :, pl.ds(mul(order(me, j), T), T)] += dot_nn(
            y_ref(OWN)[:, pl.ds(mul(final, T), T)], kb[2, j * T:(j + 1) * T, spare_cols])
    def far_products(group_nn, group_nt, pairs=(0, 1)):
        for which in pairs:
            p_slot, q_slot = far_slots(which)

            def y_piece(slot, start):
                return yb[slot - PLUS, :, pl.ds(pl.multiple_of(start, T), T)]

            for q in sorted({q for _, q in group_nn}):
                total = None
                for r in sorted({r for r, c in group_nn if c == q}):
                    k_row, k_col, p0, q0 = far_place(r, q, which)
                    part = dot_nn(y_piece(p_slot, p0), kb[4, k_row:k_row + T, k_col:k_col + T])
                    total = part if total is None else total + part
                acc[N_SUM + q_slot, :, pl.ds(pl.multiple_of(q0, T), T)] += total
            for r in sorted({r for r, _ in group_nt}):
                total = None
                for q in sorted({q for c, q in group_nt if c == r}):
                    k_row, k_col, p0, q0 = far_place(r, q, which)
                    part = dot_nt(y_piece(q_slot, q0), kb[4, k_row:k_row + T, k_col:k_col + T])
                    total = part if total is None else total + part
                acc[N_SUM + p_slot, :, pl.ds(pl.multiple_of(p0, T), T)] += total

    y_rest(1)
    y_rest(2)
    far_products(((1, 1), (1, 2)), ((1, 1), (1, 2)))
    y_forward(0)
    y_copies(order(me, 0))[1].wait_recv()
    by_row = lambda: far_products(((0, 1), (0, 2)), ())
    by_col = lambda: far_products((), ((1, 0), (2, 0)))
    pl.when(swap == 0)(by_row)
    pl.when(swap != 0)(by_col)
    for j in (1, 2):
        to_sib(1, j).start()
    y_copies(order(me, 0))[3].wait_recv()
    pl.when(swap == 0)(by_col)
    pl.when(swap != 0)(by_row)
    for j in (1, 2):
        to_plus(1, j).start()
    for j in (1, 2):
        combine(1, j)
    y_forward(last)
    far_products(((0, 0), (1, 0), (2, 0)), ((0, 0), (0, 1), (0, 2)))
    y_rest(last)
    far_products(((0, last),), ((0, last),))
    for j in (0, last):
        to_sib(1, j).start()
        to_plus(1, j).start()
    apply_nn(0, OWN, OWN, 0)
    apply_sib(0)
    for j in (0, last):
        combine(1, j)

    @pl.loop(1, N_PIECE)
    def _(k):
        apply_nn(0, OWN, OWN, k)
        apply_sib(k)

    @pl.loop(0, N_PIECE - 1)
    def _(j):
        apply_nt(2, PLUS, OWN, order(me, j))
        apply_nt(3, CROSS, OWN, order(me, j))

    apply_nt(3, CROSS, OWN, spare)
    acc[N_SUM + OWN, :, pl.ds(mul(final, T), T)] += sum(
        dot_nt(yb[MINUS - PLUS, :, pl.ds(mul(order(me, j), T), T)], kb[2, j * T:(j + 1) * T, spare_cols])
        for j in range(N_PIECE))

    def out_copy(k):
        piece = pl.ds(mul(k, T), T)
        return pltpu.make_async_copy(acc.at[OWN, :, piece], out_hbm.at[:, piece], loc.at[k])

    for k in (1, 2, first, final):
        piece = pl.ds(mul(k, T), T)
        arrived(1, k)
        acc[OWN, :, piece] = acc[N_SUM + OWN, :, piece] + rb[0, :, piece] + rb[1, :, piece]
        out_copy(k).start()
    for copy in (v_plus, v_minus, v_sib, v_cross, sib_x):
        copy.wait_send()
    for k in range(N_PIECE):
        for copy in part_copies(0, k) + part_copies(1, k) + y_copies(k):
            copy.wait_send()
        x_send(0, k).wait_send()
        x_send(1, k).wait_send()
        forward(k).wait_send()
        out_copy(k).wait()


def solution(mesh):
    n_row = mesh.shape["row"]
    assert n_row == 8

    def local_program(x_loc, v_loc, length_scale, out_scale):
        rows, feat = x_loc.shape
        cols = v_loc.shape[1]
        dma = pltpu.SemaphoreType.DMA
        out = pl.pallas_call(
            functools.partial(kernel, n_row),
            out_shape=jax.ShapeDtypeStruct((cols, rows), F32),
            in_specs=[pl.BlockSpec(memory_space=pl.ANY), pl.BlockSpec(memory_space=pl.ANY),
                      pl.BlockSpec(memory_space=pltpu.SMEM), pl.BlockSpec(memory_space=pltpu.SMEM)],
            out_specs=pl.BlockSpec(memory_space=pl.ANY),
            scratch_shapes=[
                pltpu.VMEM((4, rows, feat), BF16),
                pltpu.VMEM((5, rows, rows), BF16),
                pltpu.VMEM((5, cols, rows), BF16),
                pltpu.VMEM((3, cols, rows), BF16),
                pltpu.VMEM((4, 1, rows), F32),
                pltpu.VMEM((2 * N_SUM, cols, rows), F32),
                pltpu.VMEM((3, cols, rows), F32),
                dma((2, N_PIECE)), dma((2, N_PIECE)), dma((N_PIECE,)), dma((N_PIECE,)),
                dma, dma, dma((N_PIECE,)), dma((4,)), dma((4,)), dma((4, N_PIECE)), dma((4, N_PIECE)),
                dma((2, 3, N_PIECE)), dma((2, 3, N_PIECE)), pltpu.SemaphoreType.REGULAR,
            ],
            compiler_params=pltpu.CompilerParams(
                collective_id=0, has_side_effects=True, vmem_limit_bytes=67043328),
        )(x_loc, v_loc.T, length_scale, out_scale)
        return out.T

    row_spec = P(("task", "row"), None)
    return jax.shard_map(local_program, mesh=mesh, in_specs=(row_spec, row_spec, P("task"), P("task")),
                         out_specs=row_spec, check_vma=False)
```

```python
import functools

import jax
import jax.numpy as jnp
from jax import lax
from jax.experimental import pallas as pl
from jax.experimental.pallas import tpu as pltpu
from jax.sharding import PartitionSpec as P

F32 = jnp.float32
BF16 = jnp.bfloat16
LOG2E = 1.4426950408889634
OWN, PLUS, MINUS, CROSS, SIB = 0, 1, 2, 3, 4
N_SUM = 4
TRASH = 7
T = 512
N_PIECE = 4


def dot_nn(a, b):
    return lax.dot_general(a, b, (((1,), (0,)), ((), ())), preferred_element_type=F32)


def dot_nt(a, b):
    return lax.dot_general(a, b, (((1,), (1,)), ((), ())), preferred_element_type=F32)


def kernel(n_row, x_hbm, vt_hbm, length_scale, out_scale, out_hbm, xb, kb, vb, yb, hr, acc, rb,
           x_s, x_r, f_s, f_r, sib_s, sib_r, loc, v_s, v_r, y_s, y_r, p_s, p_r, free):
    rows = xb.shape[1]
    me = lax.axis_index("row")
    core = me % 2
    sib = me + 1 - 2 * core
    plus = (me + 2) % n_row
    minus = (me + n_row - 2) % n_row
    half_ring = n_row // 2

    def order(dev, j):
        flip = dev // half_ring
        return j + flip * (N_PIECE - 1 - 2 * j)

    def remote(src, dst, s_sem, r_sem, dev):
        return pltpu.make_async_remote_copy(
            src_ref=src, dst_ref=dst, send_sem=s_sem, recv_sem=r_sem,
            device_id={"row": dev}, device_id_type=pl.DeviceIdType.MESH)

    def x_send(direction, j):
        slot, dev = ((MINUS, plus), (PLUS, minus))[direction]
        piece = pl.ds(mul(order(dev, j), T), T)
        return remote(x_hbm.at[piece], xb.at[slot, piece], x_s.at[direction, j], x_r.at[direction, j], dev)

    def x_recv(direction, j):
        slot, dev = ((MINUS, plus), (PLUS, minus))[direction]
        piece = pl.ds(mul(order(me, j), T), T)
        return remote(x_hbm.at[piece], xb.at[slot, piece], x_s.at[direction, j], x_r.at[direction, j], dev)

    def forward(j):
        piece = pl.ds(mul(order(me, j), T), T)
        return remote(xb.at[MINUS, piece], xb.at[CROSS, piece], f_s.at[j], f_r.at[j], sib)

    def vec_copies(own, place, s_sem, r_sem):
        return (remote(own, place(MINUS), s_sem(0), r_sem(0), plus),
                remote(own, place(PLUS), s_sem(1), r_sem(1), minus),
                remote(own, place(SIB), s_sem(2), r_sem(2), sib),
                remote(place(MINUS), place(CROSS), s_sem(3), r_sem(3), sib))

    def y_ref(slot):
        return vb.at[slot] if slot in (OWN, SIB) else yb.at[slot - PLUS]

    def y_copies(k):
        piece = pl.ds(mul(k, T), T)
        return vec_copies(y_ref(OWN).at[:, piece], lambda slot: y_ref(slot).at[:, piece],
                          lambda d: y_s.at[d, k], lambda d: y_r.at[d, k])

    def part_copies(step, k):
        cols = pl.ds(mul(k, T), T)
        return tuple(remote(acc.at[step * N_SUM + slot, :, cols], rb.at[i, :, cols], p_s.at[step, i, k], p_r.at[step, i, k], dev)
                     for i, (slot, dev) in enumerate(((PLUS, plus), (MINUS, minus), (CROSS, sib))))

    def mul(i, size):
        return i * size if isinstance(i, int) else pl.multiple_of(i * size, size)

    barrier = pltpu.get_barrier_semaphore()
    for dev in (sib, plus, minus):
        pl.semaphore_signal(barrier, inc=1, device_id={"row": dev}, device_id_type=pl.DeviceIdType.MESH)
    pl.semaphore_wait(barrier, 3)

    own_x = pltpu.make_async_copy(x_hbm, xb.at[OWN], loc.at[0])
    own_v = pltpu.make_async_copy(vt_hbm, vb.at[OWN], loc.at[1])
    v_plus, v_minus, v_sib, v_cross = vec_copies(
        vt_hbm, lambda slot: vb.at[slot], lambda d: v_s.at[d], lambda d: v_r.at[d])
    sib_x = remote(x_hbm, xb.at[CROSS], sib_s, sib_r, sib)
    v_plus.start()
    v_minus.start()
    for j in range(N_PIECE):
        x_send(0, j).start()
        x_send(1, j).start()
    own_x.start()
    own_v.start()
    v_sib.start()
    sib_x.start()

    scale = jnp.full((8, 128), length_scale[0], F32)
    coef_d = (-2.0 * LOG2E / (2.0 * scale * scale))[0, 0]
    coef_s = out_scale[0]
    eye = (lax.broadcasted_iota(jnp.int32, (128, 128), 0) == lax.broadcasted_iota(jnp.int32, (128, 128), 1))

    def half_norms(slot, start, width):
        for sub in range(0, width, 128):
            x_sub = xb[slot, pl.ds(start + sub, 128), :].astype(F32)
            col = jnp.sum(x_sub * x_sub, axis=1, keepdims=True) * 0.5
            hr[slot, :, pl.ds(start + sub, 128)] = jnp.sum(jnp.where(eye, col, 0.0), axis=0, keepdims=True)

    def products(t, both):
        k_slot, k_row, k_col, p0, q0, v_p, v_q, acc_p, acc_q = t
        p_piece, q_piece = pl.ds(pl.multiple_of(p0, T), T), pl.ds(pl.multiple_of(q0, T), T)
        k_tile = kb[k_slot, pl.ds(pl.multiple_of(k_row, T), T), pl.ds(pl.multiple_of(k_col, T), T)]
        yield
        acc[acc_q, :, q_piece] += dot_nn(vb[v_p, :, p_piece], k_tile)
        yield
        if both:
            acc[acc_p, :, p_piece] += dot_nt(vb[v_q, :, q_piece], k_tile)
        yield

    def flush(pend, both):
        for _ in products(pend, both):
            pass

    def tile(p_slot, q_slot, t, pend, both):
        k_slot, k_row, k_col, p0, q0 = t[:5]
        k_row, k_col, p0, q0 = (pl.multiple_of(v, T) for v in (k_row, k_col, p0, q0))
        pending = products(pend, both)
        gram = None
        for f in range(0, xb.shape[2], 256):
            part = dot_nt(xb[p_slot, pl.ds(p0, T), pl.ds(f, 256)], xb[q_slot, pl.ds(q0, T), pl.ds(f, 256)])
            gram = part if gram is None else gram + part
            next(pending)
        h_q = hr[q_slot, :, pl.ds(q0, T)]
        for sub in range(0, T, 128):
            h_row = hr[p_slot, :, pl.ds(p0 + sub, 128)]
            h_p = jnp.sum(jnp.where(eye, h_row, 0.0), axis=1, keepdims=True)
            half_d = jnp.maximum(h_p + h_q - gram[sub:sub + 128], 0.0)
            kb[k_slot, pl.ds(k_row + sub, 128), pl.ds(k_col, T)] = (coef_s * jnp.exp2(half_d * coef_d)).astype(BF16)

    def tiles(count, unroll, place, pend, both=True):
        def step(i, pend):
            for sub in range(unroll):
                p_slot, q_slot, t = place(i, sub)
                t = tuple(jnp.int32(v) for v in t)
                tile(p_slot, q_slot, t, pend, both)
                pend = t
            return pend

        return lax.fori_loop(0, count, step, pend)

    nothing = tuple(jnp.int32(v) for v in (0, 0, 0, 0, 0, OWN, OWN, TRASH, TRASH))

    acc[...] = jnp.zeros_like(acc)
    own_x.wait()
    own_v.wait()

    def norm_loop(slot):
        @pl.loop(0, rows // 256)
        def _(i):
            half_norms(slot, mul(i, 256), 256)

    norm_loop(OWN)
    side = rows // T
    pend = tiles(side, side, lambda i, sub: (OWN, OWN, (0, i * T, sub * T, i * T, sub * T, OWN, OWN, TRASH, OWN)), nothing, False)

    sib_x.wait_recv()
    v_sib.wait_recv()
    norm_loop(CROSS)

    pend = tiles(side, side, lambda i, sub: (CROSS, OWN, (1, i * T, sub * T, i * T, sub * T, SIB, OWN, TRASH, OWN)), pend, False)
    flush(pend, False)
    pl.semaphore_signal(free, inc=1, device_id={"row": sib}, device_id_type=pl.DeviceIdType.MESH)
    v_minus.wait_recv()
    v_plus.wait_recv()
    v_cross.start()
    pl.semaphore_wait(free, 1)
    v_cross.wait_recv()

    def own_place(slot, j, sub):
        p0, q0 = sub * T, order(me, j) * T
        return OWN, slot, (2 if slot == PLUS else 3, p0, q0, p0, q0, OWN, slot, OWN, slot)

    final = order(minus, side - 1)
    spare = order(me, side - 1)

    def minus_place(j):
        return OWN, MINUS, (2, j * T, spare * T, final * T, order(me, j) * T, OWN, MINUS, OWN, MINUS)

    swap = me // half_ring

    def far_slots(which):
        other = MINUS + which
        return PLUS + swap * (other - PLUS), other + swap * (PLUS - other)

    def far_place(r, q, which):
        k_row = r + which * (N_PIECE - 1 - 2 * r)
        k_col = q + which * (N_PIECE - 1 - 2 * q)
        return k_row * T, k_col * T, order(me, r) * T, order(me, q) * T

    def far_tile(r, q, which):
        p_slot, q_slot = far_slots(which)
        return p_slot, q_slot, (4,) + far_place(r, q, which) + (p_slot, q_slot, p_slot, q_slot)

    def far_tiles(count, j, pend):
        def place(i, which):
            r = jnp.where(i == 0, 0, jnp.where(i == 1, j, 1))
            q = jnp.where(i == 1, 0, j)
            return far_tile(r, q, which)

        return tiles(count, 2, place, pend)

    def arrive(j):
        start = mul(order(me, j), T)
        x_recv(0, j).wait_recv()
        forward(j).start()
        x_recv(1, j).wait_recv()
        half_norms(PLUS, start, T)
        half_norms(MINUS, start, T)

    def arrive_cross(j):
        forward(j).wait_recv()
        half_norms(CROSS, mul(order(me, j), T), T)

    def stage(j, pend):
        arrive(j)
        pend = tiles(1, side + 1, lambda i, sub: own_place(PLUS, j, sub) if sub < side else minus_place(j), pend)
        arrive_cross(j)
        pend = tiles(1, side, lambda i, sub: own_place(CROSS, j, sub), pend)
        return far_tiles(jnp.where(j == 0, 1, 3), j, pend)

    def to_plus(step, j):
        return part_copies(step, order(me, j))[0]

    def to_minus(step, j):
        return part_copies(step, order(me, j))[1]

    def to_sib(step, j):
        return part_copies(step, order(me, j))[2]

    def combine(step, j):
        piece = pl.ds(mul(order(me, j), T), T)
        to_sib(step, j).wait_recv()
        acc[step * N_SUM + MINUS, :, piece] += rb[2, :, piece]
        to_minus(step, j).start()

    def arrived(step, k):
        for copy in part_copies(step, k)[:2]:
            copy.wait_recv()

    pend = lax.fori_loop(0, side - 1, stage, nothing)
    flush(pend, True)
    for j in (1, 2):
        to_sib(0, j).start()
        to_plus(0, j).start()
    for j in (1, 2):
        combine(0, j)
    last = side - 1
    arrive(last)
    flush(tiles(1, 2, lambda i, sub: far_tile(0, last, 0) if sub else minus_place(last), nothing), True)
    arrive_cross(last)
    flush(tiles(1, 1, lambda i, sub: far_tile(0, last, 1), nothing), True)
    to_sib(0, 0).start()
    to_plus(0, 0).start()
    to_plus(0, last).start()
    pend = tiles(1, side // 2, lambda i, sub: own_place(CROSS, last, sub), nothing, False)
    combine(0, 0)
    pend = tiles(1, side // 2, lambda i, sub: own_place(CROSS, last, side // 2 + sub), pend, False)
    flush(pend, False)
    to_sib(0, last).start()
    last_piece = pl.ds(mul(order(me, last), T), T)
    acc[OWN] += dot_nt(vb[CROSS, :, last_piece], kb[3, :, last_piece])
    combine(0, last)
    acc[pl.ds(N_SUM, N_SUM)] = jnp.zeros((N_SUM,) + acc.shape[1:], F32)

    def apply_nn(k_slot, y_slot, out, k):
        piece = pl.ds(mul(k, T), T)
        acc[N_SUM + out] += dot_nn(y_ref(y_slot)[:, piece], kb[k_slot, piece, :])

    def apply_nt(k_slot, y_slot, out, k):
        piece = pl.ds(mul(k, T), T)
        acc[N_SUM + out] += dot_nt(y_ref(y_slot)[:, piece], kb[k_slot, :, piece])

    def make_y(k):
        piece = pl.ds(mul(k, T), T)
        arrived(0, k)
        y_ref(OWN)[:, piece] = (acc[OWN, :, piece] + rb[0, :, piece] + rb[1, :, piece]).astype(BF16)

    plus_cols = pl.ds(mul(me // half_ring, T), rows - T)

    def apply_own(k):
        piece = pl.ds(mul(k, T), T)
        acc[N_SUM + PLUS, :, plus_cols] += dot_nn(y_ref(OWN)[:, piece], kb[2, piece, plus_cols])
        apply_nn(3, OWN, CROSS, k)

    @pl.loop(1, 3)
    def _(k):
        make_y(k)
        y_plus, y_minus, y_sib, _ = y_copies(k)
        y_plus.start()
        y_minus.start()
        y_sib.start()
        apply_own(k)

    first = order(minus, 0)
    make_y(first)
    make_y(final)
    y_copies(first)[1].start()
    y_copies(final)[0].start()
    y_copies(final)[1].start()
    y_copies(first)[0].start()
    y_copies(first)[2].start()
    y_copies(final)[2].start()

    def y_forward(j):
        y_copies(order(me, j))[0].wait_recv()
        y_copies(order(me, j))[3].start()

    def y_rest(j):
        y_copies(order(me, j))[1].wait_recv()
        y_copies(order(me, j))[3].wait_recv()

    def apply_sib(k):
        y_copies(k)[2].wait_recv()
        apply_nn(1, SIB, OWN, k)

    y_forward(1)
    y_forward(2)

    @pl.loop(0, 2)
    def _(i):
        apply_own(first + i * (final - first))

    spare_cols = pl.ds(mul(spare, T), T)
    for j in range(N_PIECE):
        acc[N_SUM + MINUS, :, pl.ds(mul(order(me, j), T), T)] += dot_nn(
            y_ref(OWN)[:, pl.ds(mul(final, T), T)], kb[2, j * T:(j + 1) * T, spare_cols])
    def far_products(group_nn, group_nt, pairs=(0, 1)):
        for which in pairs:
            p_slot, q_slot = far_slots(which)

            def y_piece(slot, start):
                return yb[slot - PLUS, :, pl.ds(pl.multiple_of(start, T), T)]

            for q in sorted({q for _, q in group_nn}):
                total = None
                for r in sorted({r for r, c in group_nn if c == q}):
                    k_row, k_col, p0, q0 = far_place(r, q, which)
                    part = dot_nn(y_piece(p_slot, p0), kb[4, k_row:k_row + T, k_col:k_col + T])
                    total = part if total is None else total + part
                acc[N_SUM + q_slot, :, pl.ds(pl.multiple_of(q0, T), T)] += total
            for r in sorted({r for r, _ in group_nt}):
                total = None
                for q in sorted({q for c, q in group_nt if c == r}):
                    k_row, k_col, p0, q0 = far_place(r, q, which)
                    part = dot_nt(y_piece(q_slot, q0), kb[4, k_row:k_row + T, k_col:k_col + T])
                    total = part if total is None else total + part
                acc[N_SUM + p_slot, :, pl.ds(pl.multiple_of(p0, T), T)] += total

    y_rest(1)
    y_rest(2)
    far_products(((1, 1), (1, 2)), ((1, 1), (1, 2)))
    y_forward(0)
    y_copies(order(me, 0))[1].wait_recv()
    def by_row(*pairs):
        return lambda: far_products(((0, 1), (0, 2)), (), pairs)

    def by_col(*pairs):
        return lambda: far_products((), ((1, 0), (2, 0)), pairs)

    pl.when(swap == 0)(by_row(1))
    pl.when(swap != 0)(by_col(1))
    for j in (1, 2):
        to_sib(1, j).start()
    pl.when(swap == 0)(by_row(0))
    pl.when(swap != 0)(by_col(0))
    y_copies(order(me, 0))[3].wait_recv()
    pl.when(swap == 0)(by_col(0, 1))
    pl.when(swap != 0)(by_row(0, 1))
    for j in (1, 2):
        to_plus(1, j).start()
    for j in (1, 2):
        combine(1, j)
    y_forward(last)
    far_products(((0, 0), (1, 0), (2, 0)), ((0, 0), (0, 1), (0, 2)))
    y_rest(last)
    far_products(((0, last),), ((0, last),))
    for j in (0, last):
        to_sib(1, j).start()
        to_plus(1, j).start()
    apply_nn(0, OWN, OWN, 0)
    apply_sib(0)
    for j in (0, last):
        combine(1, j)

    @pl.loop(1, N_PIECE)
    def _(k):
        apply_nn(0, OWN, OWN, k)
        apply_sib(k)

    @pl.loop(0, N_PIECE - 1)
    def _(j):
        apply_nt(2, PLUS, OWN, order(me, j))
        apply_nt(3, CROSS, OWN, order(me, j))

    apply_nt(3, CROSS, OWN, spare)
    acc[N_SUM + OWN, :, pl.ds(mul(final, T), T)] += sum(
        dot_nt(yb[MINUS - PLUS, :, pl.ds(mul(order(me, j), T), T)], kb[2, j * T:(j + 1) * T, spare_cols])
        for j in range(N_PIECE))

    def out_copy(k):
        piece = pl.ds(mul(k, T), T)
        return pltpu.make_async_copy(acc.at[OWN, :, piece], out_hbm.at[:, piece], loc.at[k])

    for k in (1, 2, first, final):
        piece = pl.ds(mul(k, T), T)
        arrived(1, k)
        acc[OWN, :, piece] = acc[N_SUM + OWN, :, piece] + rb[0, :, piece] + rb[1, :, piece]
        out_copy(k).start()
    for copy in (v_plus, v_minus, v_sib, v_cross, sib_x):
        copy.wait_send()
    for k in range(N_PIECE):
        for copy in part_copies(0, k) + part_copies(1, k) + y_copies(k):
            copy.wait_send()
        x_send(0, k).wait_send()
        x_send(1, k).wait_send()
        forward(k).wait_send()
        out_copy(k).wait()


def solution(mesh):
    n_row = mesh.shape["row"]
    assert n_row == 8

    def local_program(x_loc, v_loc, length_scale, out_scale):
        rows, feat = x_loc.shape
        cols = v_loc.shape[1]
        dma = pltpu.SemaphoreType.DMA
        out = pl.pallas_call(
            functools.partial(kernel, n_row),
            out_shape=jax.ShapeDtypeStruct((cols, rows), F32),
            in_specs=[pl.BlockSpec(memory_space=pl.ANY), pl.BlockSpec(memory_space=pl.ANY),
                      pl.BlockSpec(memory_space=pltpu.SMEM), pl.BlockSpec(memory_space=pltpu.SMEM)],
            out_specs=pl.BlockSpec(memory_space=pl.ANY),
            scratch_shapes=[
                pltpu.VMEM((4, rows, feat), BF16),
                pltpu.VMEM((5, rows, rows), BF16),
                pltpu.VMEM((5, cols, rows), BF16),
                pltpu.VMEM((3, cols, rows), BF16),
                pltpu.VMEM((4, 1, rows), F32),
                pltpu.VMEM((2 * N_SUM, cols, rows), F32),
                pltpu.VMEM((3, cols, rows), F32),
                dma((2, N_PIECE)), dma((2, N_PIECE)), dma((N_PIECE,)), dma((N_PIECE,)),
                dma, dma, dma((N_PIECE,)), dma((4,)), dma((4,)), dma((4, N_PIECE)), dma((4, N_PIECE)),
                dma((2, 3, N_PIECE)), dma((2, 3, N_PIECE)), pltpu.SemaphoreType.REGULAR,
            ],
            compiler_params=pltpu.CompilerParams(
                collective_id=0, has_side_effects=True, vmem_limit_bytes=67043328),
        )(x_loc, v_loc.T, length_scale, out_scale)
        return out.T

    row_spec = P(("task", "row"), None)
    return jax.shard_map(local_program, mesh=mesh, in_specs=(row_spec, row_spec, P("task"), P("task")),
                         out_specs=row_spec, check_vma=False)
```

```python
import functools

import jax
import jax.numpy as jnp
from jax import lax
from jax.experimental import pallas as pl
from jax.experimental.pallas import tpu as pltpu
from jax.sharding import PartitionSpec as P

F32 = jnp.float32
BF16 = jnp.bfloat16
LOG2E = 1.4426950408889634
OWN, PLUS, MINUS, CROSS, SIB = 0, 1, 2, 3, 4
N_SUM = 4
TRASH = 7
T = 512
N_PIECE = 4


def dot_nn(a, b):
    return lax.dot_general(a, b, (((1,), (0,)), ((), ())), preferred_element_type=F32)


def dot_nt(a, b):
    return lax.dot_general(a, b, (((1,), (1,)), ((), ())), preferred_element_type=F32)


def kernel(n_row, x_hbm, vt_hbm, length_scale, out_scale, out_hbm, xb, kb, vb, yb, hr, acc, rb,
           x_s, x_r, f_s, f_r, sib_s, sib_r, loc, v_s, v_r, y_s, y_r, p_s, p_r, free):
    rows = xb.shape[1]
    me = lax.axis_index("row")
    core = me % 2
    sib = me + 1 - 2 * core
    plus = (me + 2) % n_row
    minus = (me + n_row - 2) % n_row
    half_ring = n_row // 2

    def order(dev, j):
        flip = dev // half_ring
        return j + flip * (N_PIECE - 1 - 2 * j)

    def remote(src, dst, s_sem, r_sem, dev):
        return pltpu.make_async_remote_copy(
            src_ref=src, dst_ref=dst, send_sem=s_sem, recv_sem=r_sem,
            device_id={"row": dev}, device_id_type=pl.DeviceIdType.MESH)

    def x_send(direction, j):
        slot, dev = ((MINUS, plus), (PLUS, minus))[direction]
        piece = pl.ds(mul(order(dev, j), T), T)
        return remote(x_hbm.at[piece], xb.at[slot, piece], x_s.at[direction, j], x_r.at[direction, j], dev)

    def x_recv(direction, j):
        slot, dev = ((MINUS, plus), (PLUS, minus))[direction]
        piece = pl.ds(mul(order(me, j), T), T)
        return remote(x_hbm.at[piece], xb.at[slot, piece], x_s.at[direction, j], x_r.at[direction, j], dev)

    def forward(j):
        piece = pl.ds(mul(order(me, j), T), T)
        return remote(xb.at[MINUS, piece], xb.at[CROSS, piece], f_s.at[j], f_r.at[j], sib)

    def vec_copies(own, place, s_sem, r_sem):
        return (remote(own, place(MINUS), s_sem(0), r_sem(0), plus),
                remote(own, place(PLUS), s_sem(1), r_sem(1), minus),
                remote(own, place(SIB), s_sem(2), r_sem(2), sib),
                remote(place(MINUS), place(CROSS), s_sem(3), r_sem(3), sib))

    def y_ref(slot):
        return vb.at[slot] if slot in (OWN, SIB) else yb.at[slot - PLUS]

    def y_copies(k):
        piece = pl.ds(mul(k, T), T)
        return vec_copies(y_ref(OWN).at[:, piece], lambda slot: y_ref(slot).at[:, piece],
                          lambda d: y_s.at[d, k], lambda d: y_r.at[d, k])

    def part_copies(step, k):
        cols = pl.ds(mul(k, T), T)
        return tuple(remote(acc.at[step * N_SUM + slot, :, cols], rb.at[i, :, cols], p_s.at[step, i, k], p_r.at[step, i, k], dev)
                     for i, (slot, dev) in enumerate(((PLUS, plus), (MINUS, minus), (CROSS, sib))))

    def mul(i, size):
        return i * size if isinstance(i, int) else pl.multiple_of(i * size, size)

    barrier = pltpu.get_barrier_semaphore()
    for dev in (sib, plus, minus):
        pl.semaphore_signal(barrier, inc=1, device_id={"row": dev}, device_id_type=pl.DeviceIdType.MESH)
    pl.semaphore_wait(barrier, 3)

    own_x = pltpu.make_async_copy(x_hbm, xb.at[OWN], loc.at[0])
    own_v = pltpu.make_async_copy(vt_hbm, vb.at[OWN], loc.at[1])
    v_plus, v_minus, v_sib, v_cross = vec_copies(
        vt_hbm, lambda slot: vb.at[slot], lambda d: v_s.at[d], lambda d: v_r.at[d])
    sib_x = remote(x_hbm, xb.at[CROSS], sib_s, sib_r, sib)
    v_plus.start()
    v_minus.start()
    for j in range(N_PIECE):
        x_send(0, j).start()
        x_send(1, j).start()
    own_x.start()
    own_v.start()
    v_sib.start()
    sib_x.start()

    scale = jnp.full((8, 128), length_scale[0], F32)
    coef_d = (-2.0 * LOG2E / (2.0 * scale * scale))[0, 0]
    coef_s = out_scale[0]
    eye = (lax.broadcasted_iota(jnp.int32, (128, 128), 0) == lax.broadcasted_iota(jnp.int32, (128, 128), 1))

    def half_norms(slot, start, width):
        for sub in range(0, width, 128):
            x_sub = xb[slot, pl.ds(start + sub, 128), :].astype(F32)
            col = jnp.sum(x_sub * x_sub, axis=1, keepdims=True) * 0.5
            hr[slot, :, pl.ds(start + sub, 128)] = jnp.sum(jnp.where(eye, col, 0.0), axis=0, keepdims=True)

    def products(t, both):
        k_slot, k_row, k_col, p0, q0, v_p, v_q, acc_p, acc_q = t
        p_piece, q_piece = pl.ds(pl.multiple_of(p0, T), T), pl.ds(pl.multiple_of(q0, T), T)
        k_tile = kb[k_slot, pl.ds(pl.multiple_of(k_row, T), T), pl.ds(pl.multiple_of(k_col, T), T)]
        yield
        acc[acc_q, :, q_piece] += dot_nn(vb[v_p, :, p_piece], k_tile)
        yield
        if both:
            acc[acc_p, :, p_piece] += dot_nt(vb[v_q, :, q_piece], k_tile)
        yield

    def flush(pend, both):
        for _ in products(pend, both):
            pass

    def tile(p_slot, q_slot, t, pend, both):
        k_slot, k_row, k_col, p0, q0 = t[:5]
        k_row, k_col, p0, q0 = (pl.multiple_of(v, T) for v in (k_row, k_col, p0, q0))
        pending = products(pend, both)
        gram = None
        for f in range(0, xb.shape[2], 256):
            part = dot_nt(xb[p_slot, pl.ds(p0, T), pl.ds(f, 256)], xb[q_slot, pl.ds(q0, T), pl.ds(f, 256)])
            gram = part if gram is None else gram + part
            next(pending)
        h_q = hr[q_slot, :, pl.ds(q0, T)]
        for sub in range(0, T, 128):
            h_row = hr[p_slot, :, pl.ds(p0 + sub, 128)]
            h_p = jnp.sum(jnp.where(eye, h_row, 0.0), axis=1, keepdims=True)
            half_d = jnp.maximum(h_p + h_q - gram[sub:sub + 128], 0.0)
            kb[k_slot, pl.ds(k_row + sub, 128), pl.ds(k_col, T)] = (coef_s * jnp.exp2(half_d * coef_d)).astype(BF16)

    def tiles(count, unroll, place, pend, both=True):
        def step(i, pend):
            for sub in range(unroll):
                p_slot, q_slot, t = place(i, sub)
                t = tuple(jnp.int32(v) for v in t)
                tile(p_slot, q_slot, t, pend, both)
                pend = t
            return pend

        return lax.fori_loop(0, count, step, pend)

    nothing = tuple(jnp.int32(v) for v in (0, 0, 0, 0, 0, OWN, OWN, TRASH, TRASH))

    acc[...] = jnp.zeros_like(acc)
    own_x.wait()
    own_v.wait()

    def norm_loop(slot):
        @pl.loop(0, rows // 256)
        def _(i):
            half_norms(slot, mul(i, 256), 256)

    norm_loop(OWN)
    side = rows // T
    pend = tiles(side, side, lambda i, sub: (OWN, OWN, (0, i * T, sub * T, i * T, sub * T, OWN, OWN, TRASH, OWN)), nothing, False)

    sib_x.wait_recv()
    v_sib.wait_recv()
    norm_loop(CROSS)

    pend = tiles(side, side, lambda i, sub: (CROSS, OWN, (1, i * T, sub * T, i * T, sub * T, SIB, OWN, TRASH, OWN)), pend, False)
    flush(pend, False)
    pl.semaphore_signal(free, inc=1, device_id={"row": sib}, device_id_type=pl.DeviceIdType.MESH)
    v_minus.wait_recv()
    v_plus.wait_recv()
    v_cross.start()
    pl.semaphore_wait(free, 1)
    v_cross.wait_recv()

    def own_place(slot, j, sub):
        p0, q0 = sub * T, order(me, j) * T
        return OWN, slot, (2 if slot == PLUS else 3, p0, q0, p0, q0, OWN, slot, OWN, slot)

    final = order(minus, side - 1)
    spare = order(me, side - 1)

    def minus_place(j):
        return OWN, MINUS, (2, j * T, spare * T, final * T, order(me, j) * T, OWN, MINUS, OWN, MINUS)

    swap = me // half_ring

    def far_slots(which):
        other = MINUS + which
        return PLUS + swap * (other - PLUS), other + swap * (PLUS - other)

    def far_place(r, q, which):
        k_row = r + which * (N_PIECE - 1 - 2 * r)
        k_col = q + which * (N_PIECE - 1 - 2 * q)
        return k_row * T, k_col * T, order(me, r) * T, order(me, q) * T

    def far_tile(r, q, which):
        p_slot, q_slot = far_slots(which)
        return p_slot, q_slot, (4,) + far_place(r, q, which) + (p_slot, q_slot, p_slot, q_slot)

    def far_tiles(count, j, pend):
        def place(i, which):
            r = jnp.where(i == 0, 0, jnp.where(i == 1, j, 1))
            q = jnp.where(i == 1, 0, j)
            return far_tile(r, q, which)

        return tiles(count, 2, place, pend)

    def arrive(j):
        start = mul(order(me, j), T)
        x_recv(0, j).wait_recv()
        forward(j).start()
        half_norms(MINUS, start, T)
        x_recv(1, j).wait_recv()
        half_norms(PLUS, start, T)

    def arrive_cross(j):
        forward(j).wait_recv()
        half_norms(CROSS, mul(order(me, j), T), T)

    def stage(j, pend):
        arrive(j)
        pend = tiles(1, side + 1, lambda i, sub: own_place(PLUS, j, sub) if sub < side else minus_place(j), pend)
        arrive_cross(j)
        pend = tiles(1, side, lambda i, sub: own_place(CROSS, j, sub), pend)
        return far_tiles(jnp.where(j == 0, 1, 3), j, pend)

    def to_plus(step, j):
        return part_copies(step, order(me, j))[0]

    def to_minus(step, j):
        return part_copies(step, order(me, j))[1]

    def to_sib(step, j):
        return part_copies(step, order(me, j))[2]

    def combine(step, j):
        piece = pl.ds(mul(order(me, j), T), T)
        to_sib(step, j).wait_recv()
        acc[step * N_SUM + MINUS, :, piece] += rb[2, :, piece]
        to_minus(step, j).start()

    def arrived(step, k):
        for copy in part_copies(step, k)[:2]:
            copy.wait_recv()

    pend = lax.fori_loop(0, side - 1, stage, nothing)
    flush(pend, True)
    for j in (1, 2):
        to_sib(0, j).start()
        to_plus(0, j).start()
    for j in (1, 2):
        combine(0, j)
    last = side - 1
    arrive(last)
    flush(tiles(1, 2, lambda i, sub: far_tile(0, last, 0) if sub else minus_place(last), nothing), True)
    arrive_cross(last)
    flush(tiles(1, 1, lambda i, sub: far_tile(0, last, 1), nothing), True)
    to_sib(0, 0).start()
    to_plus(0, 0).start()
    to_plus(0, last).start()
    pend = tiles(1, side // 2, lambda i, sub: own_place(CROSS, last, sub), nothing, False)
    combine(0, 0)
    pend = tiles(1, side // 2, lambda i, sub: own_place(CROSS, last, side // 2 + sub), pend, False)
    flush(pend, False)
    to_sib(0, last).start()
    last_piece = pl.ds(mul(order(me, last), T), T)
    acc[OWN] += dot_nt(vb[CROSS, :, last_piece], kb[3, :, last_piece])
    combine(0, last)
    acc[pl.ds(N_SUM, N_SUM)] = jnp.zeros((N_SUM,) + acc.shape[1:], F32)

    def apply_nn(k_slot, y_slot, out, k):
        piece = pl.ds(mul(k, T), T)
        acc[N_SUM + out] += dot_nn(y_ref(y_slot)[:, piece], kb[k_slot, piece, :])

    def apply_nt(k_slot, y_slot, out, k):
        piece = pl.ds(mul(k, T), T)
        acc[N_SUM + out] += dot_nt(y_ref(y_slot)[:, piece], kb[k_slot, :, piece])

    def make_y(k):
        piece = pl.ds(mul(k, T), T)
        arrived(0, k)
        y_ref(OWN)[:, piece] = (acc[OWN, :, piece] + rb[0, :, piece] + rb[1, :, piece]).astype(BF16)

    plus_cols = pl.ds(mul(me // half_ring, T), rows - T)

    def apply_own(k):
        piece = pl.ds(mul(k, T), T)
        acc[N_SUM + PLUS, :, plus_cols] += dot_nn(y_ref(OWN)[:, piece], kb[2, piece, plus_cols])
        apply_nn(3, OWN, CROSS, k)

    @pl.loop(1, 3)
    def _(k):
        make_y(k)
        y_plus, y_minus, y_sib, _ = y_copies(k)
        y_plus.start()
        y_minus.start()
        y_sib.start()
        apply_own(k)

    first = order(minus, 0)
    make_y(first)
    make_y(final)
    y_copies(first)[1].start()
    y_copies(final)[0].start()
    y_copies(final)[1].start()
    y_copies(first)[0].start()
    y_copies(first)[2].start()
    y_copies(final)[2].start()

    def y_forward(j):
        y_copies(order(me, j))[0].wait_recv()
        y_copies(order(me, j))[3].start()

    def y_rest(j):
        y_copies(order(me, j))[1].wait_recv()
        y_copies(order(me, j))[3].wait_recv()

    def apply_sib(k):
        y_copies(k)[2].wait_recv()
        apply_nn(1, SIB, OWN, k)

    y_forward(1)
    y_forward(2)

    @pl.loop(0, 2)
    def _(i):
        apply_own(first + i * (final - first))

    spare_cols = pl.ds(mul(spare, T), T)
    for j in range(N_PIECE):
        acc[N_SUM + MINUS, :, pl.ds(mul(order(me, j), T), T)] += dot_nn(
            y_ref(OWN)[:, pl.ds(mul(final, T), T)], kb[2, j * T:(j + 1) * T, spare_cols])
    def far_products(group_nn, group_nt, pairs=(0, 1)):
        for which in pairs:
            p_slot, q_slot = far_slots(which)

            def y_piece(slot, start):
                return yb[slot - PLUS, :, pl.ds(pl.multiple_of(start, T), T)]

            for q in sorted({q for _, q in group_nn}):
                total = None
                for r in sorted({r for r, c in group_nn if c == q}):
                    k_row, k_col, p0, q0 = far_place(r, q, which)
                    part = dot_nn(y_piece(p_slot, p0), kb[4, k_row:k_row + T, k_col:k_col + T])
                    total = part if total is None else total + part
                acc[N_SUM + q_slot, :, pl.ds(pl.multiple_of(q0, T), T)] += total
            for r in sorted({r for r, _ in group_nt}):
                total = None
                for q in sorted({q for c, q in group_nt if c == r}):
                    k_row, k_col, p0, q0 = far_place(r, q, which)
                    part = dot_nt(y_piece(q_slot, q0), kb[4, k_row:k_row + T, k_col:k_col + T])
                    total = part if total is None else total + part
                acc[N_SUM + p_slot, :, pl.ds(pl.multiple_of(p0, T), T)] += total

    y_rest(1)
    y_rest(2)
    far_products(((1, 1), (1, 2)), ((1, 1), (1, 2)))
    y_forward(0)
    y_copies(order(me, 0))[1].wait_recv()
    def by_row(*pairs):
        return lambda: far_products(((0, 1), (0, 2)), (), pairs)

    def by_col(*pairs):
        return lambda: far_products((), ((1, 0), (2, 0)), pairs)

    pl.when(swap == 0)(by_row(1))
    pl.when(swap != 0)(by_col(1))
    for j in (1, 2):
        to_sib(1, j).start()
    pl.when(swap == 0)(by_row(0))
    pl.when(swap != 0)(by_col(0))
    y_copies(order(me, 0))[3].wait_recv()
    pl.when(swap == 0)(by_col(0, 1))
    pl.when(swap != 0)(by_row(0, 1))
    for j in (1, 2):
        to_plus(1, j).start()
    for j in (1, 2):
        combine(1, j)
    y_forward(last)
    far_products(((0, 0), (1, 0), (2, 0)), ((0, 0), (0, 1), (0, 2)))
    y_rest(last)
    far_products(((0, last),), ((0, last),), (1,))
    for j in (0, last):
        to_sib(1, j).start()
    far_products(((0, last),), ((0, last),), (0,))
    for j in (0, last):
        to_plus(1, j).start()
    apply_nn(0, OWN, OWN, 0)
    apply_sib(0)
    for j in (0, last):
        combine(1, j)

    @pl.loop(1, N_PIECE)
    def _(k):
        apply_nn(0, OWN, OWN, k)
        apply_sib(k)

    @pl.loop(0, N_PIECE - 1)
    def _(j):
        apply_nt(2, PLUS, OWN, order(me, j))
        apply_nt(3, CROSS, OWN, order(me, j))

    apply_nt(3, CROSS, OWN, spare)
    acc[N_SUM + OWN, :, pl.ds(mul(final, T), T)] += sum(
        dot_nt(yb[MINUS - PLUS, :, pl.ds(mul(order(me, j), T), T)], kb[2, j * T:(j + 1) * T, spare_cols])
        for j in range(N_PIECE))

    def out_copy(k):
        piece = pl.ds(mul(k, T), T)
        return pltpu.make_async_copy(acc.at[OWN, :, piece], out_hbm.at[:, piece], loc.at[k])

    for k in (1, 2, first, final):
        piece = pl.ds(mul(k, T), T)
        arrived(1, k)
        acc[OWN, :, piece] = acc[N_SUM + OWN, :, piece] + rb[0, :, piece] + rb[1, :, piece]
        out_copy(k).start()
    for copy in (v_plus, v_minus, v_sib, v_cross, sib_x):
        copy.wait_send()
    for k in range(N_PIECE):
        for copy in part_copies(0, k) + part_copies(1, k) + y_copies(k):
            copy.wait_send()
        x_send(0, k).wait_send()
        x_send(1, k).wait_send()
        forward(k).wait_send()
        out_copy(k).wait()


def solution(mesh):
    n_row = mesh.shape["row"]
    assert n_row == 8

    def local_program(x_loc, v_loc, length_scale, out_scale):
        rows, feat = x_loc.shape
        cols = v_loc.shape[1]
        dma = pltpu.SemaphoreType.DMA
        out = pl.pallas_call(
            functools.partial(kernel, n_row),
            out_shape=jax.ShapeDtypeStruct((cols, rows), F32),
            in_specs=[pl.BlockSpec(memory_space=pl.ANY), pl.BlockSpec(memory_space=pl.ANY),
                      pl.BlockSpec(memory_space=pltpu.SMEM), pl.BlockSpec(memory_space=pltpu.SMEM)],
            out_specs=pl.BlockSpec(memory_space=pl.ANY),
            scratch_shapes=[
                pltpu.VMEM((4, rows, feat), BF16),
                pltpu.VMEM((5, rows, rows), BF16),
                pltpu.VMEM((5, cols, rows), BF16),
                pltpu.VMEM((3, cols, rows), BF16),
                pltpu.VMEM((4, 1, rows), F32),
                pltpu.VMEM((2 * N_SUM, cols, rows), F32),
                pltpu.VMEM((3, cols, rows), F32),
                dma((2, N_PIECE)), dma((2, N_PIECE)), dma((N_PIECE,)), dma((N_PIECE,)),
                dma, dma, dma((N_PIECE,)), dma((4,)), dma((4,)), dma((4, N_PIECE)), dma((4, N_PIECE)),
                dma((2, 3, N_PIECE)), dma((2, 3, N_PIECE)), pltpu.SemaphoreType.REGULAR,
            ],
            compiler_params=pltpu.CompilerParams(
                collective_id=0, has_side_effects=True, vmem_limit_bytes=67043328),
        )(x_loc, v_loc.T, length_scale, out_scale)
        return out.T

    row_spec = P(("task", "row"), None)
    return jax.shard_map(local_program, mesh=mesh, in_specs=(row_spec, row_spec, P("task"), P("task")),
                         out_specs=row_spec, check_vma=False)
```
